32 devices in a mesh: section: 4 (over z), tensor: 4 (over y, x), dp: 2 (over core).
Axes of the slice: x: 2, y: 2, z: 4, core: 2. Of those that a mesh axis runs over, the one named last changes fastest.
Arguments:
- enc_hidden: bfloat16 [128, 2048], P(('dp', 'tensor'), 'section'), parts along dimension 0, may hold values from -70 to 70
- mlp_gain: float32 [2048], P('section'), may hold values from 0.25 to 1.75
- final_gain: float32 [2048], P('section'), may hold values from 0.25 to 1.75
- w_gate: bfloat16 [2048, 8192], P('section', 'tensor'), may hold values from -0.125 to 0.125
- w_up: bfloat16 [2048, 8192], P('section', 'tensor'), may hold values from -0.125 to 0.125
- w_down: bfloat16 [8192, 2048], P('tensor', 'section'), may hold values from -0.0625 to 0.0625
- key_weight: bfloat16 [4, 2048, 4096], P('section', None, 'tensor'), may hold values from -0.125 to 0.125
- value_weight: bfloat16 [4, 2048, 4096], P('section', None, 'tensor'), may hold values from -0.125 to 0.125
- queries: bfloat16 [4, 2048, 4096], P('section', 'dp', 'tensor'), parts along dimension 1, may hold values from -340 to 340
- context_grad: bfloat16 [4, 2048, 4096], P('section', 'dp', 'tensor'), parts along dimension 1, may hold values from -6 to 6
Outputs:
- query_grad: bfloat16 [4, 2048, 4096], P('section', 'dp', 'tensor'), parts along dimension 1
- hidden_grad: float32 [128, 2048], P(('dp', 'tensor'), 'section'), parts along dimension 0
- gate_weight_grad: bfloat16 [4096, 8192], P(('dp', 'section'), 'tensor'), parts along dimension 0
- up_weight_grad: bfloat16 [4096, 8192], P(('dp', 'section'), 'tensor'), parts along dimension 0
- down_weight_grad: bfloat16 [16384, 2048], P(('dp', 'tensor'), 'section'), parts along dimension 0
The draws below stay inside these ranges and needn't reach their ends.
There are 2 independent parts, one for each index of `dp`. The reference program is written for one: setup_inputs(seed, part) draws one part's arguments, and reference() takes and returns one part's arrays. A program takes and returns all parts, laid end to end along the dimension named above; an argument that names none is the same for every part. Nothing has to cross between parts.
All inputs are finite; a program needn't handle non-finite values.
Results may differ from the reference program's by a relative error of at most 0.017.
Values may be sent and summed in bfloat16 or wider, within the bound.
A program may use at most 64 MiB of HBM per device.

```python
import math
import jax
import jax.numpy as jnp
from jax import lax

D = 2048
FF = 8192
HEADS = 16
HEAD = 256
TGT = 1024
SRC = 64
LAYERS = 4
HD = 4096


def draw_enc_hidden(key, part):
    key_base = jax.random.fold_in(key, 11)
    key_rows = jax.random.fold_in(key, 12)
    key_cols = jax.random.fold_in(key, 13)
    col_trend = 1.0 + 2.0 * jnp.arange(D, dtype=jnp.float32)[None, :] / D
    col_scale = col_trend * jnp.exp(jax.random.uniform(key_cols, (1, D), jnp.float32, 0.0, math.log(10.0 / 3.0)))
    row_scale = 0.1 * jnp.exp(jax.random.uniform(key_rows, (SRC, 1), jnp.float32, 0.0, math.log(10.0)))
    base_draw = jnp.clip(jax.random.normal(key_base, (SRC, D), jnp.float32), -6.0, 6.0)
    return (base_draw * row_scale * col_scale).astype(jnp.bfloat16)


def draw_queries(key, part):
    key_base = jax.random.fold_in(key, 21)
    base_draw = jnp.clip(jax.random.normal(key_base, (LAYERS, TGT, HEADS * HEAD), jnp.float32), -6.0, 6.0)
    return base_draw.astype(jnp.bfloat16)


def draw_context_grad(key, part):
    key_base = jax.random.fold_in(key, 31)
    base_draw = jnp.clip(jax.random.normal(key_base, (LAYERS, TGT, HEADS * HEAD), jnp.float32), -6.0, 6.0)
    return base_draw.astype(jnp.bfloat16)


def steps_of(rng, dims, pieces, smallest, largest):
    loudness = 1.0
    for position, parts in pieces:
        steps = jax.random.uniform(jax.random.fold_in(jax.random.fold_in(rng, 6), position), (parts,), jnp.float32, smallest / len(pieces), largest / len(pieces))
        loudness = loudness * jnp.repeat(jnp.exp(steps), dims[position] // parts).reshape((-1,) + (1,) * (len(dims) - 1 - position))
    return loudness


def normal_values(stream_key, shape, deviation, most, pieces=(), kind=jnp.bfloat16):
    loudness = steps_of(stream_key, shape, pieces, -0.22, 0.18) if pieces else 1.0
    result = jax.random.normal(stream_key, shape, jnp.float32) * deviation * loudness
    return jnp.minimum(jnp.maximum(result, -most), most).astype(kind)


def setup_inputs(seed: int = 0, part: int = 0) -> dict:
    splits = jax.random.split(jax.random.key(seed), 11)
    part_keys = jax.random.split(jax.random.fold_in(splits[10], part), 11)
    enc_hidden = draw_enc_hidden(jax.random.fold_in(jax.random.fold_in(splits[10], part), 71), part)
    mlp_gain = jnp.clip(1.0 + 0.15 * jax.random.normal(splits[1], (D,), jnp.float32), 0.25, 1.75)
    final_gain = jnp.clip(1.0 + 0.15 * jax.random.normal(splits[2], (D,), jnp.float32), 0.25, 1.75)
    w_gate = normal_values(splits[3], (D, FF), D ** -0.5, 0.125, ((0, 4), (1, 4)))
    w_up = normal_values(splits[4], (D, FF), D ** -0.5, 0.125, ((0, 4), (1, 4)))
    w_down = normal_values(splits[5], (FF, D), FF ** -0.5, 0.0625, ((0, 4), (1, 4)))
    key_weight = normal_values(splits[6], (LAYERS, D, HD), D ** -0.5, 0.125, ((0, 4), (2, 4)))
    value_weight = normal_values(splits[7], (LAYERS, D, HD), D ** -0.5, 0.125, ((0, 4), (2, 4)))
    queries = draw_queries(jax.random.fold_in(jax.random.fold_in(splits[10], part), 71), part)
    context_grad = draw_context_grad(jax.random.fold_in(jax.random.fold_in(splits[10], part), 71), part)
    return {"enc_hidden": enc_hidden, "mlp_gain": mlp_gain, "final_gain": final_gain, "w_gate": w_gate, "w_up": w_up, "w_down": w_down, "key_weight": key_weight, "value_weight": value_weight, "queries": queries, "context_grad": context_grad}


EPSILON = 1e-06

def layer_pass(encoded, key_matrix, value_matrix, query_block, grad_block):
    scale_factor = HEAD ** (-0.5)
    keys = jnp.dot(encoded, key_matrix, preferred_element_type=jnp.float32).astype(jnp.bfloat16)
    values = jnp.dot(encoded, value_matrix, preferred_element_type=jnp.float32).astype(jnp.bfloat16)
    src_rows = keys.shape[0]
    tgt_rows = query_block.shape[0]
    query_heads = query_block.reshape(tgt_rows, HEADS, HEAD).astype(jnp.float32)
    key_heads = keys.reshape(src_rows, HEADS, HEAD).astype(jnp.float32)
    value_heads = values.reshape(src_rows, HEADS, HEAD).astype(jnp.float32)
    grad_heads = grad_block.reshape(tgt_rows, HEADS, HEAD).astype(jnp.float32)
    scores = jnp.einsum('qhd,khd->hqk', query_heads, key_heads) * scale_factor
    probs = jax.nn.softmax(scores, axis=-1)
    probs_bf = probs.astype(jnp.bfloat16)
    probs_wide = probs_bf.astype(jnp.float32)
    context = jnp.einsum('hqk,khd->qhd', probs_wide, value_heads)
    delta = lax.optimization_barrier(jnp.sum(grad_heads * context, axis=2))
    dprob = jnp.einsum('qhd,khd->hqk', grad_heads, value_heads)
    dscore = (probs * (dprob - jnp.transpose(delta)[:, :, None]) * scale_factor).astype(jnp.bfloat16)
    dscore_wide = dscore.astype(jnp.float32)
    query_grad = jnp.einsum('hqk,khd->qhd', dscore_wide, key_heads).astype(jnp.bfloat16)
    key_grad = jnp.einsum('hqk,qhd->khd', dscore_wide, query_heads).astype(jnp.bfloat16)
    value_grad = jnp.einsum('hqk,qhd->khd', probs_wide, grad_heads).astype(jnp.bfloat16)
    key_grad = key_grad.reshape(src_rows, HEADS * HEAD)
    value_grad = value_grad.reshape(src_rows, HEADS * HEAD)
    contract = (((1,), (1,)), ((), ()))
    encoded_grad = lax.dot_general(key_grad, key_matrix, contract, preferred_element_type=jnp.float32)
    encoded_grad = encoded_grad + lax.dot_general(value_grad, value_matrix, contract, preferred_element_type=jnp.float32)
    return (query_grad.reshape(tgt_rows, HEADS * HEAD), encoded_grad)

def reference(enc_hidden, mlp_gain, final_gain, w_gate, w_up, w_down, key_weight, value_weight, queries, context_grad):
    hidden_wide = enc_hidden.astype(jnp.float32)
    inv_in = lax.rsqrt(lax.optimization_barrier(jnp.mean(hidden_wide * hidden_wide, axis=1, keepdims=True)) + EPSILON)
    normed = (hidden_wide * inv_in * mlp_gain[None, :]).astype(jnp.bfloat16)
    gate_pre = jnp.dot(normed, w_gate, preferred_element_type=jnp.float32)
    up_pre = jnp.dot(normed, w_up, preferred_element_type=jnp.float32)
    sigmoid_gate = jax.nn.sigmoid(gate_pre)
    activated = gate_pre * sigmoid_gate
    hidden_act = (activated * up_pre).astype(jnp.bfloat16)
    outer = hidden_wide + jnp.dot(hidden_act, w_down, preferred_element_type=jnp.float32)
    inv_out = lax.rsqrt(lax.optimization_barrier(jnp.mean(outer * outer, axis=1, keepdims=True)) + EPSILON)
    encoded = (outer * inv_out * final_gain[None, :]).astype(jnp.bfloat16)

    def one_layer(inputs):
        return layer_pass(encoded, inputs[0], inputs[1], inputs[2], inputs[3])
    query_grad, layer_grads = lax.map(one_layer, (key_weight, value_weight, queries, context_grad))
    encoded_grad = lax.optimization_barrier(jnp.sum(layer_grads, axis=0))
    scaled_out = final_gain[None, :] * encoded_grad
    inner_out = lax.optimization_barrier(jnp.mean(scaled_out * outer, axis=1, keepdims=True))
    outer_grad = inv_out * scaled_out - outer * inv_out * inv_out * inv_out * inner_out
    outer_grad_bf = outer_grad.astype(jnp.bfloat16)
    rows_contract = (((0,), (0,)), ((), ()))
    down_weight_grad = lax.dot_general(hidden_act, outer_grad_bf, rows_contract, preferred_element_type=jnp.float32).astype(jnp.bfloat16)
    cols_contract = (((1,), (1,)), ((), ()))
    act_grad = lax.dot_general(outer_grad_bf, w_down, cols_contract, preferred_element_type=jnp.float32)
    up_grad = (act_grad * activated).astype(jnp.bfloat16)
    gate_grad = (act_grad * up_pre * sigmoid_gate * (1.0 + gate_pre * (1.0 - sigmoid_gate))).astype(jnp.bfloat16)
    gate_weight_grad = lax.dot_general(normed, gate_grad, rows_contract, preferred_element_type=jnp.float32).astype(jnp.bfloat16)
    up_weight_grad = lax.dot_general(normed, up_grad, rows_contract, preferred_element_type=jnp.float32).astype(jnp.bfloat16)
    normed_grad = lax.dot_general(gate_grad, w_gate, cols_contract, preferred_element_type=jnp.float32)
    normed_grad = normed_grad + lax.dot_general(up_grad, w_up, cols_contract, preferred_element_type=jnp.float32)
    scaled_in = mlp_gain[None, :] * normed_grad
    inner_in = lax.optimization_barrier(jnp.mean(scaled_in * hidden_wide, axis=1, keepdims=True))
    hidden_grad = outer_grad + inv_in * scaled_in - hidden_wide * inv_in * inv_in * inv_in * inner_in
    return (query_grad, hidden_grad, gate_weight_grad, up_weight_grad, down_weight_grad)
```

```python
import contextlib
import functools
import jax
import jax.numpy as jnp
from jax import lax
from jax.experimental import pallas as pl
from jax.experimental.pallas import tpu as pltpu
from jax.sharding import PartitionSpec as P

HEAD = 256
EPSILON = 1e-06
LANES = 128
MESH = pl.DeviceIdType.MESH
VMEM_LIMIT = 58 * 1024 * 1024
CHAIN_VMEM_LIMIT = 54 * 1024 * 1024
WRITE_VMEM_LIMIT = 4 * 1024 * 1024
ROWS = (((0,), (0,)), ((), ()))
COLS = (((1,), (1,)), ((), ()))
F32 = jnp.float32
BF16 = jnp.bfloat16


def mark(name):
    return contextlib.nullcontext()


def enter(sizes):
    barrier = pltpu.get_barrier_semaphore()
    for axis, n in sizes:
        me = lax.axis_index(axis)
        for k in range(1, n):
            pl.semaphore_signal(
                barrier, inc=1, device_id={axis: lax.rem(me + k, n)}, device_id_type=MESH
            )
    pl.semaphore_wait(barrier, sum(n - 1 for _, n in sizes))


def post(axis, n, source, target, send_sem, recv_sem):
    me = lax.axis_index(axis)
    copies = []
    for k in range(1, n):
        peer = lax.rem(me + k, n)
        copy = pltpu.make_async_remote_copy(
            src_ref=source(peer),
            dst_ref=target(k - 1),
            send_sem=send_sem.at[k - 1],
            recv_sem=recv_sem.at[k - 1],
            device_id={axis: peer},
            device_id_type=MESH,
        )
        copy.start()
        copies.append(copy)
    return copies


def gather(axis, n, ref, send_sem, recv_sem):
    me = lax.axis_index(axis)
    return post(axis, n, lambda peer: ref.at[me], lambda k: ref.at[me], send_sem, recv_sem)


def scatter(axis, n, out, into, send_sem, recv_sem):
    return post(axis, n, lambda peer: out.at[peer], lambda k: into.at[k], send_sem, recv_sem)


def finish(*groups):
    for copies in groups:
        for copy in copies:
            copy.wait()


def total(own, into, n):
    acc = own.astype(F32)
    for k in range(n - 1):
        acc = acc + into[k].astype(F32)
    return acc


def attend(keys, values, q, c):
    scale = HEAD ** (-0.5)
    scores = lax.dot_general(keys, q, COLS, preferred_element_type=F32) * scale
    weights = jnp.exp(scores - jnp.max(scores, axis=0, keepdims=True))
    probs = weights / jnp.sum(weights, axis=0, keepdims=True)
    probs_bf = probs.astype(BF16)
    dprob = lax.dot_general(values, c, COLS, preferred_element_type=F32)
    delta = jnp.sum(probs_bf.astype(F32) * dprob, axis=0, keepdims=True)
    dscore = (probs * (dprob - delta) * scale).astype(BF16)
    query_grad = lax.dot_general(dscore, keys, ROWS, preferred_element_type=F32).astype(BF16)
    key_grad = jnp.dot(dscore, q, preferred_element_type=F32).astype(BF16)
    value_grad = jnp.dot(probs_bf, c, preferred_element_type=F32).astype(BF16)
    return query_grad, key_grad, value_grad


def step_kernel(
    S, N, x_ref, mg_ref, fg_ref, wg_hbm, wu_hbm, wd_hbm, wk_hbm, wv_hbm, q_hbm, c_hbm,
    qg_hbm, hg_out, normed_out, hid_out, oall_out, gate_out, up_out,
    wg, wu, wd, wk, wv, q, c, qg,
    xg, sqs, sqr, gus, gur, hid_all, inv_all, ds, dr, feat, sqo, enc, af, eg,
    r6, s6, r6b, pin, oall, s9, r9, aall, s11, r11, pin2,
    load_sem, store_sem, ssem, rsem,
):
    tt, F = x_ref.shape
    T = N * tt
    ts = T // S
    H = wg.shape[1]
    D = F * S
    heads = q.shape[1] // HEAD
    sec = lax.axis_index("section")
    ten = lax.axis_index("tensor")
    loads = [
        pltpu.make_async_copy(src, dst, load_sem.at[i])
        for i, (src, dst) in enumerate((
            (wg_hbm, wg), (wu_hbm, wu), (wd_hbm, wd), (wk_hbm, wk), (wv_hbm, wv),
            (q_hbm, q), (c_hbm, c),
        ))
    ]
    for load in loads[:3]:
        load.start()
    xg[ten] = x_ref[...]
    enter((("section", S), ("tensor", N)))
    finish(post("tensor", N, lambda p: x_ref, lambda k: xg.at[ten], ssem.at[0], rsem.at[0]))
    wide = xg[...].reshape(T, F).astype(F32)
    scaled = (wide * mg_ref[...]).astype(BF16)
    square = jnp.sum(wide * wide, axis=1, keepdims=True)
    sqs[...] = jnp.broadcast_to(square, (T, LANES)).reshape(S, ts, LANES)
    loads[0].wait()
    gus[0] = jnp.dot(scaled, wg[...], preferred_element_type=F32).astype(BF16).reshape(S, ts, H)
    move_q = scatter("section", S, sqs, sqr, ssem.at[3], rsem.at[3])
    move_g = scatter("section", S, gus.at[0], gur.at[0], ssem.at[1], rsem.at[1])
    loads[1].wait()
    gus[1] = jnp.dot(scaled, wu[...], preferred_element_type=F32).astype(BF16).reshape(S, ts, H)
    move_u = scatter("section", S, gus.at[1], gur.at[1], ssem.at[2], rsem.at[2])
    for load in loads[3:]:
        load.start()
    finish(move_q, move_g)
    inv = lax.rsqrt(total(sqs[sec], sqr, S) / D + EPSILON)
    inv_all[sec] = inv
    inv = inv[:, :1]
    gate_pre = total(gus[0, sec], gur.at[0], S) * inv
    sig = jax.nn.sigmoid(gate_pre)
    act = gate_pre * sig
    af[0, sec] = act.astype(BF16)
    slope = sig * (1.0 + gate_pre * (1.0 - sig))
    finish(move_u)
    up_pre = total(gus[1, sec], gur.at[1], S) * inv
    hid_all[sec] = (act * up_pre).astype(BF16)
    move_h = gather("section", S, hid_all, ssem.at[4], rsem.at[4])
    move_i = gather("section", S, inv_all, ssem.at[5], rsem.at[5])
    af[1, sec] = (up_pre * slope).astype(BF16)
    loads[2].wait()
    finish(move_h)
    hid = hid_all[...].reshape(T, H)
    ds[...] = jnp.dot(hid, wd[...], preferred_element_type=F32).astype(BF16).reshape(N, tt, F)
    move_d = scatter("tensor", N, ds, dr, ssem.at[6], rsem.at[6])
    hid_out[...] = hid
    finish(move_i)
    inv_tok = inv_all[...].reshape(T, LANES)
    normed_out[...] = (wide * inv_tok[:, :1] * mg_ref[...]).astype(BF16)
    finish(move_d)
    outer = x_ref[...].astype(F32) + total(ds[ten], dr, N)
    feat[sec] = (outer * fg_ref[...]).astype(BF16)
    sqo[sec] = jnp.broadcast_to(jnp.sum(outer * outer, axis=1, keepdims=True), (tt, LANES))
    move_s = gather("section", S, sqo, ssem.at[8], rsem.at[8])
    move_f = gather("section", S, feat, ssem.at[7], rsem.at[7])
    finish(move_s, move_f)
    move_act = gather("section", S, af.at[0], ssem.at[10], rsem.at[10])
    move_fac = gather("section", S, af.at[1], ssem.at[11], rsem.at[11])
    inv_o = lax.rsqrt(jnp.sum(sqo[...], axis=0) / D + EPSILON)
    enc[ten] = (feat[...].astype(F32) * inv_o[None, :, :1]).astype(BF16)
    inv_o = inv_o[:, :1]
    move_e = gather("tensor", N, enc, ssem.at[9], rsem.at[9])
    for load in loads[3:]:
        load.wait()
    finish(move_e)

    width = heads * HEAD
    keys = jnp.zeros((T, width), F32)
    values = jnp.zeros((T, width), F32)
    for s in range(S):
        block = enc[:, s].reshape(T, F)
        keys += jnp.dot(block, wk[s * F : (s + 1) * F, :], preferred_element_type=F32)
        values += jnp.dot(block, wv[s * F : (s + 1) * F, :], preferred_element_type=F32)
    keys = keys.astype(BF16)
    values = values.astype(BF16)
    key_grads, value_grads, stores = [], [], []
    for h in range(heads):
        cols = slice(h * HEAD, (h + 1) * HEAD)
        query_grad, key_grad, value_grad = attend(
            keys[:, cols], values[:, cols], q[:, cols], c[:, cols]
        )
        qg[h] = query_grad
        store = pltpu.make_async_copy(qg.at[h], qg_hbm.at[:, cols], store_sem.at[h])
        store.start()
        stores.append(store)
        key_grads.append(key_grad)
        value_grads.append(value_grad)
    key_grad = jnp.concatenate(key_grads, axis=1)
    value_grad = jnp.concatenate(value_grads, axis=1)
    for s in range(S):
        rows = slice(s * F, (s + 1) * F)
        part = lax.dot_general(key_grad, wk[rows, :], COLS, preferred_element_type=F32)
        part += lax.dot_general(value_grad, wv[rows, :], COLS, preferred_element_type=F32)
        eg[:, s] = part.astype(BF16).reshape(N, tt, F)

    finish(scatter("tensor", N, eg, r6, ssem.at[12], rsem.at[12]))
    s6[...] = total(eg[ten], r6, N).astype(BF16)
    finish(scatter("section", S, s6, r6b, ssem.at[13], rsem.at[13]))
    scaled_out = fg_ref[...] * total(s6[sec], r6b, S)
    pin[sec] = jnp.broadcast_to(
        jnp.sum(scaled_out * outer, axis=1, keepdims=True), (tt, LANES)
    )
    finish(gather("section", S, pin, ssem.at[14], rsem.at[14]))
    inner = jnp.sum(pin[...], axis=0)[:, :1] / D
    outer_grad = inv_o * scaled_out - outer * (inv_o * inv_o * inv_o * inner)
    oall[ten] = outer_grad.astype(BF16)
    finish(gather("tensor", N, oall, ssem.at[15], rsem.at[15]))
    grads = oall[...].reshape(T, F)
    half = H // 2
    moves = []
    for i in range(2):
        s9[i] = (
            lax.dot_general(
                grads, wd[i * half : (i + 1) * half, :], COLS, preferred_element_type=F32
            )
            .astype(BF16)
            .reshape(S, ts, half)
        )
        moves.append(scatter("section", S, s9.at[i], r9.at[i], ssem.at[16 + i], rsem.at[16 + i]))
    oall_out[...] = grads
    finish(move_act, move_fac)
    gathers = []
    for i in range(2):
        finish(moves[i])
        aall[i, sec] = total(s9[i, sec], r9.at[i], S).astype(BF16)
        gathers.append(gather("section", S, aall.at[i], ssem.at[18 + i], rsem.at[18 + i]))
    parts = None
    for i in range(2):
        cols = slice(i * half, (i + 1) * half)
        finish(gathers[i])
        act_grad = aall[i].reshape(T, half).astype(F32)
        up_grad = (act_grad * af[0, :, :, cols].reshape(T, half).astype(F32)).astype(BF16)
        gate_grad = (act_grad * af[1, :, :, cols].reshape(T, half).astype(F32)).astype(BF16)
        up_out[:, cols] = up_grad
        gate_out[:, cols] = gate_grad
        part = lax.dot_general(gate_grad, wg[:, cols], COLS, preferred_element_type=F32)
        part += lax.dot_general(up_grad, wu[:, cols], COLS, preferred_element_type=F32)
        parts = part if parts is None else parts + part
    s11[...] = parts.astype(BF16).reshape(N, tt, F)
    finish(scatter("tensor", N, s11, r11, ssem.at[20], rsem.at[20]))
    hidden = x_ref[...].astype(F32)
    scaled_in = mg_ref[...] * total(s11[ten], r11, N)
    pin2[sec] = jnp.broadcast_to(
        jnp.sum(scaled_in * hidden, axis=1, keepdims=True), (tt, LANES)
    )
    finish(gather("section", S, pin2, ssem.at[21], rsem.at[21]))
    inner_in = jnp.sum(pin2[...], axis=0)[:, :1] / D
    inv_flat = inv_all.reshape(T, LANES)
    inv_in = inv_flat[pl.ds(pl.multiple_of(ten * tt, tt), tt), :][:, :1]
    hg_out[...] = (
        outer_grad + inv_in * scaled_in - hidden * (inv_in * inv_in * inv_in * inner_in)
    )
    for store in stores:
        store.wait()


def general(
    S, N, enc_hidden, mlp_gain, final_gain, w_gate, w_up, w_down, key_weight, value_weight,
    queries, context_grad,
):
    tt, F = enc_hidden.shape
    T = N * tt
    ts = T // S
    H = w_gate.shape[1]
    peers = max(S, N) - 1
    vmem = pl.BlockSpec(memory_space=pltpu.VMEM)
    hbm = pl.BlockSpec(memory_space=pl.ANY)
    shape = jax.ShapeDtypeStruct
    dma = pltpu.SemaphoreType.DMA
    wk, wv, q, c = key_weight[0], value_weight[0], queries[0], context_grad[0]
    large = (w_gate, w_up, w_down, wk, wv, q, c)
    rows = q.shape[0]
    heads = q.shape[1] // HEAD
    scratch = [pltpu.VMEM(w.shape, BF16) for w in large]
    scratch += [
        pltpu.VMEM((heads, rows, HEAD), BF16),
        pltpu.VMEM((N, tt, F), BF16),
        pltpu.VMEM((S, ts, LANES), F32),
        pltpu.VMEM((S - 1, ts, LANES), F32),
        pltpu.VMEM((2, S, ts, H), BF16),
        pltpu.VMEM((2, S - 1, ts, H), BF16),
        pltpu.VMEM((S, ts, H), BF16),
        pltpu.VMEM((S, ts, LANES), F32),
        pltpu.VMEM((N, tt, F), BF16),
        pltpu.VMEM((N - 1, tt, F), BF16),
        pltpu.VMEM((S, tt, F), BF16),
        pltpu.VMEM((S, tt, LANES), F32),
        pltpu.VMEM((N, S, tt, F), BF16),
        pltpu.VMEM((2, S, ts, H), BF16),
        pltpu.VMEM((N, S, tt, F), BF16),
        pltpu.VMEM((N - 1, S, tt, F), BF16),
        pltpu.VMEM((S, tt, F), BF16),
        pltpu.VMEM((S - 1, tt, F), BF16),
        pltpu.VMEM((S, tt, LANES), F32),
        pltpu.VMEM((N, tt, F), BF16),
        pltpu.VMEM((2, S, ts, H // 2), BF16),
        pltpu.VMEM((2, S - 1, ts, H // 2), BF16),
        pltpu.VMEM((2, S, ts, H // 2), BF16),
        pltpu.VMEM((N, tt, F), BF16),
        pltpu.VMEM((N - 1, tt, F), BF16),
        pltpu.VMEM((S, tt, LANES), F32),
        dma((7,)), dma((heads,)), dma((22, peers)), dma((22, peers)),
    ]
    query_grad, hidden_grad, normed, hid, outer_all, gate_all, up_all = pl.pallas_call(
        functools.partial(step_kernel, S, N),
        out_shape=[
            shape(q.shape, BF16), shape((tt, F), F32), shape((T, F), BF16),
            shape((T, H), BF16), shape((T, F), BF16), shape((T, H), BF16), shape((T, H), BF16),
        ],
        in_specs=[vmem] * 3 + [hbm] * 7,
        out_specs=[hbm] + [vmem] * 6,
        scratch_shapes=scratch,
        compiler_params=pltpu.CompilerParams(
            collective_id=0, has_side_effects=True, vmem_limit_bytes=VMEM_LIMIT
        ),
    )(enc_hidden, mlp_gain[None, :], final_gain[None, :], *large)

    outer_product = lambda a, b: lax.dot_general(
        a, b, ROWS, preferred_element_type=F32
    ).astype(BF16)
    return (
        query_grad[None, :, :],
        hidden_grad,
        outer_product(normed, gate_all),
        outer_product(normed, up_all),
        outer_product(hid, outer_all),
    )


def far_first(n):
    return sorted(range(1, n), key=lambda k: abs(2 * k - n))


def near_first(n):
    return far_first(n)[::-1]


def lane_of_row(rows, offset):
    row = lax.broadcasted_iota(jnp.int32, (rows, LANES), 0) + offset
    return (row == lax.broadcasted_iota(jnp.int32, (rows, LANES), 1)).astype(F32)


def to_row(column, offset):
    return jnp.sum(column * lane_of_row(column.shape[0], offset), axis=0, keepdims=True)


def to_column(row, rows, offset):
    return jnp.sum(row * lane_of_row(rows, offset), axis=1, keepdims=True)


def exchange(axis, n, k, source, target, send_sem, recv_sem):
    peer = lax.rem(lax.axis_index(axis) + k, n)
    copy = pltpu.make_async_remote_copy(
        src_ref=source(peer),
        dst_ref=target,
        send_sem=send_sem.at[k - 1],
        recv_sem=recv_sem.at[k - 1],
        device_id={axis: peer},
        device_id_type=MESH,
    )
    copy.start()
    return copy


def everyone(S, N, sections, source, target, send_sem, recv_sem):
    sec = lax.axis_index("section")
    ten = lax.axis_index("tensor")
    copies = {}
    for k in sections:
        for j in range(N):
            if k == 0 and j == 0:
                continue
            s = lax.rem(sec + k, S)
            n = lax.rem(ten + j, N)
            copy = pltpu.make_async_remote_copy(
                src_ref=source(s, n),
                dst_ref=target,
                send_sem=send_sem.at[k * N + j],
                recv_sem=recv_sem.at[k * N + j],
                device_id={"section": s, "tensor": n},
                device_id_type=MESH,
            )
            copy.start()
            copies[k, j] = copy
    return copies


def product(a, b):
    return lax.dot_general(a, b, ROWS, preferred_element_type=F32).astype(BF16)


def chain_kernel(
    S, N, x_hbm, mg_hbm, fg_hbm, wg_hbm, wu_hbm, wd_hbm, wk_hbm, wv_hbm, q_hbm, c_hbm,
    hg_out, qg_out, gw_out, uw_out, dw_out,
    mg, fg, wg, wu, wd, wk, wv, q, c,
    xg, sqr, gus, gur, hid, af, comb, ds, dsb, dr, encb, sso, egb, er, ror, oall,
    s9, r9, aall, rir, gate, up, s11, s11b, r11, rit, rits, dsc,
    load_sem, ssem, rsem, fsem, sall, rall,
):
    tt, F = x_hbm.shape
    T = N * tt
    H = wg.shape[1]
    Hs = H // S
    D = F * S
    heads = q.shape[1] // HEAD
    width = heads * HEAD
    sec = lax.axis_index("section")
    ten = lax.axis_index("tensor")
    sent = []

    def units(p):
        return pl.ds(pl.multiple_of(p * Hs, LANES), Hs)

    def source_of(k):
        return lax.rem(sec + S - k, S)

    def share_factor(i, half):
        part = af.at[i, sec, pl.ds(half * (T // 2), T // 2)]
        lane = 2 * i + half
        return [
            exchange("section", S, k, lambda p: part, part, fsem.at[0, lane], fsem.at[1, lane])
            for k in far_first(S)
        ]

    barrier = pltpu.get_barrier_semaphore()
    for axis, n in (("section", S), ("tensor", N)):
        me = lax.axis_index(axis)
        for k in range(1, n):
            pl.semaphore_signal(
                barrier, inc=1, device_id={axis: lax.rem(me + k, n)}, device_id_type=MESH
            )
    for k in range(1, S):
        for j in range(1, N):
            pl.semaphore_signal(
                barrier,
                inc=1,
                device_id={"section": lax.rem(sec + k, S), "tensor": lax.rem(ten + j, N)},
                device_id_type=MESH,
            )
    loads = [
        pltpu.make_async_copy(src, dst, load_sem.at[i])
        for i, (src, dst) in enumerate((
            (x_hbm, xg.at[ten]), (mg_hbm, mg), (fg_hbm, fg),
            (wg_hbm, wg), (wu_hbm, wu), (wd_hbm, wd), (wk_hbm, wk), (wv_hbm, wv),
            (q_hbm, q), (c_hbm, c),
        ))
    ]
    for load in loads[:6]:
        load.start()
    loads[0].wait()
    with mark("enter"):
        pl.semaphore_wait(barrier, S * N - 1)
    moves = [
        exchange("tensor", N, k, lambda p: xg.at[ten], xg.at[ten], ssem.at[0], rsem.at[0])
        for k in far_first(N)
    ]
    for load in loads[1:5]:
        load.wait()
    with mark("x"):
        for move in moves:
            move.wait_recv()
    sent += moves

    wide = xg[...].reshape(T, F).astype(F32)
    scaled = (wide * mg[...]).astype(BF16)
    square = jnp.sum(wide * wide, axis=1, keepdims=True)
    sqr[sec] = to_row(square, 0)
    move_q = [
        exchange("section", S, k, lambda p: sqr.at[sec], sqr.at[sec], ssem.at[1], rsem.at[1])
        for k in far_first(S)
    ]
    move_g, move_u = {}, {}
    for k in far_first(S):
        p = lax.rem(sec + k, S)
        gus[0, p] = jnp.dot(scaled, wg[:, units(p)], preferred_element_type=F32).astype(BF16)
        move_g[k] = exchange(
            "section", S, k, lambda p: gus.at[0, p], gur.at[0, k - 1], ssem.at[2], rsem.at[2]
        )
        gus[1, p] = jnp.dot(scaled, wu[:, units(p)], preferred_element_type=F32).astype(BF16)
        move_u[k] = exchange(
            "section", S, k, lambda p: gus.at[1, p], gur.at[1, k - 1], ssem.at[3], rsem.at[3]
        )
    for load in loads[6:]:
        load.start()
    gate_pre = jnp.dot(scaled, wg[:, units(sec)], preferred_element_type=F32)
    up_pre = jnp.dot(scaled, wu[:, units(sec)], preferred_element_type=F32)
    with mark("sq"):
        for move in move_q:
            move.wait_recv()
    sent += move_q
    inv = lax.rsqrt(to_column(jnp.sum(sqr[...], axis=0), T, 0) / D + EPSILON)
    normed = (wide * inv * mg[...]).astype(BF16)
    loads[5].wait()
    for k in near_first(S):
        with mark(f"gu{k}"):
            move_g[k].wait_recv()
            move_u[k].wait_recv()
        gate_pre = gate_pre + gur[0, k - 1].astype(F32)
        up_pre = up_pre + gur[1, k - 1].astype(F32)
        sent += [move_g[k], move_u[k]]
    gate_pre = gate_pre * inv
    up_pre = up_pre * inv
    sig = jax.nn.sigmoid(gate_pre)
    act = gate_pre * sig
    hid[sec] = (act * up_pre).astype(BF16)
    move_h = {
        k: exchange("section", S, k, lambda p: hid.at[sec], hid.at[sec], ssem.at[4], rsem.at[4])
        for k in far_first(S)
    }
    factor = up_pre * (sig * (1.0 + gate_pre * (1.0 - sig)))
    af[0, sec] = act.astype(BF16)
    af[1, sec] = factor.astype(BF16)
    comb[...] = act * up_pre + factor * gate_pre
    down = jnp.dot(hid[sec], wd[units(sec), :], preferred_element_type=F32)
    for k in near_first(S):
        with mark(f"hid{k}"):
            move_h[k].wait_recv()
        p = source_of(k)
        down = down + jnp.dot(hid[p], wd[units(p), :], preferred_element_type=F32)
        sent.append(move_h[k])
    ds[...] = down.reshape(N, tt, F)
    dsb[...] = down.astype(BF16).reshape(N, tt, F)
    moves = [
        exchange("tensor", N, k, lambda p: dsb.at[p], dr.at[k - 1], ssem.at[5], rsem.at[5])
        for k in far_first(N)
    ]
    move_a = share_factor(0, 0)
    with mark("ds"):
        for move in moves:
            move.wait_recv()
    sent += moves
    outer = xg[ten].astype(F32) + total(ds[ten], dr, N)
    sso[sec, ten] = to_row(jnp.sum(outer * outer, axis=1, keepdims=True), ten * tt)
    encb[sec, ten] = (outer * fg[...]).astype(BF16)
    order = [0] + near_first(S)
    move_s = everyone(
        S, N, order, lambda s, n: sso.at[sec, ten], sso.at[sec, ten], sall.at[1], rall.at[1]
    )
    move_e = {}

    def send_block(block, axis, peer, k, j):
        move_e[k, j] = pltpu.make_async_remote_copy(
            src_ref=block,
            dst_ref=block,
            send_sem=sall.at[0, k * N + j],
            recv_sem=rall.at[0, k * N + j],
            device_id={axis: peer},
            device_id_type=MESH,
        )
        move_e[k, j].start()

    for k in far_first(S):
        send_block(encb.at[sec, ten], "section", lax.rem(sec + k, S), k, 0)
    for j in far_first(N):
        send_block(encb.at[sec, ten], "tensor", lax.rem(ten + j, N), 0, j)
    move_a += share_factor(0, 1) + share_factor(1, 0) + share_factor(1, 1)
    for k in order[1:]:
        with mark(f"pass{k}"):
            move_e[k, 0].wait_recv()
        for j in far_first(N):
            send_block(encb.at[source_of(k), ten], "tensor", lax.rem(ten + j, N), k, j)
    sent += list(move_e.values()) + list(move_s.values())
    for load in loads[6:]:
        load.wait()
    keys = values = None
    for k in order:
        with mark(f"enc{k}"):
            for j in range(1, N):
                move_e[k, j].wait_recv()
        p = source_of(k)
        block = encb[p].reshape(T, F)
        rows = pl.ds(pl.multiple_of(p * F, F), F)
        key_part = jnp.dot(block, wk[rows, :], preferred_element_type=F32)
        value_part = jnp.dot(block, wv[rows, :], preferred_element_type=F32)
        keys = key_part if keys is None else keys + key_part
        values = value_part if values is None else values + value_part
    with mark("sso"):
        for move in move_s.values():
            move.wait_recv()
    squares = jnp.sum(sso[...].reshape(S * N, 1, LANES), axis=0)
    inv_all = lax.rsqrt(to_column(squares, T, 0) / D + EPSILON)
    inv_o = lax.rsqrt(to_column(squares, tt, ten * tt) / D + EPSILON)
    keys = (keys * inv_all).astype(BF16)
    values = (values * inv_all).astype(BF16)
    scale = HEAD ** (-0.5)
    key_grads, value_grads = [], []
    inner = None
    for h in range(heads):
        cols = slice(h * HEAD, (h + 1) * HEAD)
        scores = lax.dot_general(keys[:, cols], q[:, cols], COLS, preferred_element_type=F32)
        scores = scores * scale
        weights = jnp.exp(scores - jnp.max(scores, axis=0, keepdims=True))
        probs = weights / jnp.sum(weights, axis=0, keepdims=True)
        probs_bf = probs.astype(BF16)
        dprob = lax.dot_general(values[:, cols], c[:, cols], COLS, preferred_element_type=F32)
        delta = jnp.sum(probs_bf.astype(F32) * dprob, axis=0, keepdims=True)
        dscore = (probs * (dprob - delta) * scale).astype(BF16)
        dsc[h] = dscore
        key_grad = jnp.dot(dscore, q[:, cols], preferred_element_type=F32).astype(BF16)
        value_grad = jnp.dot(probs_bf, c[:, cols], preferred_element_type=F32).astype(BF16)
        part = key_grad.astype(F32) * keys[:, cols].astype(F32)
        part += value_grad.astype(F32) * values[:, cols].astype(F32)
        inner = part if inner is None else inner + part
        key_grads.append(key_grad)
        value_grads.append(value_grad)
    key_grad = jnp.concatenate(key_grads, axis=1)
    value_grad = jnp.concatenate(value_grads, axis=1)
    ror[sec, ten] = to_row(jnp.sum(inner, axis=1, keepdims=True), 0)
    move_r = everyone(
        S, N, far_first(S) + [0], lambda s, n: ror.at[sec, ten], ror.at[sec, ten],
        sall.at[2], rall.at[2],
    )
    move_g = {}
    for k in far_first(S) + [0]:
        p = lax.rem(sec + k, S)
        rows = pl.ds(pl.multiple_of(p * F, F), F)
        part = lax.dot_general(key_grad, wk[rows, :], COLS, preferred_element_type=F32)
        part += lax.dot_general(value_grad, wv[rows, :], COLS, preferred_element_type=F32)
        egb[p] = part.astype(BF16).reshape(N, tt, F)
        move_g.update(everyone(
            S, N, [k], lambda s, n: egb.at[s, n], er.at[sec, ten], sall.at[3], rall.at[3]
        ))
    er[sec, ten] = egb[sec, ten]
    for h in range(heads):
        cols = slice(h * HEAD, (h + 1) * HEAD)
        qg_out[:, cols] = product(dsc[h], keys[:, cols])
    sent += list(move_g.values()) + list(move_r.values())
    with mark("eg"):
        for move in move_r.values():
            move.wait_recv()
        for move in move_g.values():
            move.wait_recv()
    inner = to_column(jnp.sum(ror[...].reshape(S * N, 1, LANES), axis=0), tt, ten * tt)
    grad = jnp.sum(er[...].reshape(S * N, tt, F).astype(F32), axis=0)
    outer_grad = inv_o * (fg[...] * grad) - outer * (inv_o * inv_o * inner / D)
    oall[ten] = outer_grad.astype(BF16)
    moves = [
        exchange("tensor", N, k, lambda p: oall.at[ten], oall.at[ten], ssem.at[8], rsem.at[8])
        for k in far_first(N)
    ]
    with mark("oall"):
        for move in moves:
            move.wait_recv()
    sent += moves
    grads = oall[...].reshape(T, F)
    move_9 = {}
    for k in far_first(S):
        p = lax.rem(sec + k, S)
        s9[p] = lax.dot_general(
            grads, wd[units(p), :], COLS, preferred_element_type=F32
        ).astype(BF16)
        move_9[k] = exchange(
            "section", S, k, lambda p: s9.at[p], r9.at[k - 1], ssem.at[9], rsem.at[9]
        )
    act_grad = lax.dot_general(grads, wd[units(sec), :], COLS, preferred_element_type=F32)
    for s in range(S):
        dw_out[s * Hs : (s + 1) * Hs, :] = product(hid[s], grads)
    for k in near_first(S):
        with mark(f"s9_{k}"):
            move_9[k].wait_recv()
        act_grad = act_grad + r9[k - 1].astype(F32)
        sent.append(move_9[k])
    aall[sec] = act_grad.astype(BF16)
    move_g = {
        k: exchange("section", S, k, lambda p: aall.at[sec], aall.at[sec], ssem.at[10], rsem.at[10])
        for k in far_first(S)
    }
    rir[sec] = to_row(jnp.sum(act_grad * comb[...], axis=1, keepdims=True), 0)
    move_r = [
        exchange("section", S, k, lambda p: rir.at[sec], rir.at[sec], ssem.at[11], rsem.at[11])
        for k in far_first(S)
    ]
    with mark("af"):
        for move in move_a:
            move.wait_recv()
    sent += move_a + move_r
    part = None
    for k in [0] + near_first(S):
        p = source_of(k)
        if k:
            with mark(f"aall{k}"):
                move_g[k].wait_recv()
            sent.append(move_g[k])
        act_grad = aall[p].astype(F32)
        up_grad = (act_grad * af[0, p].astype(F32)).astype(BF16)
        gate_grad = (act_grad * af[1, p].astype(F32)).astype(BF16)
        up[p] = up_grad
        gate[p] = gate_grad
        more = lax.dot_general(gate_grad, wg[:, units(p)], COLS, preferred_element_type=F32)
        more += lax.dot_general(up_grad, wu[:, units(p)], COLS, preferred_element_type=F32)
        part = more if part is None else part + more
    for move in move_r:
        move.wait_recv()
    s11[...] = part.reshape(N, tt, F)
    s11b[...] = part.astype(BF16).reshape(N, tt, F)
    moves = [
        exchange("tensor", N, k, lambda p: s11b.at[p], r11.at[k - 1], ssem.at[12], rsem.at[12])
        for k in far_first(N)
    ]
    rits[...] = jnp.sum(rir[...], axis=0)
    more_moves = [
        exchange("tensor", N, k, lambda p: rits, rit.at[k - 1], ssem.at[13], rsem.at[13])
        for k in far_first(N)
    ]
    for s in range(S):
        cols = slice(s * Hs, (s + 1) * Hs)
        gw_out[:, cols] = product(normed, gate[s])
        uw_out[:, cols] = product(normed, up[s])
    with mark("s11"):
        for move in moves + more_moves:
            move.wait_recv()
    sent += moves + more_moves
    hidden = xg[ten].astype(F32)
    scaled_in = mg[...] * total(s11[ten], r11, N)
    inner = to_column(total(rits[...], rit, N), tt, ten * tt)
    squares = to_column(jnp.sum(sqr[...], axis=0), tt, ten * tt)
    inv_in = lax.rsqrt(squares / D + EPSILON)
    hg_out[...] = outer_grad + inv_in * scaled_in - hidden * (inv_in * inv_in * inner / D)
    with mark("end"):
        for move in sent:
            move.wait_send()


def write_kernel(*refs):
    count = len(refs) // 2
    sem = refs[-1]
    copies = [
        pltpu.make_async_copy(refs[i], refs[count + i], sem.at[i]) for i in range(count)
    ]
    for copy in copies:
        copy.start()
    for copy in copies:
        copy.wait()


def fast(
    S, N, enc_hidden, mlp_gain, final_gain, w_gate, w_up, w_down, key_weight, value_weight,
    queries, context_grad,
):
    tt, F = enc_hidden.shape
    T = N * tt
    H = w_gate.shape[1]
    Hs = H // S
    vmem = pl.BlockSpec(memory_space=pltpu.VMEM)
    hbm = pl.BlockSpec(memory_space=pltpu.HBM)
    shape = jax.ShapeDtypeStruct
    dma = pltpu.SemaphoreType.DMA
    wk, wv, q, c = key_weight[0], value_weight[0], queries[0], context_grad[0]
    rows, width = q.shape
    heads = width // HEAD
    buf = lambda *dims: pltpu.VMEM(dims, BF16)
    wide = lambda *dims: pltpu.VMEM(dims, F32)
    scratch = [
        wide(1, F), wide(1, F), buf(F, H), buf(F, H), buf(H, F), buf(*wk.shape), buf(*wv.shape),
        buf(rows, width), buf(rows, width),
        buf(N, tt, F),
        wide(S, 1, LANES),
        buf(2, S, T, Hs),
        buf(2, S - 1, T, Hs),
        buf(S, T, Hs),
        buf(2, S, T, Hs),
        wide(T, Hs),
        wide(N, tt, F),
        buf(N, tt, F),
        buf(N - 1, tt, F),
        buf(S, N, tt, F),
        wide(S, N, 1, LANES),
        buf(S, N, tt, F),
        buf(S, N, tt, F),
        wide(S, N, 1, LANES),
        buf(N, tt, F),
        buf(S, T, Hs),
        buf(S - 1, T, Hs),
        buf(S, T, Hs),
        wide(S, 1, LANES),
        buf(S, T, Hs),
        buf(S, T, Hs),
        wide(N, tt, F),
        buf(N, tt, F),
        buf(N - 1, tt, F),
        wide(N - 1, 1, LANES),
        wide(1, LANES),
        buf(heads, T, rows),
        dma((10,)), dma((14, max(S, N) - 1)), dma((14, max(S, N) - 1)),
        dma((2, 4, S - 1)), dma((4, S * N)), dma((4, S * N)),
    ]
    results = [
        ((tt, F), F32), ((rows, width), BF16), ((F, H), BF16), ((F, H), BF16), ((H, F), BF16)
    ]
    made = pl.pallas_call(
        functools.partial(chain_kernel, S, N),
        out_shape=[pltpu.VMEM(*result) for result in results],
        in_specs=[hbm] * 10,
        out_specs=[vmem] * 5,
        scratch_shapes=scratch,
        compiler_params=pltpu.CompilerParams(
            collective_id=0, has_side_effects=True, vmem_limit_bytes=CHAIN_VMEM_LIMIT
        ),
    )(enc_hidden, mlp_gain[None, :], final_gain[None, :], w_gate, w_up, w_down, wk, wv, q, c)
    hidden_grad, query_grad, gate_grad, up_grad, down_grad = pl.pallas_call(
        write_kernel,
        out_shape=[shape(*result) for result in results],
        in_specs=[vmem] * 5,
        out_specs=[hbm] * 5,
        scratch_shapes=[dma((5,))],
        compiler_params=pltpu.CompilerParams(vmem_limit_bytes=WRITE_VMEM_LIMIT),
    )(*made)
    return query_grad[None, :, :], hidden_grad, gate_grad, up_grad, down_grad


def on_device(S, N, enc_hidden, mlp_gain, final_gain, w_gate, *rest):
    tt, F = enc_hidden.shape
    Hs = w_gate.shape[1] // S
    fits = Hs % LANES == 0 and F % LANES == 0 and tt % 16 == 0 and N * tt <= LANES
    run = fast if fits else general
    return run(S, N, enc_hidden, mlp_gain, final_gain, w_gate, *rest)


def solution(mesh):
    in_specs = (
        P(("dp", "tensor"), "section"),
        P("section"),
        P("section"),
        P("section", "tensor"),
        P("section", "tensor"),
        P("tensor", "section"),
        P("section", None, "tensor"),
        P("section", None, "tensor"),
        P("section", "dp", "tensor"),
        P("section", "dp", "tensor"),
    )
    out_specs = (
        P("section", "dp", "tensor"),
        P(("dp", "tensor"), "section"),
        P(("dp", "section"), "tensor"),
        P(("dp", "section"), "tensor"),
        P(("dp", "tensor"), "section"),
    )
    body = functools.partial(on_device, mesh.shape["section"], mesh.shape["tensor"])
    return jax.shard_map(
        body, mesh=mesh, in_specs=in_specs, out_specs=out_specs, check_vma=False
    )
```

```python
import contextlib
import functools
import jax
import jax.numpy as jnp
from jax import lax
from jax.experimental import pallas as pl
from jax.experimental.pallas import tpu as pltpu
from jax.sharding import PartitionSpec as P

HEAD = 256
EPSILON = 1e-06
LANES = 128
MESH = pl.DeviceIdType.MESH
VMEM_LIMIT = 58 * 1024 * 1024
CHAIN_VMEM_LIMIT = 54 * 1024 * 1024
WRITE_VMEM_LIMIT = 4 * 1024 * 1024
ROWS = (((0,), (0,)), ((), ()))
COLS = (((1,), (1,)), ((), ()))
F32 = jnp.float32
BF16 = jnp.bfloat16


def mark(name):
    return contextlib.nullcontext()


def enter(sizes):
    barrier = pltpu.get_barrier_semaphore()
    for axis, n in sizes:
        me = lax.axis_index(axis)
        for k in range(1, n):
            pl.semaphore_signal(
                barrier, inc=1, device_id={axis: lax.rem(me + k, n)}, device_id_type=MESH
            )
    pl.semaphore_wait(barrier, sum(n - 1 for _, n in sizes))


def post(axis, n, source, target, send_sem, recv_sem):
    me = lax.axis_index(axis)
    copies = []
    for k in range(1, n):
        peer = lax.rem(me + k, n)
        copy = pltpu.make_async_remote_copy(
            src_ref=source(peer),
            dst_ref=target(k - 1),
            send_sem=send_sem.at[k - 1],
            recv_sem=recv_sem.at[k - 1],
            device_id={axis: peer},
            device_id_type=MESH,
        )
        copy.start()
        copies.append(copy)
    return copies


def gather(axis, n, ref, send_sem, recv_sem):
    me = lax.axis_index(axis)
    return post(axis, n, lambda peer: ref.at[me], lambda k: ref.at[me], send_sem, recv_sem)


def scatter(axis, n, out, into, send_sem, recv_sem):
    return post(axis, n, lambda peer: out.at[peer], lambda k: into.at[k], send_sem, recv_sem)


def finish(*groups):
    for copies in groups:
        for copy in copies:
            copy.wait()


def total(own, into, n):
    acc = own.astype(F32)
    for k in range(n - 1):
        acc = acc + into[k].astype(F32)
    return acc


def attend(keys, values, q, c):
    scale = HEAD ** (-0.5)
    scores = lax.dot_general(keys, q, COLS, preferred_element_type=F32) * scale
    weights = jnp.exp(scores - jnp.max(scores, axis=0, keepdims=True))
    probs = weights / jnp.sum(weights, axis=0, keepdims=True)
    probs_bf = probs.astype(BF16)
    dprob = lax.dot_general(values, c, COLS, preferred_element_type=F32)
    delta = jnp.sum(probs_bf.astype(F32) * dprob, axis=0, keepdims=True)
    dscore = (probs * (dprob - delta) * scale).astype(BF16)
    query_grad = lax.dot_general(dscore, keys, ROWS, preferred_element_type=F32).astype(BF16)
    key_grad = jnp.dot(dscore, q, preferred_element_type=F32).astype(BF16)
    value_grad = jnp.dot(probs_bf, c, preferred_element_type=F32).astype(BF16)
    return query_grad, key_grad, value_grad


def step_kernel(
    S, N, x_ref, mg_ref, fg_ref, wg_hbm, wu_hbm, wd_hbm, wk_hbm, wv_hbm, q_hbm, c_hbm,
    qg_hbm, hg_out, normed_out, hid_out, oall_out, gate_out, up_out,
    wg, wu, wd, wk, wv, q, c, qg,
    xg, sqs, sqr, gus, gur, hid_all, inv_all, ds, dr, feat, sqo, enc, af, eg,
    r6, s6, r6b, pin, oall, s9, r9, aall, s11, r11, pin2,
    load_sem, store_sem, ssem, rsem,
):
    tt, F = x_ref.shape
    T = N * tt
    ts = T // S
    H = wg.shape[1]
    D = F * S
    heads = q.shape[1] // HEAD
    sec = lax.axis_index("section")
    ten = lax.axis_index("tensor")
    loads = [
        pltpu.make_async_copy(src, dst, load_sem.at[i])
        for i, (src, dst) in enumerate((
            (wg_hbm, wg), (wu_hbm, wu), (wd_hbm, wd), (wk_hbm, wk), (wv_hbm, wv),
            (q_hbm, q), (c_hbm, c),
        ))
    ]
    for load in loads[:3]:
        load.start()
    xg[ten] = x_ref[...]
    enter((("section", S), ("tensor", N)))
    finish(post("tensor", N, lambda p: x_ref, lambda k: xg.at[ten], ssem.at[0], rsem.at[0]))
    wide = xg[...].reshape(T, F).astype(F32)
    scaled = (wide * mg_ref[...]).astype(BF16)
    square = jnp.sum(wide * wide, axis=1, keepdims=True)
    sqs[...] = jnp.broadcast_to(square, (T, LANES)).reshape(S, ts, LANES)
    loads[0].wait()
    gus[0] = jnp.dot(scaled, wg[...], preferred_element_type=F32).astype(BF16).reshape(S, ts, H)
    move_q = scatter("section", S, sqs, sqr, ssem.at[3], rsem.at[3])
    move_g = scatter("section", S, gus.at[0], gur.at[0], ssem.at[1], rsem.at[1])
    loads[1].wait()
    gus[1] = jnp.dot(scaled, wu[...], preferred_element_type=F32).astype(BF16).reshape(S, ts, H)
    move_u = scatter("section", S, gus.at[1], gur.at[1], ssem.at[2], rsem.at[2])
    for load in loads[3:]:
        load.start()
    finish(move_q, move_g)
    inv = lax.rsqrt(total(sqs[sec], sqr, S) / D + EPSILON)
    inv_all[sec] = inv
    inv = inv[:, :1]
    gate_pre = total(gus[0, sec], gur.at[0], S) * inv
    sig = jax.nn.sigmoid(gate_pre)
    act = gate_pre * sig
    af[0, sec] = act.astype(BF16)
    slope = sig * (1.0 + gate_pre * (1.0 - sig))
    finish(move_u)
    up_pre = total(gus[1, sec], gur.at[1], S) * inv
    hid_all[sec] = (act * up_pre).astype(BF16)
    move_h = gather("section", S, hid_all, ssem.at[4], rsem.at[4])
    move_i = gather("section", S, inv_all, ssem.at[5], rsem.at[5])
    af[1, sec] = (up_pre * slope).astype(BF16)
    loads[2].wait()
    finish(move_h)
    hid = hid_all[...].reshape(T, H)
    ds[...] = jnp.dot(hid, wd[...], preferred_element_type=F32).astype(BF16).reshape(N, tt, F)
    move_d = scatter("tensor", N, ds, dr, ssem.at[6], rsem.at[6])
    hid_out[...] = hid
    finish(move_i)
    inv_tok = inv_all[...].reshape(T, LANES)
    normed_out[...] = (wide * inv_tok[:, :1] * mg_ref[...]).astype(BF16)
    finish(move_d)
    outer = x_ref[...].astype(F32) + total(ds[ten], dr, N)
    feat[sec] = (outer * fg_ref[...]).astype(BF16)
    sqo[sec] = jnp.broadcast_to(jnp.sum(outer * outer, axis=1, keepdims=True), (tt, LANES))
    move_s = gather("section", S, sqo, ssem.at[8], rsem.at[8])
    move_f = gather("section", S, feat, ssem.at[7], rsem.at[7])
    finish(move_s, move_f)
    move_act = gather("section", S, af.at[0], ssem.at[10], rsem.at[10])
    move_fac = gather("section", S, af.at[1], ssem.at[11], rsem.at[11])
    inv_o = lax.rsqrt(jnp.sum(sqo[...], axis=0) / D + EPSILON)
    enc[ten] = (feat[...].astype(F32) * inv_o[None, :, :1]).astype(BF16)
    inv_o = inv_o[:, :1]
    move_e = gather("tensor", N, enc, ssem.at[9], rsem.at[9])
    for load in loads[3:]:
        load.wait()
    finish(move_e)

    width = heads * HEAD
    keys = jnp.zeros((T, width), F32)
    values = jnp.zeros((T, width), F32)
    for s in range(S):
        block = enc[:, s].reshape(T, F)
        keys += jnp.dot(block, wk[s * F : (s + 1) * F, :], preferred_element_type=F32)
        values += jnp.dot(block, wv[s * F : (s + 1) * F, :], preferred_element_type=F32)
    keys = keys.astype(BF16)
    values = values.astype(BF16)
    key_grads, value_grads, stores = [], [], []
    for h in range(heads):
        cols = slice(h * HEAD, (h + 1) * HEAD)
        query_grad, key_grad, value_grad = attend(
            keys[:, cols], values[:, cols], q[:, cols], c[:, cols]
        )
        qg[h] = query_grad
        store = pltpu.make_async_copy(qg.at[h], qg_hbm.at[:, cols], store_sem.at[h])
        store.start()
        stores.append(store)
        key_grads.append(key_grad)
        value_grads.append(value_grad)
    key_grad = jnp.concatenate(key_grads, axis=1)
    value_grad = jnp.concatenate(value_grads, axis=1)
    for s in range(S):
        rows = slice(s * F, (s + 1) * F)
        part = lax.dot_general(key_grad, wk[rows, :], COLS, preferred_element_type=F32)
        part += lax.dot_general(value_grad, wv[rows, :], COLS, preferred_element_type=F32)
        eg[:, s] = part.astype(BF16).reshape(N, tt, F)

    finish(scatter("tensor", N, eg, r6, ssem.at[12], rsem.at[12]))
    s6[...] = total(eg[ten], r6, N).astype(BF16)
    finish(scatter("section", S, s6, r6b, ssem.at[13], rsem.at[13]))
    scaled_out = fg_ref[...] * total(s6[sec], r6b, S)
    pin[sec] = jnp.broadcast_to(
        jnp.sum(scaled_out * outer, axis=1, keepdims=True), (tt, LANES)
    )
    finish(gather("section", S, pin, ssem.at[14], rsem.at[14]))
    inner = jnp.sum(pin[...], axis=0)[:, :1] / D
    outer_grad = inv_o * scaled_out - outer * (inv_o * inv_o * inv_o * inner)
    oall[ten] = outer_grad.astype(BF16)
    finish(gather("tensor", N, oall, ssem.at[15], rsem.at[15]))
    grads = oall[...].reshape(T, F)
    half = H // 2
    moves = []
    for i in range(2):
        s9[i] = (
            lax.dot_general(
                grads, wd[i * half : (i + 1) * half, :], COLS, preferred_element_type=F32
            )
            .astype(BF16)
            .reshape(S, ts, half)
        )
        moves.append(scatter("section", S, s9.at[i], r9.at[i], ssem.at[16 + i], rsem.at[16 + i]))
    oall_out[...] = grads
    finish(move_act, move_fac)
    gathers = []
    for i in range(2):
        finish(moves[i])
        aall[i, sec] = total(s9[i, sec], r9.at[i], S).astype(BF16)
        gathers.append(gather("section", S, aall.at[i], ssem.at[18 + i], rsem.at[18 + i]))
    parts = None
    for i in range(2):
        cols = slice(i * half, (i + 1) * half)
        finish(gathers[i])
        act_grad = aall[i].reshape(T, half).astype(F32)
        up_grad = (act_grad * af[0, :, :, cols].reshape(T, half).astype(F32)).astype(BF16)
        gate_grad = (act_grad * af[1, :, :, cols].reshape(T, half).astype(F32)).astype(BF16)
        up_out[:, cols] = up_grad
        gate_out[:, cols] = gate_grad
        part = lax.dot_general(gate_grad, wg[:, cols], COLS, preferred_element_type=F32)
        part += lax.dot_general(up_grad, wu[:, cols], COLS, preferred_element_type=F32)
        parts = part if parts is None else parts + part
    s11[...] = parts.astype(BF16).reshape(N, tt, F)
    finish(scatter("tensor", N, s11, r11, ssem.at[20], rsem.at[20]))
    hidden = x_ref[...].astype(F32)
    scaled_in = mg_ref[...] * total(s11[ten], r11, N)
    pin2[sec] = jnp.broadcast_to(
        jnp.sum(scaled_in * hidden, axis=1, keepdims=True), (tt, LANES)
    )
    finish(gather("section", S, pin2, ssem.at[21], rsem.at[21]))
    inner_in = jnp.sum(pin2[...], axis=0)[:, :1] / D
    inv_flat = inv_all.reshape(T, LANES)
    inv_in = inv_flat[pl.ds(pl.multiple_of(ten * tt, tt), tt), :][:, :1]
    hg_out[...] = (
        outer_grad + inv_in * scaled_in - hidden * (inv_in * inv_in * inv_in * inner_in)
    )
    for store in stores:
        store.wait()


def general(
    S, N, enc_hidden, mlp_gain, final_gain, w_gate, w_up, w_down, key_weight, value_weight,
    queries, context_grad,
):
    tt, F = enc_hidden.shape
    T = N * tt
    ts = T // S
    H = w_gate.shape[1]
    peers = max(S, N) - 1
    vmem = pl.BlockSpec(memory_space=pltpu.VMEM)
    hbm = pl.BlockSpec(memory_space=pl.ANY)
    shape = jax.ShapeDtypeStruct
    dma = pltpu.SemaphoreType.DMA
    wk, wv, q, c = key_weight[0], value_weight[0], queries[0], context_grad[0]
    large = (w_gate, w_up, w_down, wk, wv, q, c)
    rows = q.shape[0]
    heads = q.shape[1] // HEAD
    scratch = [pltpu.VMEM(w.shape, BF16) for w in large]
    scratch += [
        pltpu.VMEM((heads, rows, HEAD), BF16),
        pltpu.VMEM((N, tt, F), BF16),
        pltpu.VMEM((S, ts, LANES), F32),
        pltpu.VMEM((S - 1, ts, LANES), F32),
        pltpu.VMEM((2, S, ts, H), BF16),
        pltpu.VMEM((2, S - 1, ts, H), BF16),
        pltpu.VMEM((S, ts, H), BF16),
        pltpu.VMEM((S, ts, LANES), F32),
        pltpu.VMEM((N, tt, F), BF16),
        pltpu.VMEM((N - 1, tt, F), BF16),
        pltpu.VMEM((S, tt, F), BF16),
        pltpu.VMEM((S, tt, LANES), F32),
        pltpu.VMEM((N, S, tt, F), BF16),
        pltpu.VMEM((2, S, ts, H), BF16),
        pltpu.VMEM((N, S, tt, F), BF16),
        pltpu.VMEM((N - 1, S, tt, F), BF16),
        pltpu.VMEM((S, tt, F), BF16),
        pltpu.VMEM((S - 1, tt, F), BF16),
        pltpu.VMEM((S, tt, LANES), F32),
        pltpu.VMEM((N, tt, F), BF16),
        pltpu.VMEM((2, S, ts, H // 2), BF16),
        pltpu.VMEM((2, S - 1, ts, H // 2), BF16),
        pltpu.VMEM((2, S, ts, H // 2), BF16),
        pltpu.VMEM((N, tt, F), BF16),
        pltpu.VMEM((N - 1, tt, F), BF16),
        pltpu.VMEM((S, tt, LANES), F32),
        dma((7,)), dma((heads,)), dma((22, peers)), dma((22, peers)),
    ]
    query_grad, hidden_grad, normed, hid, outer_all, gate_all, up_all = pl.pallas_call(
        functools.partial(step_kernel, S, N),
        out_shape=[
            shape(q.shape, BF16), shape((tt, F), F32), shape((T, F), BF16),
            shape((T, H), BF16), shape((T, F), BF16), shape((T, H), BF16), shape((T, H), BF16),
        ],
        in_specs=[vmem] * 3 + [hbm] * 7,
        out_specs=[hbm] + [vmem] * 6,
        scratch_shapes=scratch,
        compiler_params=pltpu.CompilerParams(
            collective_id=0, has_side_effects=True, vmem_limit_bytes=VMEM_LIMIT
        ),
    )(enc_hidden, mlp_gain[None, :], final_gain[None, :], *large)

    outer_product = lambda a, b: lax.dot_general(
        a, b, ROWS, preferred_element_type=F32
    ).astype(BF16)
    return (
        query_grad[None, :, :],
        hidden_grad,
        outer_product(normed, gate_all),
        outer_product(normed, up_all),
        outer_product(hid, outer_all),
    )


def lane_of_row(rows, offset):
    row = lax.broadcasted_iota(jnp.int32, (rows, LANES), 0) + offset
    return (row == lax.broadcasted_iota(jnp.int32, (rows, LANES), 1)).astype(F32)


def to_row(column, offset):
    return jnp.sum(column * lane_of_row(column.shape[0], offset), axis=0, keepdims=True)


def to_column(row, rows, offset):
    return jnp.sum(row * lane_of_row(rows, offset), axis=1, keepdims=True)


def send(source, target, send_sem, recv_sem, **peer):
    pltpu.make_async_remote_copy(
        src_ref=source,
        dst_ref=target,
        send_sem=send_sem,
        recv_sem=recv_sem,
        device_id=peer,
        device_id_type=MESH,
    ).start()


def arrive(cover, sem):
    pltpu.make_async_copy(cover, cover, sem).wait()


def product(a, b):
    return lax.dot_general(a, b, ROWS, preferred_element_type=F32).astype(BF16)


def chain_kernel(
    S, N, x_hbm, mg_hbm, fg_hbm, wg_hbm, wu_hbm, wd_hbm, wk_hbm, wv_hbm, q_hbm, c_hbm,
    hg_out, qg_out, gw_out, uw_out, dw_out,
    gains, wgu, wd, wkv, qc,
    xg, sqr, gus, gur, hid, af, comb, ds, dsb, dr, encb, sso, egb, er, ror, oall,
    s9, r9, aall, rir, gate, up, s11, s11b, r11, rit, dsc,
    load_sem, ssem, rsem, psem,
):
    tt, F = x_hbm.shape
    T = N * tt
    H = wd.shape[0]
    Hs = H // S
    D = F * S
    heads = qc.shape[2] // HEAD
    sec = lax.axis_index("section")
    ten = lax.axis_index("tensor")
    turn = 1 - 2 * (sec // ((S + 1) // 2))
    sent = []

    def section(k):
        return lax.rem(sec + turn * k + S, S)

    def tensor(k):
        return lax.rem(ten + k, N)

    low = (1 - turn) // 2
    rank = low * (S - 1) + turn * sec

    def distant(i):
        other = S - 1 - i - (i + rank) // (S - 1)
        return low * (S - 1) + turn * other

    near = range(1, S)
    far = [distant(i) for i in range(S - 1)]
    across = range(1, N)

    def units(p):
        return pl.ds(pl.multiple_of(p * Hs, LANES), Hs)

    def features(p):
        return pl.ds(pl.multiple_of(p * F, F), F)

    def others(ref):
        return ref.at[pl.ds(0, ref.shape[0] - 1)]

    def to_tensor(lane, source, target, cover):
        for k in across:
            send(source(tensor(k)), target, ssem.at[lane], rsem.at[lane], tensor=tensor(k))
        sent.append((cover, lane))

    def to_section(lane, source, target, cover, sem=None):
        for p in far:
            send(
                source(p), target, ssem.at[lane], rsem.at[lane] if sem is None else sem, section=p
            )
        sent.append((cover, lane))

    def to_everyone(lane, source, target, sections):
        for p in sections:
            for j in range(N):
                if p is not sec or j:
                    send(
                        source(p, tensor(j)), target, ssem.at[lane], rsem.at[lane],
                        section=p, tensor=tensor(j),
                    )

    barrier = pltpu.get_barrier_semaphore()
    for k in range(S):
        for j in range(N):
            if k or j:
                pl.semaphore_signal(
                    barrier,
                    inc=1,
                    device_id={"section": section(k), "tensor": tensor(j)},
                    device_id_type=MESH,
                )
    loads = [
        pltpu.make_async_copy(src, dst, load_sem.at[i])
        for src, dst, i in (
            (x_hbm, xg.at[ten], 0), (mg_hbm, gains.at[0], 1), (fg_hbm, gains.at[1], 1),
            (wg_hbm, wgu.at[0], 2), (wu_hbm, wgu.at[1], 2), (wd_hbm, wd, 3),
            (wk_hbm, wkv.at[0], 4), (wv_hbm, wkv.at[1], 4),
            (q_hbm, qc.at[0], 5), (c_hbm, qc.at[1], 5),
        )
    ]
    for load in loads[:6]:
        load.start()
    loads[0].wait()
    with mark("enter"):
        pl.semaphore_wait(barrier, S * N - 1)
    to_tensor(0, lambda p: xg.at[ten], xg.at[ten], others(xg))
    arrive(gains, load_sem.at[1])
    arrive(wgu, load_sem.at[2])
    mg, fg = gains.at[0], gains.at[1]
    wg, wu = wgu.at[0], wgu.at[1]
    wk, wv = wkv.at[0], wkv.at[1]
    with mark("x"):
        arrive(others(xg), rsem.at[0])

    wide = xg[...].reshape(T, F).astype(F32)
    scaled = (wide * mg[...]).astype(BF16)
    square = jnp.sum(wide * wide, axis=1, keepdims=True)
    sqr[sec] = to_row(square, 0)
    to_section(1, lambda p: sqr.at[sec], sqr.at[sec], others(sqr))
    for p in far:
        gus[p, 0] = jnp.dot(scaled, wg[:, units(p)], preferred_element_type=F32).astype(BF16)
        gus[p, 1] = jnp.dot(scaled, wu[:, units(p)], preferred_element_type=F32).astype(BF16)
        send(gus.at[p], gur.at[sec], ssem.at[2], rsem.at[2], section=p)
    sent.append((others(gus), 2))
    for load in loads[6:]:
        load.start()
    gate_pre = jnp.dot(scaled, wg[:, units(sec)], preferred_element_type=F32)
    up_pre = jnp.dot(scaled, wu[:, units(sec)], preferred_element_type=F32)
    with mark("sq"):
        arrive(others(sqr), rsem.at[1])
    inv = lax.rsqrt(to_column(jnp.sum(sqr[...], axis=0), T, 0) / D + EPSILON)
    normed = (wide * inv * mg[...]).astype(BF16)
    loads[5].wait()
    with mark("gu"):
        arrive(others(gur), rsem.at[2])
    for k in near:
        gate_pre = gate_pre + gur[section(k), 0].astype(F32)
        up_pre = up_pre + gur[section(k), 1].astype(F32)
    gate_pre = gate_pre * inv
    up_pre = up_pre * inv
    sig = jax.nn.sigmoid(gate_pre)
    act = gate_pre * sig
    hid[sec] = (act * up_pre).astype(BF16)
    to_section(3, lambda p: hid.at[sec], hid.at[sec], others(hid), psem.at[0, sec])
    factor = up_pre * (sig * (1.0 + gate_pre * (1.0 - sig)))
    piece = T // 2
    af[sec, 0] = act[:piece].astype(BF16)
    af[sec, 1] = act[piece:].astype(BF16)
    af[sec, 2] = factor[:piece].astype(BF16)
    af[sec, 3] = factor[piece:].astype(BF16)
    comb[...] = act * up_pre + factor * gate_pre
    down = jnp.dot(hid[sec], wd[units(sec), :], preferred_element_type=F32)
    for k in near:
        p = section(k)
        with mark(f"hid{k}"):
            arrive(hid.at[p], psem.at[0, p])
        down = down + jnp.dot(hid[p], wd[units(p), :], preferred_element_type=F32)
    ds[...] = down.reshape(N, tt, F)
    dsb[...] = down.astype(BF16).reshape(N, tt, F)
    to_tensor(4, lambda p: dsb.at[p], dr.at[ten], others(dsb))
    early = lambda p: af.at[p, pl.ds(0, 1)]
    late = lambda p: af.at[p, pl.ds(1, 3)]
    to_section(5, lambda p: early(sec), early(sec), af.at[pl.ds(0, S - 1), pl.ds(0, 1)])
    with mark("ds"):
        arrive(others(dr), rsem.at[4])
    outer = xg[ten].astype(F32) + ds[ten]
    for k in across:
        outer = outer + dr[tensor(k)].astype(F32)
    me = sec * N + ten
    sso[me] = to_row(jnp.sum(outer * outer, axis=1, keepdims=True), ten * tt)
    encb[me] = (outer * fg[...]).astype(BF16)
    to_everyone(6, lambda s, n: sso.at[me], sso.at[me], [*far, sec])
    sent.append((others(sso), 6))
    for p in far:
        send(encb.at[me], encb.at[me], ssem.at[7], psem.at[1, sec], section=p)
    for k in across:
        send(encb.at[me], encb.at[me], ssem.at[7], psem.at[2, sec], tensor=tensor(k))
    for k in near:
        block = section(k) * N + ten
        with mark(f"pass{k}"):
            arrive(encb.at[block], psem.at[1, section(k)])
        for j in across:
            send(
                encb.at[block], encb.at[block], ssem.at[7], psem.at[2, section(k)],
                tensor=tensor(j),
            )
    sent.append((others(encb), 7))
    to_section(8, lambda p: late(sec), late(sec), af.at[pl.ds(0, S - 1), pl.ds(1, 3)])
    arrive(wkv, load_sem.at[4])
    arrive(qc, load_sem.at[5])
    keys = values = None
    for k in range(S):
        p = section(k)
        with mark(f"enc{k}"):
            arrive(encb.at[pl.ds(0, N - 1)], psem.at[2, p])
        block = encb[pl.ds(p * N, N)].reshape(T, F)
        key_part = jnp.dot(block, wk[features(p), :], preferred_element_type=F32)
        value_part = jnp.dot(block, wv[features(p), :], preferred_element_type=F32)
        keys = key_part if keys is None else keys + key_part
        values = value_part if values is None else values + value_part
    with mark("sso"):
        arrive(others(sso), rsem.at[6])
    squares = jnp.sum(sso[...], axis=0)
    inv_all = lax.rsqrt(to_column(squares, T, 0) / D + EPSILON)
    inv_o = lax.rsqrt(to_column(squares, tt, ten * tt) / D + EPSILON)
    keys = (keys * inv_all).astype(BF16)
    values = (values * inv_all).astype(BF16)
    scale = HEAD ** (-0.5)
    key_grads, value_grads = [], []
    inner = None
    for h in range(heads):
        cols = slice(h * HEAD, (h + 1) * HEAD)
        q, c = qc[0, :, cols], qc[1, :, cols]
        scores = lax.dot_general(keys[:, cols], q, COLS, preferred_element_type=F32) * scale
        weights = jnp.exp(scores - jnp.max(scores, axis=0, keepdims=True))
        probs = weights / jnp.sum(weights, axis=0, keepdims=True)
        probs_bf = probs.astype(BF16)
        dprob = lax.dot_general(values[:, cols], c, COLS, preferred_element_type=F32)
        delta = jnp.sum(probs_bf.astype(F32) * dprob, axis=0, keepdims=True)
        dscore = (probs * (dprob - delta) * scale).astype(BF16)
        dsc[h] = dscore
        key_grad = jnp.dot(dscore, q, preferred_element_type=F32).astype(BF16)
        value_grad = jnp.dot(probs_bf, c, preferred_element_type=F32).astype(BF16)
        part = key_grad.astype(F32) * keys[:, cols].astype(F32)
        part += value_grad.astype(F32) * values[:, cols].astype(F32)
        inner = part if inner is None else inner + part
        key_grads.append(key_grad)
        value_grads.append(value_grad)
    key_grad = jnp.concatenate(key_grads, axis=1)
    value_grad = jnp.concatenate(value_grads, axis=1)
    ror[me] = to_row(jnp.sum(inner, axis=1, keepdims=True), 0)
    to_everyone(9, lambda s, n: ror.at[me], ror.at[me], [*far, sec])
    sent.append((others(ror), 9))
    for p in [*far, sec]:
        part = lax.dot_general(key_grad, wk[features(p), :], COLS, preferred_element_type=F32)
        part += lax.dot_general(value_grad, wv[features(p), :], COLS, preferred_element_type=F32)
        egb[pl.ds(p * N, N)] = part.astype(BF16).reshape(N, tt, F)
        to_everyone(10, lambda s, n: egb.at[s * N + n], er.at[me], [p])
    sent.append((others(egb), 10))
    er[me] = egb[me]
    for h in range(heads):
        cols = slice(h * HEAD, (h + 1) * HEAD)
        qg_out[:, cols] = product(dsc[h], keys[:, cols])
    with mark("eg"):
        arrive(others(ror), rsem.at[9])
        arrive(others(er), rsem.at[10])
    inner = to_column(jnp.sum(ror[...], axis=0), tt, ten * tt)
    grad = jnp.sum(er[...].astype(F32), axis=0)
    outer_grad = inv_o * (fg[...] * grad) - outer * (inv_o * inv_o * inner / D)
    oall[ten] = outer_grad.astype(BF16)
    to_tensor(11, lambda p: oall.at[ten], oall.at[ten], others(oall))
    with mark("oall"):
        arrive(others(oall), rsem.at[11])
    grads = oall[...].reshape(T, F)
    for p in far:
        s9[p] = lax.dot_general(
            grads, wd[units(p), :], COLS, preferred_element_type=F32
        ).astype(BF16)
        send(s9.at[p], r9.at[sec], ssem.at[12], rsem.at[12], section=p)
    sent.append((others(s9), 12))
    act_grad = lax.dot_general(grads, wd[units(sec), :], COLS, preferred_element_type=F32)
    for s in range(S):
        dw_out[s * Hs : (s + 1) * Hs, :] = product(hid[s], grads)
    with mark("s9"):
        arrive(others(r9), rsem.at[12])
    for k in near:
        act_grad = act_grad + r9[section(k)].astype(F32)
    aall[sec] = act_grad.astype(BF16)
    to_section(13, lambda p: aall.at[sec], aall.at[sec], others(aall), psem.at[3, sec])
    rir[sec] = to_row(jnp.sum(act_grad * comb[...], axis=1, keepdims=True), 0)
    to_section(14, lambda p: rir.at[sec], rir.at[sec], others(rir))
    with mark("af"):
        arrive(af.at[pl.ds(0, S - 1), pl.ds(0, 1)], rsem.at[5])
        arrive(af.at[pl.ds(0, S - 1), pl.ds(1, 3)], rsem.at[8])
    part = None
    for k in range(S):
        p = section(k)
        if k:
            with mark(f"aall{k}"):
                arrive(aall.at[p], psem.at[3, p])
        act_grad = aall[p].astype(F32)
        factors = af[p].reshape(2, T, Hs)
        up_grad = (act_grad * factors[0].astype(F32)).astype(BF16)
        gate_grad = (act_grad * factors[1].astype(F32)).astype(BF16)
        up[p] = up_grad
        gate[p] = gate_grad
        more = lax.dot_general(gate_grad, wg[:, units(p)], COLS, preferred_element_type=F32)
        more += lax.dot_general(up_grad, wu[:, units(p)], COLS, preferred_element_type=F32)
        part = more if part is None else part + more
    s11[...] = part.reshape(N, tt, F)
    s11b[...] = part.astype(BF16).reshape(N, tt, F)
    to_tensor(15, lambda p: s11b.at[p], r11.at[ten], others(s11b))
    with mark("rir"):
        arrive(others(rir), rsem.at[14])
    rit[ten] = jnp.sum(rir[...], axis=0)
    to_tensor(16, lambda p: rit.at[ten], rit.at[ten], others(rit))
    for s in range(S):
        cols = slice(s * Hs, (s + 1) * Hs)
        gw_out[:, cols] = product(normed, gate[s])
        uw_out[:, cols] = product(normed, up[s])
    with mark("s11"):
        arrive(others(r11), rsem.at[15])
        arrive(others(rit), rsem.at[16])
    hidden = xg[ten].astype(F32)
    scaled_in = s11[ten]
    for k in across:
        scaled_in = scaled_in + r11[tensor(k)].astype(F32)
    scaled_in = mg[...] * scaled_in
    inner = to_column(jnp.sum(rit[...], axis=0), tt, ten * tt)
    squares = to_column(jnp.sum(sqr[...], axis=0), tt, ten * tt)
    inv_in = lax.rsqrt(squares / D + EPSILON)
    hg_out[...] = outer_grad + inv_in * scaled_in - hidden * (inv_in * inv_in * inner / D)
    with mark("end"):
        for cover, lane in sent:
            arrive(cover, ssem.at[lane])


def write_kernel(*refs):
    count = len(refs) // 2
    sem = refs[-1]
    copies = [
        pltpu.make_async_copy(refs[i], refs[count + i], sem.at[i]) for i in range(count)
    ]
    for copy in copies:
        copy.start()
    for copy in copies:
        copy.wait()


def fast(
    S, N, enc_hidden, mlp_gain, final_gain, w_gate, w_up, w_down, key_weight, value_weight,
    queries, context_grad,
):
    tt, F = enc_hidden.shape
    T = N * tt
    H = w_gate.shape[1]
    Hs = H // S
    vmem = pl.BlockSpec(memory_space=pltpu.VMEM)
    hbm = pl.BlockSpec(memory_space=pltpu.HBM)
    shape = jax.ShapeDtypeStruct
    dma = pltpu.SemaphoreType.DMA
    wk, wv, q, c = key_weight[0], value_weight[0], queries[0], context_grad[0]
    rows, width = q.shape
    heads = width // HEAD
    buf = lambda *dims: pltpu.VMEM(dims, BF16)
    wide = lambda *dims: pltpu.VMEM(dims, F32)
    scratch = [
        wide(2, 1, F), buf(2, F, H), buf(H, F), buf(2, *wk.shape), buf(2, rows, width),
        buf(N, tt, F),
        wide(S, 1, LANES),
        buf(S, 2, T, Hs),
        buf(S, 2, T, Hs),
        buf(S, T, Hs),
        buf(S, 4, T // 2, Hs),
        wide(T, Hs),
        wide(N, tt, F),
        buf(N, tt, F),
        buf(N, tt, F),
        buf(S * N, tt, F),
        wide(S * N, 1, LANES),
        buf(S * N, tt, F),
        buf(S * N, tt, F),
        wide(S * N, 1, LANES),
        buf(N, tt, F),
        buf(S, T, Hs),
        buf(S, T, Hs),
        buf(S, T, Hs),
        wide(S, 1, LANES),
        buf(S, T, Hs),
        buf(S, T, Hs),
        wide(N, tt, F),
        buf(N, tt, F),
        buf(N, tt, F),
        wide(N, 1, LANES),
        buf(heads, T, rows),
        dma((6,)), dma((17,)), dma((17,)), dma((4, S)),
    ]
    results = [
        ((tt, F), F32), ((rows, width), BF16), ((F, H), BF16), ((F, H), BF16), ((H, F), BF16)
    ]
    made = pl.pallas_call(
        functools.partial(chain_kernel, S, N),
        out_shape=[pltpu.VMEM(*result) for result in results],
        in_specs=[hbm] * 10,
        out_specs=[vmem] * 5,
        scratch_shapes=scratch,
        compiler_params=pltpu.CompilerParams(
            collective_id=0, has_side_effects=True, vmem_limit_bytes=CHAIN_VMEM_LIMIT
        ),
    )(enc_hidden, mlp_gain[None, :], final_gain[None, :], w_gate, w_up, w_down, wk, wv, q, c)
    hidden_grad, query_grad, gate_grad, up_grad, down_grad = pl.pallas_call(
        write_kernel,
        out_shape=[shape(*result) for result in results],
        in_specs=[vmem] * 5,
        out_specs=[hbm] * 5,
        scratch_shapes=[dma((5,))],
        compiler_params=pltpu.CompilerParams(vmem_limit_bytes=WRITE_VMEM_LIMIT),
    )(*made)
    return query_grad[None, :, :], hidden_grad, gate_grad, up_grad, down_grad


def on_device(S, N, enc_hidden, mlp_gain, final_gain, w_gate, *rest):
    tt, F = enc_hidden.shape
    Hs = w_gate.shape[1] // S
    fits = Hs % LANES == 0 and F % LANES == 0 and tt % 16 == 0 and N * tt <= LANES
    run = fast if fits else general
    return run(S, N, enc_hidden, mlp_gain, final_gain, w_gate, *rest)


def solution(mesh):
    in_specs = (
        P(("dp", "tensor"), "section"),
        P("section"),
        P("section"),
        P("section", "tensor"),
        P("section", "tensor"),
        P("tensor", "section"),
        P("section", None, "tensor"),
        P("section", None, "tensor"),
        P("section", "dp", "tensor"),
        P("section", "dp", "tensor"),
    )
    out_specs = (
        P("section", "dp", "tensor"),
        P(("dp", "tensor"), "section"),
        P(("dp", "section"), "tensor"),
        P(("dp", "section"), "tensor"),
        P(("dp", "tensor"), "section"),
    )
    body = functools.partial(on_device, mesh.shape["section"], mesh.shape["tensor"])
    return jax.shard_map(
        body, mesh=mesh, in_specs=in_specs, out_specs=out_specs, check_vma=False
    )
```

```python
import contextlib
import functools
import jax
import jax.numpy as jnp
from jax import lax
from jax.experimental import pallas as pl
from jax.experimental.pallas import tpu as pltpu
from jax.sharding import PartitionSpec as P

HEAD = 256
EPSILON = 1e-06
LANES = 128
MESH = pl.DeviceIdType.MESH
VMEM_LIMIT = 58 * 1024 * 1024
CHAIN_VMEM_LIMIT = 54 * 1024 * 1024
WRITE_VMEM_LIMIT = 4 * 1024 * 1024
ROWS = (((0,), (0,)), ((), ()))
COLS = (((1,), (1,)), ((), ()))
F32 = jnp.float32
BF16 = jnp.bfloat16


def mark(name):
    return contextlib.nullcontext()


def enter(sizes):
    barrier = pltpu.get_barrier_semaphore()
    for axis, n in sizes:
        me = lax.axis_index(axis)
        for k in range(1, n):
            pl.semaphore_signal(
                barrier, inc=1, device_id={axis: lax.rem(me + k, n)}, device_id_type=MESH
            )
    pl.semaphore_wait(barrier, sum(n - 1 for _, n in sizes))


def post(axis, n, source, target, send_sem, recv_sem):
    me = lax.axis_index(axis)
    copies = []
    for k in range(1, n):
        peer = lax.rem(me + k, n)
        copy = pltpu.make_async_remote_copy(
            src_ref=source(peer),
            dst_ref=target(k - 1),
            send_sem=send_sem.at[k - 1],
            recv_sem=recv_sem.at[k - 1],
            device_id={axis: peer},
            device_id_type=MESH,
        )
        copy.start()
        copies.append(copy)
    return copies


def gather(axis, n, ref, send_sem, recv_sem):
    me = lax.axis_index(axis)
    return post(axis, n, lambda peer: ref.at[me], lambda k: ref.at[me], send_sem, recv_sem)


def scatter(axis, n, out, into, send_sem, recv_sem):
    return post(axis, n, lambda peer: out.at[peer], lambda k: into.at[k], send_sem, recv_sem)


def finish(*groups):
    for copies in groups:
        for copy in copies:
            copy.wait()


def total(own, into, n):
    acc = own.astype(F32)
    for k in range(n - 1):
        acc = acc + into[k].astype(F32)
    return acc


def attend(keys, values, q, c):
    scale = HEAD ** (-0.5)
    scores = lax.dot_general(keys, q, COLS, preferred_element_type=F32) * scale
    weights = jnp.exp(scores - jnp.max(scores, axis=0, keepdims=True))
    probs = weights / jnp.sum(weights, axis=0, keepdims=True)
    probs_bf = probs.astype(BF16)
    dprob = lax.dot_general(values, c, COLS, preferred_element_type=F32)
    delta = jnp.sum(probs_bf.astype(F32) * dprob, axis=0, keepdims=True)
    dscore = (probs * (dprob - delta) * scale).astype(BF16)
    query_grad = lax.dot_general(dscore, keys, ROWS, preferred_element_type=F32).astype(BF16)
    key_grad = jnp.dot(dscore, q, preferred_element_type=F32).astype(BF16)
    value_grad = jnp.dot(probs_bf, c, preferred_element_type=F32).astype(BF16)
    return query_grad, key_grad, value_grad


def step_kernel(
    S, N, x_ref, mg_ref, fg_ref, wg_hbm, wu_hbm, wd_hbm, wk_hbm, wv_hbm, q_hbm, c_hbm,
    qg_hbm, hg_out, normed_out, hid_out, oall_out, gate_out, up_out,
    wg, wu, wd, wk, wv, q, c, qg,
    xg, sqs, sqr, gus, gur, hid_all, inv_all, ds, dr, feat, sqo, enc, af, eg,
    r6, s6, r6b, pin, oall, s9, r9, aall, s11, r11, pin2,
    load_sem, store_sem, ssem, rsem,
):
    tt, F = x_ref.shape
    T = N * tt
    ts = T // S
    H = wg.shape[1]
    D = F * S
    heads = q.shape[1] // HEAD
    sec = lax.axis_index("section")
    ten = lax.axis_index("tensor")
    loads = [
        pltpu.make_async_copy(src, dst, load_sem.at[i])
        for i, (src, dst) in enumerate((
            (wg_hbm, wg), (wu_hbm, wu), (wd_hbm, wd), (wk_hbm, wk), (wv_hbm, wv),
            (q_hbm, q), (c_hbm, c),
        ))
    ]
    for load in loads[:3]:
        load.start()
    xg[ten] = x_ref[...]
    enter((("section", S), ("tensor", N)))
    finish(post("tensor", N, lambda p: x_ref, lambda k: xg.at[ten], ssem.at[0], rsem.at[0]))
    wide = xg[...].reshape(T, F).astype(F32)
    scaled = (wide * mg_ref[...]).astype(BF16)
    square = jnp.sum(wide * wide, axis=1, keepdims=True)
    sqs[...] = jnp.broadcast_to(square, (T, LANES)).reshape(S, ts, LANES)
    loads[0].wait()
    gus[0] = jnp.dot(scaled, wg[...], preferred_element_type=F32).astype(BF16).reshape(S, ts, H)
    move_q = scatter("section", S, sqs, sqr, ssem.at[3], rsem.at[3])
    move_g = scatter("section", S, gus.at[0], gur.at[0], ssem.at[1], rsem.at[1])
    loads[1].wait()
    gus[1] = jnp.dot(scaled, wu[...], preferred_element_type=F32).astype(BF16).reshape(S, ts, H)
    move_u = scatter("section", S, gus.at[1], gur.at[1], ssem.at[2], rsem.at[2])
    for load in loads[3:]:
        load.start()
    finish(move_q, move_g)
    inv = lax.rsqrt(total(sqs[sec], sqr, S) / D + EPSILON)
    inv_all[sec] = inv
    inv = inv[:, :1]
    gate_pre = total(gus[0, sec], gur.at[0], S) * inv
    sig = jax.nn.sigmoid(gate_pre)
    act = gate_pre * sig
    af[0, sec] = act.astype(BF16)
    slope = sig * (1.0 + gate_pre * (1.0 - sig))
    finish(move_u)
    up_pre = total(gus[1, sec], gur.at[1], S) * inv
    hid_all[sec] = (act * up_pre).astype(BF16)
    move_h = gather("section", S, hid_all, ssem.at[4], rsem.at[4])
    move_i = gather("section", S, inv_all, ssem.at[5], rsem.at[5])
    af[1, sec] = (up_pre * slope).astype(BF16)
    loads[2].wait()
    finish(move_h)
    hid = hid_all[...].reshape(T, H)
    ds[...] = jnp.dot(hid, wd[...], preferred_element_type=F32).astype(BF16).reshape(N, tt, F)
    move_d = scatter("tensor", N, ds, dr, ssem.at[6], rsem.at[6])
    hid_out[...] = hid
    finish(move_i)
    inv_tok = inv_all[...].reshape(T, LANES)
    normed_out[...] = (wide * inv_tok[:, :1] * mg_ref[...]).astype(BF16)
    finish(move_d)
    outer = x_ref[...].astype(F32) + total(ds[ten], dr, N)
    feat[sec] = (outer * fg_ref[...]).astype(BF16)
    sqo[sec] = jnp.broadcast_to(jnp.sum(outer * outer, axis=1, keepdims=True), (tt, LANES))
    move_s = gather("section", S, sqo, ssem.at[8], rsem.at[8])
    move_f = gather("section", S, feat, ssem.at[7], rsem.at[7])
    finish(move_s, move_f)
    move_act = gather("section", S, af.at[0], ssem.at[10], rsem.at[10])
    move_fac = gather("section", S, af.at[1], ssem.at[11], rsem.at[11])
    inv_o = lax.rsqrt(jnp.sum(sqo[...], axis=0) / D + EPSILON)
    enc[ten] = (feat[...].astype(F32) * inv_o[None, :, :1]).astype(BF16)
    inv_o = inv_o[:, :1]
    move_e = gather("tensor", N, enc, ssem.at[9], rsem.at[9])
    for load in loads[3:]:
        load.wait()
    finish(move_e)

    width = heads * HEAD
    keys = jnp.zeros((T, width), F32)
    values = jnp.zeros((T, width), F32)
    for s in range(S):
        block = enc[:, s].reshape(T, F)
        keys += jnp.dot(block, wk[s * F : (s + 1) * F, :], preferred_element_type=F32)
        values += jnp.dot(block, wv[s * F : (s + 1) * F, :], preferred_element_type=F32)
    keys = keys.astype(BF16)
    values = values.astype(BF16)
    key_grads, value_grads, stores = [], [], []
    for h in range(heads):
        cols = slice(h * HEAD, (h + 1) * HEAD)
        query_grad, key_grad, value_grad = attend(
            keys[:, cols], values[:, cols], q[:, cols], c[:, cols]
        )
        qg[h] = query_grad
        store = pltpu.make_async_copy(qg.at[h], qg_hbm.at[:, cols], store_sem.at[h])
        store.start()
        stores.append(store)
        key_grads.append(key_grad)
        value_grads.append(value_grad)
    key_grad = jnp.concatenate(key_grads, axis=1)
    value_grad = jnp.concatenate(value_grads, axis=1)
    for s in range(S):
        rows = slice(s * F, (s + 1) * F)
        part = lax.dot_general(key_grad, wk[rows, :], COLS, preferred_element_type=F32)
        part += lax.dot_general(value_grad, wv[rows, :], COLS, preferred_element_type=F32)
        eg[:, s] = part.astype(BF16).reshape(N, tt, F)

    finish(scatter("tensor", N, eg, r6, ssem.at[12], rsem.at[12]))
    s6[...] = total(eg[ten], r6, N).astype(BF16)
    finish(scatter("section", S, s6, r6b, ssem.at[13], rsem.at[13]))
    scaled_out = fg_ref[...] * total(s6[sec], r6b, S)
    pin[sec] = jnp.broadcast_to(
        jnp.sum(scaled_out * outer, axis=1, keepdims=True), (tt, LANES)
    )
    finish(gather("section", S, pin, ssem.at[14], rsem.at[14]))
    inner = jnp.sum(pin[...], axis=0)[:, :1] / D
    outer_grad = inv_o * scaled_out - outer * (inv_o * inv_o * inv_o * inner)
    oall[ten] = outer_grad.astype(BF16)
    finish(gather("tensor", N, oall, ssem.at[15], rsem.at[15]))
    grads = oall[...].reshape(T, F)
    half = H // 2
    moves = []
    for i in range(2):
        s9[i] = (
            lax.dot_general(
                grads, wd[i * half : (i + 1) * half, :], COLS, preferred_element_type=F32
            )
            .astype(BF16)
            .reshape(S, ts, half)
        )
        moves.append(scatter("section", S, s9.at[i], r9.at[i], ssem.at[16 + i], rsem.at[16 + i]))
    oall_out[...] = grads
    finish(move_act, move_fac)
    gathers = []
    for i in range(2):
        finish(moves[i])
        aall[i, sec] = total(s9[i, sec], r9.at[i], S).astype(BF16)
        gathers.append(gather("section", S, aall.at[i], ssem.at[18 + i], rsem.at[18 + i]))
    parts = None
    for i in range(2):
        cols = slice(i * half, (i + 1) * half)
        finish(gathers[i])
        act_grad = aall[i].reshape(T, half).astype(F32)
        up_grad = (act_grad * af[0, :, :, cols].reshape(T, half).astype(F32)).astype(BF16)
        gate_grad = (act_grad * af[1, :, :, cols].reshape(T, half).astype(F32)).astype(BF16)
        up_out[:, cols] = up_grad
        gate_out[:, cols] = gate_grad
        part = lax.dot_general(gate_grad, wg[:, cols], COLS, preferred_element_type=F32)
        part += lax.dot_general(up_grad, wu[:, cols], COLS, preferred_element_type=F32)
        parts = part if parts is None else parts + part
    s11[...] = parts.astype(BF16).reshape(N, tt, F)
    finish(scatter("tensor", N, s11, r11, ssem.at[20], rsem.at[20]))
    hidden = x_ref[...].astype(F32)
    scaled_in = mg_ref[...] * total(s11[ten], r11, N)
    pin2[sec] = jnp.broadcast_to(
        jnp.sum(scaled_in * hidden, axis=1, keepdims=True), (tt, LANES)
    )
    finish(gather("section", S, pin2, ssem.at[21], rsem.at[21]))
    inner_in = jnp.sum(pin2[...], axis=0)[:, :1] / D
    inv_flat = inv_all.reshape(T, LANES)
    inv_in = inv_flat[pl.ds(pl.multiple_of(ten * tt, tt), tt), :][:, :1]
    hg_out[...] = (
        outer_grad + inv_in * scaled_in - hidden * (inv_in * inv_in * inv_in * inner_in)
    )
    for store in stores:
        store.wait()


def general(
    S, N, enc_hidden, mlp_gain, final_gain, w_gate, w_up, w_down, key_weight, value_weight,
    queries, context_grad,
):
    tt, F = enc_hidden.shape
    T = N * tt
    ts = T // S
    H = w_gate.shape[1]
    peers = max(S, N) - 1
    vmem = pl.BlockSpec(memory_space=pltpu.VMEM)
    hbm = pl.BlockSpec(memory_space=pl.ANY)
    shape = jax.ShapeDtypeStruct
    dma = pltpu.SemaphoreType.DMA
    wk, wv, q, c = key_weight[0], value_weight[0], queries[0], context_grad[0]
    large = (w_gate, w_up, w_down, wk, wv, q, c)
    rows = q.shape[0]
    heads = q.shape[1] // HEAD
    scratch = [pltpu.VMEM(w.shape, BF16) for w in large]
    scratch += [
        pltpu.VMEM((heads, rows, HEAD), BF16),
        pltpu.VMEM((N, tt, F), BF16),
        pltpu.VMEM((S, ts, LANES), F32),
        pltpu.VMEM((S - 1, ts, LANES), F32),
        pltpu.VMEM((2, S, ts, H), BF16),
        pltpu.VMEM((2, S - 1, ts, H), BF16),
        pltpu.VMEM((S, ts, H), BF16),
        pltpu.VMEM((S, ts, LANES), F32),
        pltpu.VMEM((N, tt, F), BF16),
        pltpu.VMEM((N - 1, tt, F), BF16),
        pltpu.VMEM((S, tt, F), BF16),
        pltpu.VMEM((S, tt, LANES), F32),
        pltpu.VMEM((N, S, tt, F), BF16),
        pltpu.VMEM((2, S, ts, H), BF16),
        pltpu.VMEM((N, S, tt, F), BF16),
        pltpu.VMEM((N - 1, S, tt, F), BF16),
        pltpu.VMEM((S, tt, F), BF16),
        pltpu.VMEM((S - 1, tt, F), BF16),
        pltpu.VMEM((S, tt, LANES), F32),
        pltpu.VMEM((N, tt, F), BF16),
        pltpu.VMEM((2, S, ts, H // 2), BF16),
        pltpu.VMEM((2, S - 1, ts, H // 2), BF16),
        pltpu.VMEM((2, S, ts, H // 2), BF16),
        pltpu.VMEM((N, tt, F), BF16),
        pltpu.VMEM((N - 1, tt, F), BF16),
        pltpu.VMEM((S, tt, LANES), F32),
        dma((7,)), dma((heads,)), dma((22, peers)), dma((22, peers)),
    ]
    query_grad, hidden_grad, normed, hid, outer_all, gate_all, up_all = pl.pallas_call(
        functools.partial(step_kernel, S, N),
        out_shape=[
            shape(q.shape, BF16), shape((tt, F), F32), shape((T, F), BF16),
            shape((T, H), BF16), shape((T, F), BF16), shape((T, H), BF16), shape((T, H), BF16),
        ],
        in_specs=[vmem] * 3 + [hbm] * 7,
        out_specs=[hbm] + [vmem] * 6,
        scratch_shapes=scratch,
        compiler_params=pltpu.CompilerParams(
            collective_id=0, has_side_effects=True, vmem_limit_bytes=VMEM_LIMIT
        ),
    )(enc_hidden, mlp_gain[None, :], final_gain[None, :], *large)

    outer_product = lambda a, b: lax.dot_general(
        a, b, ROWS, preferred_element_type=F32
    ).astype(BF16)
    return (
        query_grad[None, :, :],
        hidden_grad,
        outer_product(normed, gate_all),
        outer_product(normed, up_all),
        outer_product(hid, outer_all),
    )


def lane_of_row(rows, offset):
    row = lax.broadcasted_iota(jnp.int32, (rows, LANES), 0) + offset
    return (row == lax.broadcasted_iota(jnp.int32, (rows, LANES), 1)).astype(F32)


def to_row(column, offset):
    return jnp.sum(column * lane_of_row(column.shape[0], offset), axis=0, keepdims=True)


def to_column(row, rows, offset):
    return jnp.sum(row * lane_of_row(rows, offset), axis=1, keepdims=True)


def send(source, target, send_sem, recv_sem, **peer):
    pltpu.make_async_remote_copy(
        src_ref=source,
        dst_ref=target,
        send_sem=send_sem,
        recv_sem=recv_sem,
        device_id=peer,
        device_id_type=MESH,
    ).start()


def arrive(cover, sem):
    pltpu.make_async_copy(cover, cover, sem).wait()


def product(a, b):
    return lax.dot_general(a, b, ROWS, preferred_element_type=F32).astype(BF16)


def chain_kernel(
    S, N, x_hbm, mg_hbm, fg_hbm, wg_hbm, wu_hbm, wd_hbm, wk_hbm, wv_hbm, q_hbm, c_hbm,
    hg_out, qg_out, gw_out, uw_out, dw_out,
    gains, wgu, wd, wkv, qc,
    xg, sqr, gus, gur, hold, stage, joined, hid, af, comb, ds, dsb, dr, encb, sso, egb, er, ror, oall,
    s9, r9, aall, rir, gate, up, s11, s11b, r11, rit, dsc,
    load_sem, ssem, rsem, psem,
):
    tt, F = x_hbm.shape
    T = N * tt
    H = wd.shape[0]
    Hs = H // S
    D = F * S
    heads = qc.shape[2] // HEAD
    sec = lax.axis_index("section")
    ten = lax.axis_index("tensor")
    turn = 1 - 2 * (sec // ((S + 1) // 2))
    sent = []

    def section(k):
        return lax.rem(sec + turn * k + S, S)

    def tensor(k):
        return lax.rem(ten + k, N)

    low = (1 - turn) // 2
    rank = low * (S - 1) + turn * sec

    def distant(i):
        other = S - 1 - i - (i + rank) // (S - 1)
        return low * (S - 1) + turn * other

    def place(y):
        return low * (S - 1) + turn * y

    near = range(1, S)
    far = [distant(i) for i in range(S - 1)]
    across = range(1, N)

    def units(p):
        return pl.ds(pl.multiple_of(p * Hs, LANES), Hs)

    def features(p):
        return pl.ds(pl.multiple_of(p * F, F), F)

    def others(ref):
        return ref.at[pl.ds(0, ref.shape[0] - 1)]

    def to_tensor(lane, source, target, cover):
        for k in across:
            send(source(tensor(k)), target, ssem.at[lane], rsem.at[lane], tensor=tensor(k))
        sent.append((cover, lane))

    def to_section(lane, source, target, cover, sem=None):
        for p in far:
            send(
                source(p), target, ssem.at[lane], rsem.at[lane] if sem is None else sem, section=p
            )
        sent.append((cover, lane))

    def to_everyone(lane, source, target, sections):
        for p in sections:
            for j in range(N):
                if p is not sec or j:
                    send(
                        source(p, tensor(j)), target, ssem.at[lane], rsem.at[lane],
                        section=p, tensor=tensor(j),
                    )

    barrier = pltpu.get_barrier_semaphore()
    for k in range(S):
        for j in range(N):
            if k or j:
                pl.semaphore_signal(
                    barrier,
                    inc=1,
                    device_id={"section": section(k), "tensor": tensor(j)},
                    device_id_type=MESH,
                )
    loads = [
        pltpu.make_async_copy(src, dst, load_sem.at[i])
        for src, dst, i in (
            (x_hbm, xg.at[ten], 0), (mg_hbm, gains.at[0], 1), (fg_hbm, gains.at[1], 1),
            (wg_hbm, wgu.at[0], 2), (wu_hbm, wgu.at[1], 2), (wd_hbm, wd, 3),
            (wk_hbm, wkv.at[0], 4), (wv_hbm, wkv.at[1], 4),
            (q_hbm, qc.at[0], 5), (c_hbm, qc.at[1], 5),
        )
    ]
    for load in loads[:6]:
        load.start()
    loads[0].wait()
    with mark("enter"):
        pl.semaphore_wait(barrier, S * N - 1)
    to_tensor(0, lambda p: xg.at[ten], xg.at[ten], others(xg))
    arrive(gains, load_sem.at[1])
    arrive(wgu, load_sem.at[2])
    mg, fg = gains.at[0], gains.at[1]
    wg, wu = wgu.at[0], wgu.at[1]
    wk, wv = wkv.at[0], wkv.at[1]
    with mark("x"):
        arrive(others(xg), rsem.at[0])

    wide = xg[...].reshape(T, F).astype(F32)
    scaled = (wide * mg[...]).astype(BF16)
    square = jnp.sum(wide * wide, axis=1, keepdims=True)
    sqr[sec] = to_row(square, 0)
    to_section(1, lambda p: sqr.at[sec], sqr.at[sec], others(sqr))
    line = S == 4
    for i, p in enumerate(far):
        for side, weight in enumerate((wg, wu)):
            part = jnp.dot(scaled, weight[:, units(p)], preferred_element_type=F32)
            gus[p, side] = part.astype(BF16)
            if line and i == 0:
                hold[side] = part

                @pl.when(rank == 0)
                def _(p=p, side=side):
                    send(
                        gus.at[p, side], stage.at[side], ssem.at[2], psem.at[4, side],
                        section=place(1),
                    )

        if not (line and i == 0):
            send(gus.at[p], gur.at[sec], ssem.at[2], rsem.at[2], section=p)
    sent.append((others(gus), 2))
    for load in loads[6:]:
        load.start()
    gate_pre = jnp.dot(scaled, wg[:, units(sec)], preferred_element_type=F32)
    up_pre = jnp.dot(scaled, wu[:, units(sec)], preferred_element_type=F32)
    if line:
        end = place(S - 1)

        @pl.when(rank == 0)
        def _():
            gur[end] = jnp.zeros(gur.shape[1:], BF16)

        @pl.when(rank == 1)
        def _():
            for side in range(2):
                with mark(f"stage{side}"):
                    arrive(stage.at[side], psem.at[4, side])
                joined[side] = (hold[side] + stage[side].astype(F32)).astype(BF16)
                send(joined.at[side], gur.at[sec, side], ssem.at[2], rsem.at[2], section=end)

    with mark("sq"):
        arrive(others(sqr), rsem.at[1])
    inv = lax.rsqrt(to_column(jnp.sum(sqr[...], axis=0), T, 0) / D + EPSILON)
    normed = (wide * inv * mg[...]).astype(BF16)
    loads[5].wait()
    with mark("gu"):
        if line:
            @pl.when(rank == 0)
            def _():
                arrive(gur.at[pl.ds(0, S - 2)], rsem.at[2])

            @pl.when(rank == 1)
            def _():
                arrive(others(gur), rsem.at[2])
        else:
            arrive(others(gur), rsem.at[2])
    for k in near:
        gate_pre = gate_pre + gur[section(k), 0].astype(F32)
        up_pre = up_pre + gur[section(k), 1].astype(F32)
    gate_pre = gate_pre * inv
    up_pre = up_pre * inv
    sig = jax.nn.sigmoid(gate_pre)
    act = gate_pre * sig
    hid[sec] = (act * up_pre).astype(BF16)
    to_section(3, lambda p: hid.at[sec], hid.at[sec], others(hid), psem.at[0, sec])
    factor = up_pre * (sig * (1.0 + gate_pre * (1.0 - sig)))
    piece = T // 2
    af[sec, 0] = act[:piece].astype(BF16)
    af[sec, 1] = act[piece:].astype(BF16)
    af[sec, 2] = factor[:piece].astype(BF16)
    af[sec, 3] = factor[piece:].astype(BF16)
    comb[...] = act * up_pre + factor * gate_pre
    down = jnp.dot(hid[sec], wd[units(sec), :], preferred_element_type=F32)
    for k in near:
        p = section(k)
        with mark(f"hid{k}"):
            arrive(hid.at[p], psem.at[0, p])
        down = down + jnp.dot(hid[p], wd[units(p), :], preferred_element_type=F32)
    ds[...] = down.reshape(N, tt, F)
    dsb[...] = down.astype(BF16).reshape(N, tt, F)
    to_tensor(4, lambda p: dsb.at[p], dr.at[ten], others(dsb))
    early = lambda p: af.at[p, pl.ds(0, 1)]
    late = lambda p: af.at[p, pl.ds(1, 3)]
    to_section(5, lambda p: early(sec), early(sec), af.at[pl.ds(0, S - 1), pl.ds(0, 1)])
    with mark("ds"):
        arrive(others(dr), rsem.at[4])
    outer = xg[ten].astype(F32) + ds[ten]
    for k in across:
        outer = outer + dr[tensor(k)].astype(F32)
    me = sec * N + ten
    sso[me] = to_row(jnp.sum(outer * outer, axis=1, keepdims=True), ten * tt)
    encb[me] = (outer * fg[...]).astype(BF16)
    to_everyone(6, lambda s, n: sso.at[me], sso.at[me], [*far, sec])
    sent.append((others(sso), 6))
    for p in far:
        send(encb.at[me], encb.at[me], ssem.at[7], psem.at[1, sec], section=p)
    for k in across:
        send(encb.at[me], encb.at[me], ssem.at[7], psem.at[2, sec], tensor=tensor(k))
    for k in near:
        block = section(k) * N + ten
        with mark(f"pass{k}"):
            arrive(encb.at[block], psem.at[1, section(k)])
        for j in across:
            send(
                encb.at[block], encb.at[block], ssem.at[7], psem.at[2, section(k)],
                tensor=tensor(j),
            )
    sent.append((others(encb), 7))
    to_section(8, lambda p: late(sec), late(sec), af.at[pl.ds(0, S - 1), pl.ds(1, 3)])
    arrive(wkv, load_sem.at[4])
    arrive(qc, load_sem.at[5])
    keys = values = None
    for k in range(S):
        p = section(k)
        with mark(f"enc{k}"):
            arrive(encb.at[pl.ds(0, N - 1)], psem.at[2, p])
        block = encb[pl.ds(p * N, N)].reshape(T, F)
        key_part = jnp.dot(block, wk[features(p), :], preferred_element_type=F32)
        value_part = jnp.dot(block, wv[features(p), :], preferred_element_type=F32)
        keys = key_part if keys is None else keys + key_part
        values = value_part if values is None else values + value_part
    with mark("sso"):
        arrive(others(sso), rsem.at[6])
    squares = jnp.sum(sso[...], axis=0)
    inv_all = lax.rsqrt(to_column(squares, T, 0) / D + EPSILON)
    inv_o = lax.rsqrt(to_column(squares, tt, ten * tt) / D + EPSILON)
    keys = (keys * inv_all).astype(BF16)
    values = (values * inv_all).astype(BF16)
    scale = HEAD ** (-0.5)
    key_grads, value_grads = [], []
    inner = None
    for h in range(heads):
        cols = slice(h * HEAD, (h + 1) * HEAD)
        q, c = qc[0, :, cols], qc[1, :, cols]
        scores = lax.dot_general(keys[:, cols], q, COLS, preferred_element_type=F32) * scale
        weights = jnp.exp(scores - jnp.max(scores, axis=0, keepdims=True))
        probs = weights / jnp.sum(weights, axis=0, keepdims=True)
        probs_bf = probs.astype(BF16)
        dprob = lax.dot_general(values[:, cols], c, COLS, preferred_element_type=F32)
        delta = jnp.sum(probs_bf.astype(F32) * dprob, axis=0, keepdims=True)
        dscore = (probs * (dprob - delta) * scale).astype(BF16)
        dsc[h] = dscore
        key_grad = jnp.dot(dscore, q, preferred_element_type=F32).astype(BF16)
        value_grad = jnp.dot(probs_bf, c, preferred_element_type=F32).astype(BF16)
        part = key_grad.astype(F32) * keys[:, cols].astype(F32)
        part += value_grad.astype(F32) * values[:, cols].astype(F32)
        inner = part if inner is None else inner + part
        key_grads.append(key_grad)
        value_grads.append(value_grad)
    key_grad = jnp.concatenate(key_grads, axis=1)
    value_grad = jnp.concatenate(value_grads, axis=1)
    ror[me] = to_row(jnp.sum(inner, axis=1, keepdims=True), 0)
    to_everyone(9, lambda s, n: ror.at[me], ror.at[me], [*far, sec])
    sent.append((others(ror), 9))
    for p in [*far, sec]:
        part = lax.dot_general(key_grad, wk[features(p), :], COLS, preferred_element_type=F32)
        part += lax.dot_general(value_grad, wv[features(p), :], COLS, preferred_element_type=F32)
        egb[pl.ds(p * N, N)] = part.astype(BF16).reshape(N, tt, F)
        to_everyone(10, lambda s, n: egb.at[s * N + n], er.at[me], [p])
    sent.append((others(egb), 10))
    er[me] = egb[me]
    for h in range(heads):
        cols = slice(h * HEAD, (h + 1) * HEAD)
        qg_out[:, cols] = product(dsc[h], keys[:, cols])
    with mark("eg"):
        arrive(others(ror), rsem.at[9])
        arrive(others(er), rsem.at[10])
    inner = to_column(jnp.sum(ror[...], axis=0), tt, ten * tt)
    grad = jnp.sum(er[...].astype(F32), axis=0)
    outer_grad = inv_o * (fg[...] * grad) - outer * (inv_o * inv_o * inner / D)
    oall[ten] = outer_grad.astype(BF16)
    to_tensor(11, lambda p: oall.at[ten], oall.at[ten], others(oall))
    with mark("oall"):
        arrive(others(oall), rsem.at[11])
    grads = oall[...].reshape(T, F)
    for p in far:
        s9[p] = lax.dot_general(
            grads, wd[units(p), :], COLS, preferred_element_type=F32
        ).astype(BF16)
        send(s9.at[p], r9.at[sec], ssem.at[12], rsem.at[12], section=p)
    sent.append((others(s9), 12))
    act_grad = lax.dot_general(grads, wd[units(sec), :], COLS, preferred_element_type=F32)
    for s in range(S):
        dw_out[s * Hs : (s + 1) * Hs, :] = product(hid[s], grads)
    with mark("s9"):
        arrive(others(r9), rsem.at[12])
    for k in near:
        act_grad = act_grad + r9[section(k)].astype(F32)
    aall[sec] = act_grad.astype(BF16)
    to_section(13, lambda p: aall.at[sec], aall.at[sec], others(aall), psem.at[3, sec])
    rir[sec] = to_row(jnp.sum(act_grad * comb[...], axis=1, keepdims=True), 0)
    to_section(14, lambda p: rir.at[sec], rir.at[sec], others(rir))
    with mark("af"):
        arrive(af.at[pl.ds(0, S - 1), pl.ds(0, 1)], rsem.at[5])
        arrive(af.at[pl.ds(0, S - 1), pl.ds(1, 3)], rsem.at[8])
    part = None
    for k in range(S):
        p = section(k)
        if k:
            with mark(f"aall{k}"):
                arrive(aall.at[p], psem.at[3, p])
        act_grad = aall[p].astype(F32)
        factors = af[p].reshape(2, T, Hs)
        up_grad = (act_grad * factors[0].astype(F32)).astype(BF16)
        gate_grad = (act_grad * factors[1].astype(F32)).astype(BF16)
        up[p] = up_grad
        gate[p] = gate_grad
        more = lax.dot_general(gate_grad, wg[:, units(p)], COLS, preferred_element_type=F32)
        more += lax.dot_general(up_grad, wu[:, units(p)], COLS, preferred_element_type=F32)
        part = more if part is None else part + more
    s11[...] = part.reshape(N, tt, F)
    s11b[...] = part.astype(BF16).reshape(N, tt, F)
    to_tensor(15, lambda p: s11b.at[p], r11.at[ten], others(s11b))
    with mark("rir"):
        arrive(others(rir), rsem.at[14])
    rit[ten] = jnp.sum(rir[...], axis=0)
    to_tensor(16, lambda p: rit.at[ten], rit.at[ten], others(rit))
    for s in range(S):
        cols = slice(s * Hs, (s + 1) * Hs)
        gw_out[:, cols] = product(normed, gate[s])
        uw_out[:, cols] = product(normed, up[s])
    with mark("s11"):
        arrive(others(r11), rsem.at[15])
        arrive(others(rit), rsem.at[16])
    hidden = xg[ten].astype(F32)
    scaled_in = s11[ten]
    for k in across:
        scaled_in = scaled_in + r11[tensor(k)].astype(F32)
    scaled_in = mg[...] * scaled_in
    inner = to_column(jnp.sum(rit[...], axis=0), tt, ten * tt)
    squares = to_column(jnp.sum(sqr[...], axis=0), tt, ten * tt)
    inv_in = lax.rsqrt(squares / D + EPSILON)
    hg_out[...] = outer_grad + inv_in * scaled_in - hidden * (inv_in * inv_in * inner / D)
    with mark("end"):
        for cover, lane in sent:
            arrive(cover, ssem.at[lane])


def write_kernel(*refs):
    count = len(refs) // 2
    sem = refs[-1]
    copies = [
        pltpu.make_async_copy(refs[i], refs[count + i], sem.at[i]) for i in range(count)
    ]
    for copy in copies:
        copy.start()
    for copy in copies:
        copy.wait()


def fast(
    S, N, enc_hidden, mlp_gain, final_gain, w_gate, w_up, w_down, key_weight, value_weight,
    queries, context_grad,
):
    tt, F = enc_hidden.shape
    T = N * tt
    H = w_gate.shape[1]
    Hs = H // S
    vmem = pl.BlockSpec(memory_space=pltpu.VMEM)
    hbm = pl.BlockSpec(memory_space=pltpu.HBM)
    shape = jax.ShapeDtypeStruct
    dma = pltpu.SemaphoreType.DMA
    wk, wv, q, c = key_weight[0], value_weight[0], queries[0], context_grad[0]
    rows, width = q.shape
    heads = width // HEAD
    buf = lambda *dims: pltpu.VMEM(dims, BF16)
    wide = lambda *dims: pltpu.VMEM(dims, F32)
    scratch = [
        wide(2, 1, F), buf(2, F, H), buf(H, F), buf(2, *wk.shape), buf(2, rows, width),
        buf(N, tt, F),
        wide(S, 1, LANES),
        buf(S, 2, T, Hs),
        buf(S, 2, T, Hs),
        wide(2, T, Hs),
        buf(2, T, Hs),
        buf(2, T, Hs),
        buf(S, T, Hs),
        buf(S, 4, T // 2, Hs),
        wide(T, Hs),
        wide(N, tt, F),
        buf(N, tt, F),
        buf(N, tt, F),
        buf(S * N, tt, F),
        wide(S * N, 1, LANES),
        buf(S * N, tt, F),
        buf(S * N, tt, F),
        wide(S * N, 1, LANES),
        buf(N, tt, F),
        buf(S, T, Hs),
        buf(S, T, Hs),
        buf(S, T, Hs),
        wide(S, 1, LANES),
        buf(S, T, Hs),
        buf(S, T, Hs),
        wide(N, tt, F),
        buf(N, tt, F),
        buf(N, tt, F),
        wide(N, 1, LANES),
        buf(heads, T, rows),
        dma((6,)), dma((17,)), dma((17,)), dma((5, S)),
    ]
    results = [
        ((tt, F), F32), ((rows, width), BF16), ((F, H), BF16), ((F, H), BF16), ((H, F), BF16)
    ]
    made = pl.pallas_call(
        functools.partial(chain_kernel, S, N),
        out_shape=[pltpu.VMEM(*result) for result in results],
        in_specs=[hbm] * 10,
        out_specs=[vmem] * 5,
        scratch_shapes=scratch,
        compiler_params=pltpu.CompilerParams(
            collective_id=0, has_side_effects=True, vmem_limit_bytes=CHAIN_VMEM_LIMIT
        ),
    )(enc_hidden, mlp_gain[None, :], final_gain[None, :], w_gate, w_up, w_down, wk, wv, q, c)
    hidden_grad, query_grad, gate_grad, up_grad, down_grad = pl.pallas_call(
        write_kernel,
        out_shape=[shape(*result) for result in results],
        in_specs=[vmem] * 5,
        out_specs=[hbm] * 5,
        scratch_shapes=[dma((5,))],
        compiler_params=pltpu.CompilerParams(vmem_limit_bytes=WRITE_VMEM_LIMIT),
    )(*made)
    return query_grad[None, :, :], hidden_grad, gate_grad, up_grad, down_grad


def on_device(S, N, enc_hidden, mlp_gain, final_gain, w_gate, *rest):
    tt, F = enc_hidden.shape
    Hs = w_gate.shape[1] // S
    fits = Hs % LANES == 0 and F % LANES == 0 and tt % 16 == 0 and N * tt <= LANES
    run = fast if fits else general
    return run(S, N, enc_hidden, mlp_gain, final_gain, w_gate, *rest)


def solution(mesh):
    in_specs = (
        P(("dp", "tensor"), "section"),
        P("section"),
        P("section"),
        P("section", "tensor"),
        P("section", "tensor"),
        P("tensor", "section"),
        P("section", None, "tensor"),
        P("section", None, "tensor"),
        P("section", "dp", "tensor"),
        P("section", "dp", "tensor"),
    )
    out_specs = (
        P("section", "dp", "tensor"),
        P(("dp", "tensor"), "section"),
        P(("dp", "section"), "tensor"),
        P(("dp", "section"), "tensor"),
        P(("dp", "tensor"), "section"),
    )
    body = functools.partial(on_device, mesh.shape["section"], mesh.shape["tensor"])
    return jax.shard_map(
        body, mesh=mesh, in_specs=in_specs, out_specs=out_specs, check_vma=False
    )
```

```python
import contextlib
import functools
import jax
import jax.numpy as jnp
from jax import lax
from jax.experimental import pallas as pl
from jax.experimental.pallas import tpu as pltpu
from jax.sharding import PartitionSpec as P

HEAD = 256
EPSILON = 1e-06
LANES = 128
MESH = pl.DeviceIdType.MESH
VMEM_LIMIT = 58 * 1024 * 1024
CHAIN_VMEM_LIMIT = 54 * 1024 * 1024
WRITE_VMEM_LIMIT = 4 * 1024 * 1024
ROWS = (((0,), (0,)), ((), ()))
COLS = (((1,), (1,)), ((), ()))
F32 = jnp.float32
BF16 = jnp.bfloat16


def mark(name):
    return contextlib.nullcontext()


def enter(sizes):
    barrier = pltpu.get_barrier_semaphore()
    for axis, n in sizes:
        me = lax.axis_index(axis)
        for k in range(1, n):
            pl.semaphore_signal(
                barrier, inc=1, device_id={axis: lax.rem(me + k, n)}, device_id_type=MESH
            )
    pl.semaphore_wait(barrier, sum(n - 1 for _, n in sizes))


def post(axis, n, source, target, send_sem, recv_sem):
    me = lax.axis_index(axis)
    copies = []
    for k in range(1, n):
        peer = lax.rem(me + k, n)
        copy = pltpu.make_async_remote_copy(
            src_ref=source(peer),
            dst_ref=target(k - 1),
            send_sem=send_sem.at[k - 1],
            recv_sem=recv_sem.at[k - 1],
            device_id={axis: peer},
            device_id_type=MESH,
        )
        copy.start()
        copies.append(copy)
    return copies


def gather(axis, n, ref, send_sem, recv_sem):
    me = lax.axis_index(axis)
    return post(axis, n, lambda peer: ref.at[me], lambda k: ref.at[me], send_sem, recv_sem)


def scatter(axis, n, out, into, send_sem, recv_sem):
    return post(axis, n, lambda peer: out.at[peer], lambda k: into.at[k], send_sem, recv_sem)


def finish(*groups):
    for copies in groups:
        for copy in copies:
            copy.wait()


def total(own, into, n):
    acc = own.astype(F32)
    for k in range(n - 1):
        acc = acc + into[k].astype(F32)
    return acc


def attend(keys, values, q, c):
    scale = HEAD ** (-0.5)
    scores = lax.dot_general(keys, q, COLS, preferred_element_type=F32) * scale
    weights = jnp.exp(scores - jnp.max(scores, axis=0, keepdims=True))
    probs = weights / jnp.sum(weights, axis=0, keepdims=True)
    probs_bf = probs.astype(BF16)
    dprob = lax.dot_general(values, c, COLS, preferred_element_type=F32)
    delta = jnp.sum(probs_bf.astype(F32) * dprob, axis=0, keepdims=True)
    dscore = (probs * (dprob - delta) * scale).astype(BF16)
    query_grad = lax.dot_general(dscore, keys, ROWS, preferred_element_type=F32).astype(BF16)
    key_grad = jnp.dot(dscore, q, preferred_element_type=F32).astype(BF16)
    value_grad = jnp.dot(probs_bf, c, preferred_element_type=F32).astype(BF16)
    return query_grad, key_grad, value_grad


def step_kernel(
    S, N, x_ref, mg_ref, fg_ref, wg_hbm, wu_hbm, wd_hbm, wk_hbm, wv_hbm, q_hbm, c_hbm,
    qg_hbm, hg_out, normed_out, hid_out, oall_out, gate_out, up_out,
    wg, wu, wd, wk, wv, q, c, qg,
    xg, sqs, sqr, gus, gur, hid_all, inv_all, ds, dr, feat, sqo, enc, af, eg,
    r6, s6, r6b, pin, oall, s9, r9, aall, s11, r11, pin2,
    load_sem, store_sem, ssem, rsem,
):
    tt, F = x_ref.shape
    T = N * tt
    ts = T // S
    H = wg.shape[1]
    D = F * S
    heads = q.shape[1] // HEAD
    sec = lax.axis_index("section")
    ten = lax.axis_index("tensor")
    loads = [
        pltpu.make_async_copy(src, dst, load_sem.at[i])
        for i, (src, dst) in enumerate((
            (wg_hbm, wg), (wu_hbm, wu), (wd_hbm, wd), (wk_hbm, wk), (wv_hbm, wv),
            (q_hbm, q), (c_hbm, c),
        ))
    ]
    for load in loads[:3]:
        load.start()
    xg[ten] = x_ref[...]
    enter((("section", S), ("tensor", N)))
    finish(post("tensor", N, lambda p: x_ref, lambda k: xg.at[ten], ssem.at[0], rsem.at[0]))
    wide = xg[...].reshape(T, F).astype(F32)
    scaled = (wide * mg_ref[...]).astype(BF16)
    square = jnp.sum(wide * wide, axis=1, keepdims=True)
    sqs[...] = jnp.broadcast_to(square, (T, LANES)).reshape(S, ts, LANES)
    loads[0].wait()
    gus[0] = jnp.dot(scaled, wg[...], preferred_element_type=F32).astype(BF16).reshape(S, ts, H)
    move_q = scatter("section", S, sqs, sqr, ssem.at[3], rsem.at[3])
    move_g = scatter("section", S, gus.at[0], gur.at[0], ssem.at[1], rsem.at[1])
    loads[1].wait()
    gus[1] = jnp.dot(scaled, wu[...], preferred_element_type=F32).astype(BF16).reshape(S, ts, H)
    move_u = scatter("section", S, gus.at[1], gur.at[1], ssem.at[2], rsem.at[2])
    for load in loads[3:]:
        load.start()
    finish(move_q, move_g)
    inv = lax.rsqrt(total(sqs[sec], sqr, S) / D + EPSILON)
    inv_all[sec] = inv
    inv = inv[:, :1]
    gate_pre = total(gus[0, sec], gur.at[0], S) * inv
    sig = jax.nn.sigmoid(gate_pre)
    act = gate_pre * sig
    af[0, sec] = act.astype(BF16)
    slope = sig * (1.0 + gate_pre * (1.0 - sig))
    finish(move_u)
    up_pre = total(gus[1, sec], gur.at[1], S) * inv
    hid_all[sec] = (act * up_pre).astype(BF16)
    move_h = gather("section", S, hid_all, ssem.at[4], rsem.at[4])
    move_i = gather("section", S, inv_all, ssem.at[5], rsem.at[5])
    af[1, sec] = (up_pre * slope).astype(BF16)
    loads[2].wait()
    finish(move_h)
    hid = hid_all[...].reshape(T, H)
    ds[...] = jnp.dot(hid, wd[...], preferred_element_type=F32).astype(BF16).reshape(N, tt, F)
    move_d = scatter("tensor", N, ds, dr, ssem.at[6], rsem.at[6])
    hid_out[...] = hid
    finish(move_i)
    inv_tok = inv_all[...].reshape(T, LANES)
    normed_out[...] = (wide * inv_tok[:, :1] * mg_ref[...]).astype(BF16)
    finish(move_d)
    outer = x_ref[...].astype(F32) + total(ds[ten], dr, N)
    feat[sec] = (outer * fg_ref[...]).astype(BF16)
    sqo[sec] = jnp.broadcast_to(jnp.sum(outer * outer, axis=1, keepdims=True), (tt, LANES))
    move_s = gather("section", S, sqo, ssem.at[8], rsem.at[8])
    move_f = gather("section", S, feat, ssem.at[7], rsem.at[7])
    finish(move_s, move_f)
    move_act = gather("section", S, af.at[0], ssem.at[10], rsem.at[10])
    move_fac = gather("section", S, af.at[1], ssem.at[11], rsem.at[11])
    inv_o = lax.rsqrt(jnp.sum(sqo[...], axis=0) / D + EPSILON)
    enc[ten] = (feat[...].astype(F32) * inv_o[None, :, :1]).astype(BF16)
    inv_o = inv_o[:, :1]
    move_e = gather("tensor", N, enc, ssem.at[9], rsem.at[9])
    for load in loads[3:]:
        load.wait()
    finish(move_e)

    width = heads * HEAD
    keys = jnp.zeros((T, width), F32)
    values = jnp.zeros((T, width), F32)
    for s in range(S):
        block = enc[:, s].reshape(T, F)
        keys += jnp.dot(block, wk[s * F : (s + 1) * F, :], preferred_element_type=F32)
        values += jnp.dot(block, wv[s * F : (s + 1) * F, :], preferred_element_type=F32)
    keys = keys.astype(BF16)
    values = values.astype(BF16)
    key_grads, value_grads, stores = [], [], []
    for h in range(heads):
        cols = slice(h * HEAD, (h + 1) * HEAD)
        query_grad, key_grad, value_grad = attend(
            keys[:, cols], values[:, cols], q[:, cols], c[:, cols]
        )
        qg[h] = query_grad
        store = pltpu.make_async_copy(qg.at[h], qg_hbm.at[:, cols], store_sem.at[h])
        store.start()
        stores.append(store)
        key_grads.append(key_grad)
        value_grads.append(value_grad)
    key_grad = jnp.concatenate(key_grads, axis=1)
    value_grad = jnp.concatenate(value_grads, axis=1)
    for s in range(S):
        rows = slice(s * F, (s + 1) * F)
        part = lax.dot_general(key_grad, wk[rows, :], COLS, preferred_element_type=F32)
        part += lax.dot_general(value_grad, wv[rows, :], COLS, preferred_element_type=F32)
        eg[:, s] = part.astype(BF16).reshape(N, tt, F)

    finish(scatter("tensor", N, eg, r6, ssem.at[12], rsem.at[12]))
    s6[...] = total(eg[ten], r6, N).astype(BF16)
    finish(scatter("section", S, s6, r6b, ssem.at[13], rsem.at[13]))
    scaled_out = fg_ref[...] * total(s6[sec], r6b, S)
    pin[sec] = jnp.broadcast_to(
        jnp.sum(scaled_out * outer, axis=1, keepdims=True), (tt, LANES)
    )
    finish(gather("section", S, pin, ssem.at[14], rsem.at[14]))
    inner = jnp.sum(pin[...], axis=0)[:, :1] / D
    outer_grad = inv_o * scaled_out - outer * (inv_o * inv_o * inv_o * inner)
    oall[ten] = outer_grad.astype(BF16)
    finish(gather("tensor", N, oall, ssem.at[15], rsem.at[15]))
    grads = oall[...].reshape(T, F)
    half = H // 2
    moves = []
    for i in range(2):
        s9[i] = (
            lax.dot_general(
                grads, wd[i * half : (i + 1) * half, :], COLS, preferred_element_type=F32
            )
            .astype(BF16)
            .reshape(S, ts, half)
        )
        moves.append(scatter("section", S, s9.at[i], r9.at[i], ssem.at[16 + i], rsem.at[16 + i]))
    oall_out[...] = grads
    finish(move_act, move_fac)
    gathers = []
    for i in range(2):
        finish(moves[i])
        aall[i, sec] = total(s9[i, sec], r9.at[i], S).astype(BF16)
        gathers.append(gather("section", S, aall.at[i], ssem.at[18 + i], rsem.at[18 + i]))
    parts = None
    for i in range(2):
        cols = slice(i * half, (i + 1) * half)
        finish(gathers[i])
        act_grad = aall[i].reshape(T, half).astype(F32)
        up_grad = (act_grad * af[0, :, :, cols].reshape(T, half).astype(F32)).astype(BF16)
        gate_grad = (act_grad * af[1, :, :, cols].reshape(T, half).astype(F32)).astype(BF16)
        up_out[:, cols] = up_grad
        gate_out[:, cols] = gate_grad
        part = lax.dot_general(gate_grad, wg[:, cols], COLS, preferred_element_type=F32)
        part += lax.dot_general(up_grad, wu[:, cols], COLS, preferred_element_type=F32)
        parts = part if parts is None else parts + part
    s11[...] = parts.astype(BF16).reshape(N, tt, F)
    finish(scatter("tensor", N, s11, r11, ssem.at[20], rsem.at[20]))
    hidden = x_ref[...].astype(F32)
    scaled_in = mg_ref[...] * total(s11[ten], r11, N)
    pin2[sec] = jnp.broadcast_to(
        jnp.sum(scaled_in * hidden, axis=1, keepdims=True), (tt, LANES)
    )
    finish(gather("section", S, pin2, ssem.at[21], rsem.at[21]))
    inner_in = jnp.sum(pin2[...], axis=0)[:, :1] / D
    inv_flat = inv_all.reshape(T, LANES)
    inv_in = inv_flat[pl.ds(pl.multiple_of(ten * tt, tt), tt), :][:, :1]
    hg_out[...] = (
        outer_grad + inv_in * scaled_in - hidden * (inv_in * inv_in * inv_in * inner_in)
    )
    for store in stores:
        store.wait()


def general(
    S, N, enc_hidden, mlp_gain, final_gain, w_gate, w_up, w_down, key_weight, value_weight,
    queries, context_grad,
):
    tt, F = enc_hidden.shape
    T = N * tt
    ts = T // S
    H = w_gate.shape[1]
    peers = max(S, N) - 1
    vmem = pl.BlockSpec(memory_space=pltpu.VMEM)
    hbm = pl.BlockSpec(memory_space=pl.ANY)
    shape = jax.ShapeDtypeStruct
    dma = pltpu.SemaphoreType.DMA
    wk, wv, q, c = key_weight[0], value_weight[0], queries[0], context_grad[0]
    large = (w_gate, w_up, w_down, wk, wv, q, c)
    rows = q.shape[0]
    heads = q.shape[1] // HEAD
    scratch = [pltpu.VMEM(w.shape, BF16) for w in large]
    scratch += [
        pltpu.VMEM((heads, rows, HEAD), BF16),
        pltpu.VMEM((N, tt, F), BF16),
        pltpu.VMEM((S, ts, LANES), F32),
        pltpu.VMEM((S - 1, ts, LANES), F32),
        pltpu.VMEM((2, S, ts, H), BF16),
        pltpu.VMEM((2, S - 1, ts, H), BF16),
        pltpu.VMEM((S, ts, H), BF16),
        pltpu.VMEM((S, ts, LANES), F32),
        pltpu.VMEM((N, tt, F), BF16),
        pltpu.VMEM((N - 1, tt, F), BF16),
        pltpu.VMEM((S, tt, F), BF16),
        pltpu.VMEM((S, tt, LANES), F32),
        pltpu.VMEM((N, S, tt, F), BF16),
        pltpu.VMEM((2, S, ts, H), BF16),
        pltpu.VMEM((N, S, tt, F), BF16),
        pltpu.VMEM((N - 1, S, tt, F), BF16),
        pltpu.VMEM((S, tt, F), BF16),
        pltpu.VMEM((S - 1, tt, F), BF16),
        pltpu.VMEM((S, tt, LANES), F32),
        pltpu.VMEM((N, tt, F), BF16),
        pltpu.VMEM((2, S, ts, H // 2), BF16),
        pltpu.VMEM((2, S - 1, ts, H // 2), BF16),
        pltpu.VMEM((2, S, ts, H // 2), BF16),
        pltpu.VMEM((N, tt, F), BF16),
        pltpu.VMEM((N - 1, tt, F), BF16),
        pltpu.VMEM((S, tt, LANES), F32),
        dma((7,)), dma((heads,)), dma((22, peers)), dma((22, peers)),
    ]
    query_grad, hidden_grad, normed, hid, outer_all, gate_all, up_all = pl.pallas_call(
        functools.partial(step_kernel, S, N),
        out_shape=[
            shape(q.shape, BF16), shape((tt, F), F32), shape((T, F), BF16),
            shape((T, H), BF16), shape((T, F), BF16), shape((T, H), BF16), shape((T, H), BF16),
        ],
        in_specs=[vmem] * 3 + [hbm] * 7,
        out_specs=[hbm] + [vmem] * 6,
        scratch_shapes=scratch,
        compiler_params=pltpu.CompilerParams(
            collective_id=0, has_side_effects=True, vmem_limit_bytes=VMEM_LIMIT
        ),
    )(enc_hidden, mlp_gain[None, :], final_gain[None, :], *large)

    outer_product = lambda a, b: lax.dot_general(
        a, b, ROWS, preferred_element_type=F32
    ).astype(BF16)
    return (
        query_grad[None, :, :],
        hidden_grad,
        outer_product(normed, gate_all),
        outer_product(normed, up_all),
        outer_product(hid, outer_all),
    )


def lane_of_row(rows, offset):
    row = lax.broadcasted_iota(jnp.int32, (rows, LANES), 0) + offset
    return (row == lax.broadcasted_iota(jnp.int32, (rows, LANES), 1)).astype(F32)


def to_row(column, offset):
    return jnp.sum(column * lane_of_row(column.shape[0], offset), axis=0, keepdims=True)


def to_column(row, rows, offset):
    return jnp.sum(row * lane_of_row(rows, offset), axis=1, keepdims=True)


def send(source, target, send_sem, recv_sem, **peer):
    pltpu.make_async_remote_copy(
        src_ref=source,
        dst_ref=target,
        send_sem=send_sem,
        recv_sem=recv_sem,
        device_id=peer,
        device_id_type=MESH,
    ).start()


def arrive(cover, sem):
    pltpu.make_async_copy(cover, cover, sem).wait()


def product(a, b):
    return lax.dot_general(a, b, ROWS, preferred_element_type=F32).astype(BF16)


def chain_kernel(
    S, N, G, x_hbm, mg_hbm, fg_hbm, wg_hbm, wu_hbm, wd_hbm, wk_hbm, wv_hbm, q_hbm, c_hbm,
    hg_out, qg_out, gw_out, uw_out, dw_out,
    gains, wgu, wd, wkv, qc,
    xg, sqr, gus, gur, hold, stage, joined, hid, af, afg, comb, combg, ds, dsb, dr, encb, sso, egb, er, ror, oall, oallg,
    s9, r9, aall, rir, gateg, upg, gate, up, s11b, r11, rits, rit, dsc,
    load_sem, ssem, rsem, psem,
):
    tt, F = x_hbm.shape
    T = N * tt
    H = wd.shape[0]
    Hs = H // S
    D = F * S
    heads = qc.shape[2] // HEAD
    sec = lax.axis_index("section")
    ten = lax.axis_index("tensor")
    partner = lax.rem(lax.axis_index("dp") + 1, G)
    turn = 1 - 2 * (sec // ((S + 1) // 2))
    sent = []

    def section(k):
        return lax.rem(sec + turn * k + S, S)

    def tensor(k):
        return lax.rem(ten + k, N)

    low = (1 - turn) // 2
    rank = low * (S - 1) + turn * sec

    def distant(i):
        other = S - 1 - i - (i + rank) // (S - 1)
        return low * (S - 1) + turn * other

    def place(y):
        return low * (S - 1) + turn * y

    near = range(1, S)
    far = [distant(i) for i in range(S - 1)]
    across = range(1, N)

    def units(p):
        return pl.ds(pl.multiple_of(p * Hs, LANES), Hs)

    def features(p):
        return pl.ds(pl.multiple_of(p * F, F), F)

    def others(ref):
        return ref.at[pl.ds(0, ref.shape[0] - 1)]

    def to_tensor(lane, source, target, cover):
        for k in across:
            send(source(tensor(k)), target, ssem.at[lane], rsem.at[lane], tensor=tensor(k))
        sent.append((cover, lane))

    def to_section(lane, source, target, cover, sem=None):
        for p in far:
            send(
                source(p), target, ssem.at[lane], rsem.at[lane] if sem is None else sem, section=p
            )
        sent.append((cover, lane))

    def to_everyone(lane, source, target, sections):
        for p in sections:
            for j in range(N):
                if p is not sec or j:
                    send(
                        source(p, tensor(j)), target, ssem.at[lane], rsem.at[lane],
                        section=p, tensor=tensor(j),
                    )

    barrier = pltpu.get_barrier_semaphore()
    for k in range(S):
        for j in range(N):
            if k or j:
                pl.semaphore_signal(
                    barrier,
                    inc=1,
                    device_id={"section": section(k), "tensor": tensor(j)},
                    device_id_type=MESH,
                )
    crossed = [(p, ten) for p in [sec, *far]] + [(sec, tensor(j)) for j in across]
    for p, n in crossed:
        pl.semaphore_signal(
            barrier,
            inc=1,
            device_id={"section": p, "tensor": n, "dp": partner},
            device_id_type=MESH,
        )
    loads = [
        pltpu.make_async_copy(src, dst, load_sem.at[i])
        for src, dst, i in (
            (x_hbm, xg.at[ten], 0), (mg_hbm, gains.at[0], 1), (fg_hbm, gains.at[1], 1),
            (wg_hbm, wgu.at[0], 2), (wu_hbm, wgu.at[1], 2), (wd_hbm, wd, 3),
            (wk_hbm, wkv.at[0], 4), (wv_hbm, wkv.at[1], 4),
            (q_hbm, qc.at[0], 5), (c_hbm, qc.at[1], 5),
        )
    ]
    for load in loads[:6]:
        load.start()
    loads[0].wait()
    with mark("enter"):
        pl.semaphore_wait(barrier, S * N - 1 + len(crossed))
    to_tensor(0, lambda p: xg.at[ten], xg.at[ten], others(xg))
    arrive(gains, load_sem.at[1])
    arrive(wgu, load_sem.at[2])
    mg, fg = gains.at[0], gains.at[1]
    wg, wu = wgu.at[0], wgu.at[1]
    wk, wv = wkv.at[0], wkv.at[1]
    with mark("x"):
        arrive(others(xg), rsem.at[0])

    wide = xg[...].reshape(T, F).astype(F32)
    scaled = (wide * mg[...]).astype(BF16)
    square = jnp.sum(wide * wide, axis=1, keepdims=True)
    sqr[sec] = to_row(square, 0)
    to_section(1, lambda p: sqr.at[sec], sqr.at[sec], others(sqr))
    line = S == 4
    for i, p in enumerate(far):
        for side, weight in enumerate((wg, wu)):
            part = jnp.dot(scaled, weight[:, units(p)], preferred_element_type=F32)
            gus[p, side] = part.astype(BF16)
            if line and i == 0:
                hold[side] = part

                @pl.when(rank == 0)
                def _(p=p, side=side):
                    send(
                        gus.at[p, side], stage.at[side], ssem.at[2], psem.at[4, side],
                        section=place(1),
                    )

        if not (line and i == 0):
            send(gus.at[p], gur.at[sec], ssem.at[2], rsem.at[2], section=p)
    sent.append((others(gus), 2))
    for load in loads[6:]:
        load.start()
    gate_pre = jnp.dot(scaled, wg[:, units(sec)], preferred_element_type=F32)
    up_pre = jnp.dot(scaled, wu[:, units(sec)], preferred_element_type=F32)
    if line:
        end = place(S - 1)

        @pl.when(rank == 0)
        def _():
            gur[end] = jnp.zeros(gur.shape[1:], BF16)

        @pl.when(rank == 1)
        def _():
            for side in range(2):
                with mark(f"stage{side}"):
                    arrive(stage.at[side], psem.at[4, side])
                joined[side] = (hold[side] + stage[side].astype(F32)).astype(BF16)
                send(joined.at[side], gur.at[sec, side], ssem.at[2], rsem.at[2], section=end)

    with mark("sq"):
        arrive(others(sqr), rsem.at[1])
    inv = lax.rsqrt(to_column(jnp.sum(sqr[...], axis=0), T, 0) / D + EPSILON)
    normed = (wide * inv * mg[...]).astype(BF16)
    loads[5].wait()
    with mark("gu"):
        if line:
            @pl.when(rank == 0)
            def _():
                arrive(gur.at[pl.ds(0, S - 2)], rsem.at[2])

            @pl.when(rank == 1)
            def _():
                arrive(others(gur), rsem.at[2])
        else:
            arrive(others(gur), rsem.at[2])
    for k in near:
        gate_pre = gate_pre + gur[section(k), 0].astype(F32)
        up_pre = up_pre + gur[section(k), 1].astype(F32)
    gate_pre = gate_pre * inv
    up_pre = up_pre * inv
    sig = jax.nn.sigmoid(gate_pre)
    act = gate_pre * sig
    hid[sec] = (act * up_pre).astype(BF16)
    to_section(3, lambda p: hid.at[sec], hid.at[sec], others(hid), psem.at[0, sec])
    factor = up_pre * (sig * (1.0 + gate_pre * (1.0 - sig)))
    piece = T // 2
    af[0] = act[:piece].astype(BF16)
    af[1] = act[piece:].astype(BF16)
    af[2] = factor[:piece].astype(BF16)
    af[3] = factor[piece:].astype(BF16)
    comb[...] = act * up_pre + factor * gate_pre
    send(comb, combg, ssem.at[17], rsem.at[17], dp=partner)
    sent.append((comb, 17))
    down = jnp.dot(hid[sec], wd[units(sec), :], preferred_element_type=F32)
    for k in near:
        p = section(k)
        with mark(f"hid{k}"):
            arrive(hid.at[p], psem.at[0, p])
        down = down + jnp.dot(hid[p], wd[units(p), :], preferred_element_type=F32)
    ds[...] = down.reshape(N, tt, F)
    dsb[...] = down.astype(BF16).reshape(N, tt, F)
    to_tensor(4, lambda p: dsb.at[p], dr.at[ten], others(dsb))
    early, late = pl.ds(0, 1), pl.ds(1, 3)

    def share_factors(lane, pieces):
        for p in [*far, sec]:
            send(
                af.at[pieces], afg.at[sec, pieces], ssem.at[lane], rsem.at[lane],
                section=p, dp=partner,
            )
        sent.append((afg.at[:, pieces], lane))

    share_factors(5, early)
    with mark("ds"):
        arrive(others(dr), rsem.at[4])
    outer = xg[ten].astype(F32) + ds[ten]
    for k in across:
        outer = outer + dr[tensor(k)].astype(F32)
    me = sec * N + ten
    sso[me] = to_row(jnp.sum(outer * outer, axis=1, keepdims=True), ten * tt)
    encb[me] = (outer * fg[...]).astype(BF16)
    to_everyone(6, lambda s, n: sso.at[me], sso.at[me], [*far, sec])
    sent.append((others(sso), 6))
    for p in far:
        send(encb.at[me], encb.at[me], ssem.at[7], psem.at[1, sec], section=p)
    for k in across:
        send(encb.at[me], encb.at[me], ssem.at[7], psem.at[2, sec], tensor=tensor(k))
    for k in near:
        block = section(k) * N + ten
        with mark(f"pass{k}"):
            arrive(encb.at[block], psem.at[1, section(k)])
        for j in across:
            send(
                encb.at[block], encb.at[block], ssem.at[7], psem.at[2, section(k)],
                tensor=tensor(j),
            )
    sent.append((others(encb), 7))
    share_factors(8, late)
    arrive(wkv, load_sem.at[4])
    arrive(qc, load_sem.at[5])
    keys = values = None
    for k in range(S):
        p = section(k)
        with mark(f"enc{k}"):
            arrive(encb.at[pl.ds(0, N - 1)], psem.at[2, p])
        block = encb[pl.ds(p * N, N)].reshape(T, F)
        key_part = jnp.dot(block, wk[features(p), :], preferred_element_type=F32)
        value_part = jnp.dot(block, wv[features(p), :], preferred_element_type=F32)
        keys = key_part if keys is None else keys + key_part
        values = value_part if values is None else values + value_part
    with mark("sso"):
        arrive(others(sso), rsem.at[6])
    squares = jnp.sum(sso[...], axis=0)
    inv_all = lax.rsqrt(to_column(squares, T, 0) / D + EPSILON)
    inv_o = lax.rsqrt(to_column(squares, tt, ten * tt) / D + EPSILON)
    keys = (keys * inv_all).astype(BF16)
    values = (values * inv_all).astype(BF16)
    scale = HEAD ** (-0.5)
    key_grads, value_grads = [], []
    inner = None
    for h in range(heads):
        cols = slice(h * HEAD, (h + 1) * HEAD)
        q, c = qc[0, :, cols], qc[1, :, cols]
        scores = lax.dot_general(keys[:, cols], q, COLS, preferred_element_type=F32) * scale
        weights = jnp.exp(scores - jnp.max(scores, axis=0, keepdims=True))
        probs = weights / jnp.sum(weights, axis=0, keepdims=True)
        probs_bf = probs.astype(BF16)
        dprob = lax.dot_general(values[:, cols], c, COLS, preferred_element_type=F32)
        delta = jnp.sum(probs_bf.astype(F32) * dprob, axis=0, keepdims=True)
        dscore = (probs * (dprob - delta) * scale).astype(BF16)
        dsc[h] = dscore
        key_grad = jnp.dot(dscore, q, preferred_element_type=F32).astype(BF16)
        value_grad = jnp.dot(probs_bf, c, preferred_element_type=F32).astype(BF16)
        part = key_grad.astype(F32) * keys[:, cols].astype(F32)
        part += value_grad.astype(F32) * values[:, cols].astype(F32)
        inner = part if inner is None else inner + part
        key_grads.append(key_grad)
        value_grads.append(value_grad)
    key_grad = jnp.concatenate(key_grads, axis=1)
    value_grad = jnp.concatenate(value_grads, axis=1)
    ror[me] = to_row(jnp.sum(inner, axis=1, keepdims=True), 0)
    to_everyone(9, lambda s, n: ror.at[me], ror.at[me], [*far, sec])
    sent.append((others(ror), 9))
    for p in [*far, sec]:
        part = lax.dot_general(key_grad, wk[features(p), :], COLS, preferred_element_type=F32)
        part += lax.dot_general(value_grad, wv[features(p), :], COLS, preferred_element_type=F32)
        egb[pl.ds(p * N, N)] = part.astype(BF16).reshape(N, tt, F)
        to_everyone(10, lambda s, n: egb.at[s * N + n], er.at[me], [p])
    sent.append((others(egb), 10))
    er[me] = egb[me]
    for h in range(heads):
        cols = slice(h * HEAD, (h + 1) * HEAD)
        qg_out[:, cols] = product(dsc[h], keys[:, cols])
    with mark("eg"):
        arrive(others(ror), rsem.at[9])
        arrive(others(er), rsem.at[10])
    inner = to_column(jnp.sum(ror[...], axis=0), tt, ten * tt)
    grad = jnp.sum(er[...].astype(F32), axis=0)
    outer_grad = inv_o * (fg[...] * grad) - outer * (inv_o * inv_o * inner / D)
    oall[ten] = outer_grad.astype(BF16)
    for k in range(N):
        send(
            oall.at[ten], oallg.at[ten], ssem.at[18], rsem.at[18], tensor=tensor(k), dp=partner
        )
    sent.append((oall, 18))
    to_tensor(11, lambda p: oall.at[ten], oall.at[ten], others(oall))
    with mark("oall"):
        arrive(oallg, rsem.at[18])
    grads = oallg[...].reshape(T, F)
    for p in far:
        s9[p] = lax.dot_general(
            grads, wd[units(p), :], COLS, preferred_element_type=F32
        ).astype(BF16)
        send(s9.at[p], r9.at[sec], ssem.at[12], rsem.at[12], section=p)
    sent.append((others(s9), 12))
    act_grad = lax.dot_general(grads, wd[units(sec), :], COLS, preferred_element_type=F32)
    arrive(others(oall), rsem.at[11])
    grads = oall[...].reshape(T, F)
    for s in range(S):
        dw_out[s * Hs : (s + 1) * Hs, :] = product(hid[s], grads)
    with mark("s9"):
        arrive(others(r9), rsem.at[12])
    for k in near:
        act_grad = act_grad + r9[section(k)].astype(F32)
    aall[sec] = act_grad.astype(BF16)
    to_section(13, lambda p: aall.at[sec], aall.at[sec], others(aall), psem.at[3, sec])
    arrive(combg, rsem.at[17])
    rir[sec] = to_row(jnp.sum(act_grad * combg[...], axis=1, keepdims=True), 0)
    to_section(14, lambda p: rir.at[sec], rir.at[sec], others(rir))
    with mark("af"):
        arrive(afg.at[:, early], rsem.at[5])
        arrive(afg.at[:, late], rsem.at[8])
    part = None
    for k in range(S):
        p = section(k)
        if k:
            with mark(f"aall{k}"):
                arrive(aall.at[p], psem.at[3, p])
        act_grad = aall[p].astype(F32)
        factors = afg[p].reshape(2, T, Hs)
        up_grad = (act_grad * factors[0].astype(F32)).astype(BF16)
        gate_grad = (act_grad * factors[1].astype(F32)).astype(BF16)
        upg[p] = up_grad
        gateg[p] = gate_grad
        send(upg.at[p], up.at[p], ssem.at[19], rsem.at[19], dp=partner)
        send(gateg.at[p], gate.at[p], ssem.at[20], rsem.at[20], dp=partner)
        more = lax.dot_general(gate_grad, wg[:, units(p)], COLS, preferred_element_type=F32)
        more += lax.dot_general(up_grad, wu[:, units(p)], COLS, preferred_element_type=F32)
        part = more if part is None else part + more
    sent += [(upg, 19), (gateg, 20)]
    s11b[...] = part.astype(BF16).reshape(N, tt, F)
    for k in [*across, 0]:
        p = tensor(k)
        send(s11b.at[p], r11.at[ten], ssem.at[15], rsem.at[15], tensor=p, dp=partner)
    sent.append((s11b, 15))
    with mark("rir"):
        arrive(others(rir), rsem.at[14])
    rits[...] = jnp.sum(rir[...], axis=0)
    for k in [*across, 0]:
        send(rits, rit.at[ten], ssem.at[16], rsem.at[16], tensor=tensor(k), dp=partner)
    sent.append((rit, 16))
    with mark("gateup"):
        arrive(up, rsem.at[19])
        arrive(gate, rsem.at[20])
    for s in range(S):
        cols = slice(s * Hs, (s + 1) * Hs)
        gw_out[:, cols] = product(normed, gate[s])
        uw_out[:, cols] = product(normed, up[s])
    with mark("s11"):
        arrive(r11, rsem.at[15])
        arrive(rit, rsem.at[16])
    hidden = xg[ten].astype(F32)
    scaled_in = mg[...] * jnp.sum(r11[...].astype(F32), axis=0)
    inner = to_column(jnp.sum(rit[...], axis=0), tt, ten * tt)
    squares = to_column(jnp.sum(sqr[...], axis=0), tt, ten * tt)
    inv_in = lax.rsqrt(squares / D + EPSILON)
    hg_out[...] = outer_grad + inv_in * scaled_in - hidden * (inv_in * inv_in * inner / D)
    with mark("end"):
        for cover, lane in sent:
            arrive(cover, ssem.at[lane])


def write_kernel(*refs):
    count = len(refs) // 2
    sem = refs[-1]
    copies = [
        pltpu.make_async_copy(refs[i], refs[count + i], sem.at[i]) for i in range(count)
    ]
    for copy in copies:
        copy.start()
    for copy in copies:
        copy.wait()


def fast(
    S, N, G, enc_hidden, mlp_gain, final_gain, w_gate, w_up, w_down, key_weight, value_weight,
    queries, context_grad,
):
    tt, F = enc_hidden.shape
    T = N * tt
    H = w_gate.shape[1]
    Hs = H // S
    vmem = pl.BlockSpec(memory_space=pltpu.VMEM)
    hbm = pl.BlockSpec(memory_space=pltpu.HBM)
    shape = jax.ShapeDtypeStruct
    dma = pltpu.SemaphoreType.DMA
    wk, wv, q, c = key_weight[0], value_weight[0], queries[0], context_grad[0]
    rows, width = q.shape
    heads = width // HEAD
    buf = lambda *dims: pltpu.VMEM(dims, BF16)
    wide = lambda *dims: pltpu.VMEM(dims, F32)
    scratch = [
        wide(2, 1, F), buf(2, F, H), buf(H, F), buf(2, *wk.shape), buf(2, rows, width),
        buf(N, tt, F),
        wide(S, 1, LANES),
        buf(S, 2, T, Hs),
        buf(S, 2, T, Hs),
        wide(2, T, Hs),
        buf(2, T, Hs),
        buf(2, T, Hs),
        buf(S, T, Hs),
        buf(4, T // 2, Hs),
        buf(S, 4, T // 2, Hs),
        wide(T, Hs),
        wide(T, Hs),
        wide(N, tt, F),
        buf(N, tt, F),
        buf(N, tt, F),
        buf(S * N, tt, F),
        wide(S * N, 1, LANES),
        buf(S * N, tt, F),
        buf(S * N, tt, F),
        wide(S * N, 1, LANES),
        buf(N, tt, F),
        buf(N, tt, F),
        buf(S, T, Hs),
        buf(S, T, Hs),
        buf(S, T, Hs),
        wide(S, 1, LANES),
        buf(S, T, Hs),
        buf(S, T, Hs),
        buf(S, T, Hs),
        buf(S, T, Hs),
        buf(N, tt, F),
        buf(N, tt, F),
        wide(1, LANES),
        wide(N, 1, LANES),
        buf(heads, T, rows),
        dma((6,)), dma((21,)), dma((21,)), dma((5, S)),
    ]
    results = [
        ((tt, F), F32), ((rows, width), BF16), ((F, H), BF16), ((F, H), BF16), ((H, F), BF16)
    ]
    made = pl.pallas_call(
        functools.partial(chain_kernel, S, N, G),
        out_shape=[pltpu.VMEM(*result) for result in results],
        in_specs=[hbm] * 10,
        out_specs=[vmem] * 5,
        scratch_shapes=scratch,
        compiler_params=pltpu.CompilerParams(
            collective_id=0, has_side_effects=True, vmem_limit_bytes=CHAIN_VMEM_LIMIT
        ),
    )(enc_hidden, mlp_gain[None, :], final_gain[None, :], w_gate, w_up, w_down, wk, wv, q, c)
    hidden_grad, query_grad, gate_grad, up_grad, down_grad = pl.pallas_call(
        write_kernel,
        out_shape=[shape(*result) for result in results],
        in_specs=[vmem] * 5,
        out_specs=[hbm] * 5,
        scratch_shapes=[dma((5,))],
        compiler_params=pltpu.CompilerParams(vmem_limit_bytes=WRITE_VMEM_LIMIT),
    )(*made)
    return query_grad[None, :, :], hidden_grad, gate_grad, up_grad, down_grad


def on_device(S, N, G, enc_hidden, mlp_gain, final_gain, w_gate, *rest):
    tt, F = enc_hidden.shape
    Hs = w_gate.shape[1] // S
    fits = Hs % LANES == 0 and F % LANES == 0 and tt % 16 == 0 and N * tt <= LANES
    run = functools.partial(fast, S, N, G) if fits and G == 2 else functools.partial(general, S, N)
    return run(enc_hidden, mlp_gain, final_gain, w_gate, *rest)


def solution(mesh):
    in_specs = (
        P(("dp", "tensor"), "section"),
        P("section"),
        P("section"),
        P("section", "tensor"),
        P("section", "tensor"),
        P("tensor", "section"),
        P("section", None, "tensor"),
        P("section", None, "tensor"),
        P("section", "dp", "tensor"),
        P("section", "dp", "tensor"),
    )
    out_specs = (
        P("section", "dp", "tensor"),
        P(("dp", "tensor"), "section"),
        P(("dp", "section"), "tensor"),
        P(("dp", "section"), "tensor"),
        P(("dp", "tensor"), "section"),
    )
    sizes = [mesh.shape[axis] for axis in ("section", "tensor", "dp")]
    body = functools.partial(on_device, *sizes)
    return jax.shard_map(
        body, mesh=mesh, in_specs=in_specs, out_specs=out_specs, check_vma=False
    )
```

```python
import contextlib
import functools
import jax
import jax.numpy as jnp
from jax import lax
from jax.experimental import pallas as pl
from jax.experimental.pallas import tpu as pltpu
from jax.sharding import PartitionSpec as P

HEAD = 256
EPSILON = 1e-06
LANES = 128
MESH = pl.DeviceIdType.MESH
VMEM_LIMIT = 58 * 1024 * 1024
CHAIN_VMEM_LIMIT = 54 * 1024 * 1024
WRITE_VMEM_LIMIT = 4 * 1024 * 1024
ROWS = (((0,), (0,)), ((), ()))
COLS = (((1,), (1,)), ((), ()))
F32 = jnp.float32
BF16 = jnp.bfloat16


def mark(name):
    return contextlib.nullcontext()


def enter(sizes):
    barrier = pltpu.get_barrier_semaphore()
    for axis, n in sizes:
        me = lax.axis_index(axis)
        for k in range(1, n):
            pl.semaphore_signal(
                barrier, inc=1, device_id={axis: lax.rem(me + k, n)}, device_id_type=MESH
            )
    pl.semaphore_wait(barrier, sum(n - 1 for _, n in sizes))


def post(axis, n, source, target, send_sem, recv_sem):
    me = lax.axis_index(axis)
    copies = []
    for k in range(1, n):
        peer = lax.rem(me + k, n)
        copy = pltpu.make_async_remote_copy(
            src_ref=source(peer),
            dst_ref=target(k - 1),
            send_sem=send_sem.at[k - 1],
            recv_sem=recv_sem.at[k - 1],
            device_id={axis: peer},
            device_id_type=MESH,
        )
        copy.start()
        copies.append(copy)
    return copies


def gather(axis, n, ref, send_sem, recv_sem):
    me = lax.axis_index(axis)
    return post(axis, n, lambda peer: ref.at[me], lambda k: ref.at[me], send_sem, recv_sem)


def scatter(axis, n, out, into, send_sem, recv_sem):
    return post(axis, n, lambda peer: out.at[peer], lambda k: into.at[k], send_sem, recv_sem)


def finish(*groups):
    for copies in groups:
        for copy in copies:
            copy.wait()


def total(own, into, n):
    acc = own.astype(F32)
    for k in range(n - 1):
        acc = acc + into[k].astype(F32)
    return acc


def attend(keys, values, q, c):
    scale = HEAD ** (-0.5)
    scores = lax.dot_general(keys, q, COLS, preferred_element_type=F32) * scale
    weights = jnp.exp(scores - jnp.max(scores, axis=0, keepdims=True))
    probs = weights / jnp.sum(weights, axis=0, keepdims=True)
    probs_bf = probs.astype(BF16)
    dprob = lax.dot_general(values, c, COLS, preferred_element_type=F32)
    delta = jnp.sum(probs_bf.astype(F32) * dprob, axis=0, keepdims=True)
    dscore = (probs * (dprob - delta) * scale).astype(BF16)
    query_grad = lax.dot_general(dscore, keys, ROWS, preferred_element_type=F32).astype(BF16)
    key_grad = jnp.dot(dscore, q, preferred_element_type=F32).astype(BF16)
    value_grad = jnp.dot(probs_bf, c, preferred_element_type=F32).astype(BF16)
    return query_grad, key_grad, value_grad


def step_kernel(
    S, N, x_ref, mg_ref, fg_ref, wg_hbm, wu_hbm, wd_hbm, wk_hbm, wv_hbm, q_hbm, c_hbm,
    qg_hbm, hg_out, normed_out, hid_out, oall_out, gate_out, up_out,
    wg, wu, wd, wk, wv, q, c, qg,
    xg, sqs, sqr, gus, gur, hid_all, inv_all, ds, dr, feat, sqo, enc, af, eg,
    r6, s6, r6b, pin, oall, s9, r9, aall, s11, r11, pin2,
    load_sem, store_sem, ssem, rsem,
):
    tt, F = x_ref.shape
    T = N * tt
    ts = T // S
    H = wg.shape[1]
    D = F * S
    heads = q.shape[1] // HEAD
    sec = lax.axis_index("section")
    ten = lax.axis_index("tensor")
    loads = [
        pltpu.make_async_copy(src, dst, load_sem.at[i])
        for i, (src, dst) in enumerate((
            (wg_hbm, wg), (wu_hbm, wu), (wd_hbm, wd), (wk_hbm, wk), (wv_hbm, wv),
            (q_hbm, q), (c_hbm, c),
        ))
    ]
    for load in loads[:3]:
        load.start()
    xg[ten] = x_ref[...]
    enter((("section", S), ("tensor", N)))
    finish(post("tensor", N, lambda p: x_ref, lambda k: xg.at[ten], ssem.at[0], rsem.at[0]))
    wide = xg[...].reshape(T, F).astype(F32)
    scaled = (wide * mg_ref[...]).astype(BF16)
    square = jnp.sum(wide * wide, axis=1, keepdims=True)
    sqs[...] = jnp.broadcast_to(square, (T, LANES)).reshape(S, ts, LANES)
    loads[0].wait()
    gus[0] = jnp.dot(scaled, wg[...], preferred_element_type=F32).astype(BF16).reshape(S, ts, H)
    move_q = scatter("section", S, sqs, sqr, ssem.at[3], rsem.at[3])
    move_g = scatter("section", S, gus.at[0], gur.at[0], ssem.at[1], rsem.at[1])
    loads[1].wait()
    gus[1] = jnp.dot(scaled, wu[...], preferred_element_type=F32).astype(BF16).reshape(S, ts, H)
    move_u = scatter("section", S, gus.at[1], gur.at[1], ssem.at[2], rsem.at[2])
    for load in loads[3:]:
        load.start()
    finish(move_q, move_g)
    inv = lax.rsqrt(total(sqs[sec], sqr, S) / D + EPSILON)
    inv_all[sec] = inv
    inv = inv[:, :1]
    gate_pre = total(gus[0, sec], gur.at[0], S) * inv
    sig = jax.nn.sigmoid(gate_pre)
    act = gate_pre * sig
    af[0, sec] = act.astype(BF16)
    slope = sig * (1.0 + gate_pre * (1.0 - sig))
    finish(move_u)
    up_pre = total(gus[1, sec], gur.at[1], S) * inv
    hid_all[sec] = (act * up_pre).astype(BF16)
    move_h = gather("section", S, hid_all, ssem.at[4], rsem.at[4])
    move_i = gather("section", S, inv_all, ssem.at[5], rsem.at[5])
    af[1, sec] = (up_pre * slope).astype(BF16)
    loads[2].wait()
    finish(move_h)
    hid = hid_all[...].reshape(T, H)
    ds[...] = jnp.dot(hid, wd[...], preferred_element_type=F32).astype(BF16).reshape(N, tt, F)
    move_d = scatter("tensor", N, ds, dr, ssem.at[6], rsem.at[6])
    hid_out[...] = hid
    finish(move_i)
    inv_tok = inv_all[...].reshape(T, LANES)
    normed_out[...] = (wide * inv_tok[:, :1] * mg_ref[...]).astype(BF16)
    finish(move_d)
    outer = x_ref[...].astype(F32) + total(ds[ten], dr, N)
    feat[sec] = (outer * fg_ref[...]).astype(BF16)
    sqo[sec] = jnp.broadcast_to(jnp.sum(outer * outer, axis=1, keepdims=True), (tt, LANES))
    move_s = gather("section", S, sqo, ssem.at[8], rsem.at[8])
    move_f = gather("section", S, feat, ssem.at[7], rsem.at[7])
    finish(move_s, move_f)
    move_act = gather("section", S, af.at[0], ssem.at[10], rsem.at[10])
    move_fac = gather("section", S, af.at[1], ssem.at[11], rsem.at[11])
    inv_o = lax.rsqrt(jnp.sum(sqo[...], axis=0) / D + EPSILON)
    enc[ten] = (feat[...].astype(F32) * inv_o[None, :, :1]).astype(BF16)
    inv_o = inv_o[:, :1]
    move_e = gather("tensor", N, enc, ssem.at[9], rsem.at[9])
    for load in loads[3:]:
        load.wait()
    finish(move_e)

    width = heads * HEAD
    keys = jnp.zeros((T, width), F32)
    values = jnp.zeros((T, width), F32)
    for s in range(S):
        block = enc[:, s].reshape(T, F)
        keys += jnp.dot(block, wk[s * F : (s + 1) * F, :], preferred_element_type=F32)
        values += jnp.dot(block, wv[s * F : (s + 1) * F, :], preferred_element_type=F32)
    keys = keys.astype(BF16)
    values = values.astype(BF16)
    key_grads, value_grads, stores = [], [], []
    for h in range(heads):
        cols = slice(h * HEAD, (h + 1) * HEAD)
        query_grad, key_grad, value_grad = attend(
            keys[:, cols], values[:, cols], q[:, cols], c[:, cols]
        )
        qg[h] = query_grad
        store = pltpu.make_async_copy(qg.at[h], qg_hbm.at[:, cols], store_sem.at[h])
        store.start()
        stores.append(store)
        key_grads.append(key_grad)
        value_grads.append(value_grad)
    key_grad = jnp.concatenate(key_grads, axis=1)
    value_grad = jnp.concatenate(value_grads, axis=1)
    for s in range(S):
        rows = slice(s * F, (s + 1) * F)
        part = lax.dot_general(key_grad, wk[rows, :], COLS, preferred_element_type=F32)
        part += lax.dot_general(value_grad, wv[rows, :], COLS, preferred_element_type=F32)
        eg[:, s] = part.astype(BF16).reshape(N, tt, F)

    finish(scatter("tensor", N, eg, r6, ssem.at[12], rsem.at[12]))
    s6[...] = total(eg[ten], r6, N).astype(BF16)
    finish(scatter("section", S, s6, r6b, ssem.at[13], rsem.at[13]))
    scaled_out = fg_ref[...] * total(s6[sec], r6b, S)
    pin[sec] = jnp.broadcast_to(
        jnp.sum(scaled_out * outer, axis=1, keepdims=True), (tt, LANES)
    )
    finish(gather("section", S, pin, ssem.at[14], rsem.at[14]))
    inner = jnp.sum(pin[...], axis=0)[:, :1] / D
    outer_grad = inv_o * scaled_out - outer * (inv_o * inv_o * inv_o * inner)
    oall[ten] = outer_grad.astype(BF16)
    finish(gather("tensor", N, oall, ssem.at[15], rsem.at[15]))
    grads = oall[...].reshape(T, F)
    half = H // 2
    moves = []
    for i in range(2):
        s9[i] = (
            lax.dot_general(
                grads, wd[i * half : (i + 1) * half, :], COLS, preferred_element_type=F32
            )
            .astype(BF16)
            .reshape(S, ts, half)
        )
        moves.append(scatter("section", S, s9.at[i], r9.at[i], ssem.at[16 + i], rsem.at[16 + i]))
    oall_out[...] = grads
    finish(move_act, move_fac)
    gathers = []
    for i in range(2):
        finish(moves[i])
        aall[i, sec] = total(s9[i, sec], r9.at[i], S).astype(BF16)
        gathers.append(gather("section", S, aall.at[i], ssem.at[18 + i], rsem.at[18 + i]))
    parts = None
    for i in range(2):
        cols = slice(i * half, (i + 1) * half)
        finish(gathers[i])
        act_grad = aall[i].reshape(T, half).astype(F32)
        up_grad = (act_grad * af[0, :, :, cols].reshape(T, half).astype(F32)).astype(BF16)
        gate_grad = (act_grad * af[1, :, :, cols].reshape(T, half).astype(F32)).astype(BF16)
        up_out[:, cols] = up_grad
        gate_out[:, cols] = gate_grad
        part = lax.dot_general(gate_grad, wg[:, cols], COLS, preferred_element_type=F32)
        part += lax.dot_general(up_grad, wu[:, cols], COLS, preferred_element_type=F32)
        parts = part if parts is None else parts + part
    s11[...] = parts.astype(BF16).reshape(N, tt, F)
    finish(scatter("tensor", N, s11, r11, ssem.at[20], rsem.at[20]))
    hidden = x_ref[...].astype(F32)
    scaled_in = mg_ref[...] * total(s11[ten], r11, N)
    pin2[sec] = jnp.broadcast_to(
        jnp.sum(scaled_in * hidden, axis=1, keepdims=True), (tt, LANES)
    )
    finish(gather("section", S, pin2, ssem.at[21], rsem.at[21]))
    inner_in = jnp.sum(pin2[...], axis=0)[:, :1] / D
    inv_flat = inv_all.reshape(T, LANES)
    inv_in = inv_flat[pl.ds(pl.multiple_of(ten * tt, tt), tt), :][:, :1]
    hg_out[...] = (
        outer_grad + inv_in * scaled_in - hidden * (inv_in * inv_in * inv_in * inner_in)
    )
    for store in stores:
        store.wait()


def general(
    S, N, enc_hidden, mlp_gain, final_gain, w_gate, w_up, w_down, key_weight, value_weight,
    queries, context_grad,
):
    tt, F = enc_hidden.shape
    T = N * tt
    ts = T // S
    H = w_gate.shape[1]
    peers = max(S, N) - 1
    vmem = pl.BlockSpec(memory_space=pltpu.VMEM)
    hbm = pl.BlockSpec(memory_space=pl.ANY)
    shape = jax.ShapeDtypeStruct
    dma = pltpu.SemaphoreType.DMA
    wk, wv, q, c = key_weight[0], value_weight[0], queries[0], context_grad[0]
    large = (w_gate, w_up, w_down, wk, wv, q, c)
    rows = q.shape[0]
    heads = q.shape[1] // HEAD
    scratch = [pltpu.VMEM(w.shape, BF16) for w in large]
    scratch += [
        pltpu.VMEM((heads, rows, HEAD), BF16),
        pltpu.VMEM((N, tt, F), BF16),
        pltpu.VMEM((S, ts, LANES), F32),
        pltpu.VMEM((S - 1, ts, LANES), F32),
        pltpu.VMEM((2, S, ts, H), BF16),
        pltpu.VMEM((2, S - 1, ts, H), BF16),
        pltpu.VMEM((S, ts, H), BF16),
        pltpu.VMEM((S, ts, LANES), F32),
        pltpu.VMEM((N, tt, F), BF16),
        pltpu.VMEM((N - 1, tt, F), BF16),
        pltpu.VMEM((S, tt, F), BF16),
        pltpu.VMEM((S, tt, LANES), F32),
        pltpu.VMEM((N, S, tt, F), BF16),
        pltpu.VMEM((2, S, ts, H), BF16),
        pltpu.VMEM((N, S, tt, F), BF16),
        pltpu.VMEM((N - 1, S, tt, F), BF16),
        pltpu.VMEM((S, tt, F), BF16),
        pltpu.VMEM((S - 1, tt, F), BF16),
        pltpu.VMEM((S, tt, LANES), F32),
        pltpu.VMEM((N, tt, F), BF16),
        pltpu.VMEM((2, S, ts, H // 2), BF16),
        pltpu.VMEM((2, S - 1, ts, H // 2), BF16),
        pltpu.VMEM((2, S, ts, H // 2), BF16),
        pltpu.VMEM((N, tt, F), BF16),
        pltpu.VMEM((N - 1, tt, F), BF16),
        pltpu.VMEM((S, tt, LANES), F32),
        dma((7,)), dma((heads,)), dma((22, peers)), dma((22, peers)),
    ]
    query_grad, hidden_grad, normed, hid, outer_all, gate_all, up_all = pl.pallas_call(
        functools.partial(step_kernel, S, N),
        out_shape=[
            shape(q.shape, BF16), shape((tt, F), F32), shape((T, F), BF16),
            shape((T, H), BF16), shape((T, F), BF16), shape((T, H), BF16), shape((T, H), BF16),
        ],
        in_specs=[vmem] * 3 + [hbm] * 7,
        out_specs=[hbm] + [vmem] * 6,
        scratch_shapes=scratch,
        compiler_params=pltpu.CompilerParams(
            collective_id=0, has_side_effects=True, vmem_limit_bytes=VMEM_LIMIT
        ),
    )(enc_hidden, mlp_gain[None, :], final_gain[None, :], *large)

    outer_product = lambda a, b: lax.dot_general(
        a, b, ROWS, preferred_element_type=F32
    ).astype(BF16)
    return (
        query_grad[None, :, :],
        hidden_grad,
        outer_product(normed, gate_all),
        outer_product(normed, up_all),
        outer_product(hid, outer_all),
    )


def lane_of_row(rows, offset):
    row = lax.broadcasted_iota(jnp.int32, (rows, LANES), 0) + offset
    return (row == lax.broadcasted_iota(jnp.int32, (rows, LANES), 1)).astype(F32)


def to_row(column, offset):
    return jnp.sum(column * lane_of_row(column.shape[0], offset), axis=0, keepdims=True)


def to_column(row, rows, offset):
    return jnp.sum(row * lane_of_row(rows, offset), axis=1, keepdims=True)


def send(source, target, send_sem, recv_sem, **peer):
    pltpu.make_async_remote_copy(
        src_ref=source,
        dst_ref=target,
        send_sem=send_sem,
        recv_sem=recv_sem,
        device_id=peer,
        device_id_type=MESH,
    ).start()


def arrive(cover, sem):
    pltpu.make_async_copy(cover, cover, sem).wait()


def product(a, b):
    return lax.dot_general(a, b, ROWS, preferred_element_type=F32).astype(BF16)


def chain_kernel(
    S, N, G, x_hbm, mg_hbm, fg_hbm, wg_hbm, wu_hbm, wd_hbm, wk_hbm, wv_hbm, q_hbm, c_hbm,
    hg_out, qg_out, gw_out, uw_out, dw_out,
    gains, wgu, wd, wkv, qc,
    xg, sqr, gus, gur, hold, stage, joined, hid, af, afg, comb, combg, ds, dsb, dr, encb, sso, egb, er, ror, oall, oallg,
    s9, r9, aall, rir, gateg, upg, gate, up, s11b, r11, rits, rit, dsc,
    load_sem, ssem, rsem, psem,
):
    tt, F = x_hbm.shape
    T = N * tt
    H = wd.shape[0]
    Hs = H // S
    D = F * S
    heads = qc.shape[2] // HEAD
    sec = lax.axis_index("section")
    ten = lax.axis_index("tensor")
    partner = lax.rem(lax.axis_index("dp") + 1, G)
    turn = 1 - 2 * (sec // ((S + 1) // 2))
    sent = []

    def section(k):
        return lax.rem(sec + turn * k + S, S)

    def tensor(k):
        return lax.rem(ten + k, N)

    low = (1 - turn) // 2
    rank = low * (S - 1) + turn * sec

    def distant(i):
        other = S - 1 - i - (i + rank) // (S - 1)
        return low * (S - 1) + turn * other

    def place(y):
        return low * (S - 1) + turn * y

    near = range(1, S)
    far = [distant(i) for i in range(S - 1)]
    across = range(1, N)

    def units(p):
        return pl.ds(pl.multiple_of(p * Hs, LANES), Hs)

    def features(p):
        return pl.ds(pl.multiple_of(p * F, F), F)

    def others(ref):
        return ref.at[pl.ds(0, ref.shape[0] - 1)]

    def to_tensor(lane, source, target, cover):
        for k in across:
            send(source(tensor(k)), target, ssem.at[lane], rsem.at[lane], tensor=tensor(k))
        sent.append((cover, lane))

    def to_section(lane, source, target, cover, sem=None):
        for p in far:
            send(
                source(p), target, ssem.at[lane], rsem.at[lane] if sem is None else sem, section=p
            )
        sent.append((cover, lane))

    def to_everyone(lane, source, target, sections):
        for p in sections:
            for j in range(N):
                if p is not sec or j:
                    send(
                        source(p, tensor(j)), target, ssem.at[lane], rsem.at[lane],
                        section=p, tensor=tensor(j),
                    )

    barrier = pltpu.get_barrier_semaphore()
    for k in range(S):
        for j in range(N):
            if k or j:
                pl.semaphore_signal(
                    barrier,
                    inc=1,
                    device_id={"section": section(k), "tensor": tensor(j)},
                    device_id_type=MESH,
                )
    crossed = [(p, ten) for p in [sec, *far]] + [(sec, tensor(j)) for j in across]
    for p, n in crossed:
        pl.semaphore_signal(
            barrier,
            inc=1,
            device_id={"section": p, "tensor": n, "dp": partner},
            device_id_type=MESH,
        )
    loads = [
        pltpu.make_async_copy(src, dst, load_sem.at[i])
        for src, dst, i in (
            (x_hbm, xg.at[ten], 0), (mg_hbm, gains.at[0], 1), (fg_hbm, gains.at[1], 1),
            (wg_hbm, wgu.at[0], 2), (wu_hbm, wgu.at[1], 2), (wd_hbm, wd, 3),
            (wk_hbm, wkv.at[0], 4), (wv_hbm, wkv.at[1], 4),
            (q_hbm, qc.at[0], 5), (c_hbm, qc.at[1], 5),
        )
    ]
    for load in loads[:6]:
        load.start()
    loads[0].wait()
    with mark("enter"):
        pl.semaphore_wait(barrier, S * N - 1 + len(crossed))
    to_tensor(0, lambda p: xg.at[ten], xg.at[ten], others(xg))
    arrive(gains, load_sem.at[1])
    arrive(wgu, load_sem.at[2])
    mg, fg = gains.at[0], gains.at[1]
    wg, wu = wgu.at[0], wgu.at[1]
    wk, wv = wkv.at[0], wkv.at[1]
    with mark("x"):
        arrive(others(xg), rsem.at[0])

    wide = xg[...].reshape(T, F).astype(F32)
    scaled = (wide * mg[...]).astype(BF16)
    square = jnp.sum(wide * wide, axis=1, keepdims=True)
    sqr[sec] = to_row(square, 0)
    to_section(1, lambda p: sqr.at[sec], sqr.at[sec], others(sqr))
    line = S == 4
    for i, p in enumerate(far):
        for side, weight in enumerate((wg, wu)):
            part = jnp.dot(scaled, weight[:, units(p)], preferred_element_type=F32)
            gus[p, side] = part.astype(BF16)
            if line and i == 0:
                hold[side] = part

                @pl.when(rank == 0)
                def _(p=p, side=side):
                    send(
                        gus.at[p, side], stage.at[side], ssem.at[2], psem.at[4, side],
                        section=place(1),
                    )

        if not (line and i == 0):
            send(gus.at[p], gur.at[sec], ssem.at[2], rsem.at[2], section=p)
    sent.append((others(gus), 2))
    for load in loads[6:]:
        load.start()
    gate_pre = jnp.dot(scaled, wg[:, units(sec)], preferred_element_type=F32)
    up_pre = jnp.dot(scaled, wu[:, units(sec)], preferred_element_type=F32)
    if line:
        end = place(S - 1)

        @pl.when(rank == 0)
        def _():
            gur[end] = jnp.zeros(gur.shape[1:], BF16)

        @pl.when(rank == 1)
        def _():
            for side in range(2):
                with mark(f"stage{side}"):
                    arrive(stage.at[side], psem.at[4, side])
                joined[side] = (hold[side] + stage[side].astype(F32)).astype(BF16)
                send(joined.at[side], gur.at[sec, side], ssem.at[2], rsem.at[2], section=end)

    with mark("sq"):
        arrive(others(sqr), rsem.at[1])
    inv = lax.rsqrt(to_column(jnp.sum(sqr[...], axis=0), T, 0) / D + EPSILON)
    normed = (wide * inv * mg[...]).astype(BF16)
    loads[5].wait()
    with mark("gu"):
        if line:
            @pl.when(rank == 0)
            def _():
                arrive(gur.at[pl.ds(0, S - 2)], rsem.at[2])

            @pl.when(rank == 1)
            def _():
                arrive(others(gur), rsem.at[2])
        else:
            arrive(others(gur), rsem.at[2])
    for k in near:
        gate_pre = gate_pre + gur[section(k), 0].astype(F32)
        up_pre = up_pre + gur[section(k), 1].astype(F32)
    gate_pre = gate_pre * inv
    up_pre = up_pre * inv
    sig = jax.nn.sigmoid(gate_pre)
    act = gate_pre * sig
    hid[sec] = (act * up_pre).astype(BF16)
    to_section(3, lambda p: hid.at[sec], hid.at[sec], others(hid), psem.at[0, sec])
    factor = up_pre * (sig * (1.0 + gate_pre * (1.0 - sig)))
    piece = T // 2
    af[0] = act[:piece].astype(BF16)
    af[1] = act[piece:].astype(BF16)
    af[2] = factor[:piece].astype(BF16)
    af[3] = factor[piece:].astype(BF16)
    comb[...] = act * up_pre + factor * gate_pre
    send(comb, combg, ssem.at[17], rsem.at[17], dp=partner)
    sent.append((comb, 17))
    down = jnp.dot(hid[sec], wd[units(sec), :], preferred_element_type=F32)
    for k in near:
        p = section(k)
        with mark(f"hid{k}"):
            arrive(hid.at[p], psem.at[0, p])
        down = down + jnp.dot(hid[p], wd[units(p), :], preferred_element_type=F32)
    ds[...] = down.reshape(N, tt, F)
    dsb[...] = down.astype(BF16).reshape(N, tt, F)
    to_tensor(4, lambda p: dsb.at[p], dr.at[ten], others(dsb))
    early, late = pl.ds(0, 2), pl.ds(2, 2)

    def share_factors(lane, pieces):
        for p in [*far, sec]:
            send(
                af.at[pieces], afg.at[sec, pieces], ssem.at[lane], rsem.at[lane],
                section=p, dp=partner,
            )
        sent.append((afg.at[:, pieces], lane))

    share_factors(5, early)
    with mark("ds"):
        arrive(others(dr), rsem.at[4])
    outer = xg[ten].astype(F32) + ds[ten]
    for k in across:
        outer = outer + dr[tensor(k)].astype(F32)
    me = sec * N + ten
    sso[me] = to_row(jnp.sum(outer * outer, axis=1, keepdims=True), ten * tt)
    encb[me] = (outer * fg[...]).astype(BF16)
    to_everyone(6, lambda s, n: sso.at[me], sso.at[me], [*far, sec])
    sent.append((others(sso), 6))
    for p in far:
        send(encb.at[me], encb.at[me], ssem.at[7], psem.at[1, sec], section=p)
    for k in across:
        send(encb.at[me], encb.at[me], ssem.at[7], psem.at[2, sec], tensor=tensor(k))
    for k in near:
        block = section(k) * N + ten
        with mark(f"pass{k}"):
            arrive(encb.at[block], psem.at[1, section(k)])
        for j in across:
            send(
                encb.at[block], encb.at[block], ssem.at[7], psem.at[2, section(k)],
                tensor=tensor(j),
            )
    sent.append((others(encb), 7))
    share_factors(8, late)
    arrive(wkv, load_sem.at[4])
    arrive(qc, load_sem.at[5])
    keys = values = None
    for k in range(S):
        p = section(k)
        with mark(f"enc{k}"):
            arrive(encb.at[pl.ds(0, N - 1)], psem.at[2, p])
        block = encb[pl.ds(p * N, N)].reshape(T, F)
        key_part = jnp.dot(block, wk[features(p), :], preferred_element_type=F32)
        value_part = jnp.dot(block, wv[features(p), :], preferred_element_type=F32)
        keys = key_part if keys is None else keys + key_part
        values = value_part if values is None else values + value_part
    with mark("sso"):
        arrive(others(sso), rsem.at[6])
    squares = jnp.sum(sso[...], axis=0)
    inv_all = lax.rsqrt(to_column(squares, T, 0) / D + EPSILON)
    inv_o = lax.rsqrt(to_column(squares, tt, ten * tt) / D + EPSILON)
    keys = (keys * inv_all).astype(BF16)
    values = (values * inv_all).astype(BF16)
    scale = HEAD ** (-0.5)
    key_grads, value_grads = [], []
    inner = None
    for h in range(heads):
        cols = slice(h * HEAD, (h + 1) * HEAD)
        q, c = qc[0, :, cols], qc[1, :, cols]
        scores = lax.dot_general(keys[:, cols], q, COLS, preferred_element_type=F32) * scale
        weights = jnp.exp(scores - jnp.max(scores, axis=0, keepdims=True))
        probs = weights / jnp.sum(weights, axis=0, keepdims=True)
        probs_bf = probs.astype(BF16)
        dprob = lax.dot_general(values[:, cols], c, COLS, preferred_element_type=F32)
        delta = jnp.sum(probs_bf.astype(F32) * dprob, axis=0, keepdims=True)
        dscore = (probs * (dprob - delta) * scale).astype(BF16)
        dsc[h] = dscore
        key_grad = jnp.dot(dscore, q, preferred_element_type=F32).astype(BF16)
        value_grad = jnp.dot(probs_bf, c, preferred_element_type=F32).astype(BF16)
        part = key_grad.astype(F32) * keys[:, cols].astype(F32)
        part += value_grad.astype(F32) * values[:, cols].astype(F32)
        inner = part if inner is None else inner + part
        key_grads.append(key_grad)
        value_grads.append(value_grad)
    key_grad = jnp.concatenate(key_grads, axis=1)
    value_grad = jnp.concatenate(value_grads, axis=1)
    ror[me] = to_row(jnp.sum(inner, axis=1, keepdims=True), 0)
    to_everyone(9, lambda s, n: ror.at[me], ror.at[me], [*far, sec])
    sent.append((others(ror), 9))
    for p in [*far, sec]:
        part = lax.dot_general(key_grad, wk[features(p), :], COLS, preferred_element_type=F32)
        part += lax.dot_general(value_grad, wv[features(p), :], COLS, preferred_element_type=F32)
        egb[pl.ds(p * N, N)] = part.astype(BF16).reshape(N, tt, F)
        to_everyone(10, lambda s, n: egb.at[s * N + n], er.at[me], [p])
    sent.append((others(egb), 10))
    er[me] = egb[me]
    for h in range(heads):
        cols = slice(h * HEAD, (h + 1) * HEAD)
        qg_out[:, cols] = product(dsc[h], keys[:, cols])
    with mark("eg"):
        arrive(others(ror), rsem.at[9])
        arrive(others(er), rsem.at[10])
    inner = to_column(jnp.sum(ror[...], axis=0), tt, ten * tt)
    grad = jnp.sum(er[...].astype(F32), axis=0)
    outer_grad = inv_o * (fg[...] * grad) - outer * (inv_o * inv_o * inner / D)
    oall[ten] = outer_grad.astype(BF16)
    for k in range(N):
        send(
            oall.at[ten], oallg.at[ten], ssem.at[18], rsem.at[18], tensor=tensor(k), dp=partner
        )
    sent.append((oall, 18))
    to_tensor(11, lambda p: oall.at[ten], oall.at[ten], others(oall))
    with mark("oall"):
        arrive(oallg, rsem.at[18])
    grads = oallg[...].reshape(T, F)
    for p in far:
        s9[p] = lax.dot_general(
            grads, wd[units(p), :], COLS, preferred_element_type=F32
        ).astype(BF16)
        send(s9.at[p], r9.at[sec], ssem.at[12], rsem.at[12], section=p)
    sent.append((others(s9), 12))
    act_grad = lax.dot_general(grads, wd[units(sec), :], COLS, preferred_element_type=F32)
    arrive(others(oall), rsem.at[11])
    grads = oall[...].reshape(T, F)
    for s in range(S):
        dw_out[s * Hs : (s + 1) * Hs, :] = product(hid[s], grads)
    with mark("s9"):
        arrive(others(r9), rsem.at[12])
    for k in near:
        act_grad = act_grad + r9[section(k)].astype(F32)
    aall[sec] = act_grad.astype(BF16)
    to_section(13, lambda p: aall.at[sec], aall.at[sec], others(aall), psem.at[3, sec])
    arrive(combg, rsem.at[17])
    rir[sec] = to_row(jnp.sum(act_grad * combg[...], axis=1, keepdims=True), 0)
    to_section(14, lambda p: rir.at[sec], rir.at[sec], others(rir))
    with mark("af"):
        arrive(afg.at[:, early], rsem.at[5])
        arrive(afg.at[:, late], rsem.at[8])
    part = None
    for k in range(S):
        p = section(k)
        if k:
            with mark(f"aall{k}"):
                arrive(aall.at[p], psem.at[3, p])
        act_grad = aall[p].astype(F32)
        factors = afg[p].reshape(2, T, Hs)
        up_grad = (act_grad * factors[0].astype(F32)).astype(BF16)
        gate_grad = (act_grad * factors[1].astype(F32)).astype(BF16)
        upg[p] = up_grad
        gateg[p] = gate_grad
        send(upg.at[p], up.at[p], ssem.at[19], rsem.at[19], dp=partner)
        send(gateg.at[p], gate.at[p], ssem.at[20], rsem.at[20], dp=partner)
        more = lax.dot_general(gate_grad, wg[:, units(p)], COLS, preferred_element_type=F32)
        more += lax.dot_general(up_grad, wu[:, units(p)], COLS, preferred_element_type=F32)
        part = more if part is None else part + more
    sent += [(upg, 19), (gateg, 20)]
    s11b[...] = part.astype(BF16).reshape(N, tt, F)
    for k in [*across, 0]:
        p = tensor(k)
        send(s11b.at[p], r11.at[ten], ssem.at[15], rsem.at[15], tensor=p, dp=partner)
    sent.append((s11b, 15))
    with mark("rir"):
        arrive(others(rir), rsem.at[14])
    rits[...] = jnp.sum(rir[...], axis=0)
    for k in [*across, 0]:
        send(rits, rit.at[ten], ssem.at[16], rsem.at[16], tensor=tensor(k), dp=partner)
    sent.append((rit, 16))
    with mark("gateup"):
        arrive(up, rsem.at[19])
        arrive(gate, rsem.at[20])
    for s in range(S):
        cols = slice(s * Hs, (s + 1) * Hs)
        gw_out[:, cols] = product(normed, gate[s])
        uw_out[:, cols] = product(normed, up[s])
    with mark("s11"):
        arrive(r11, rsem.at[15])
        arrive(rit, rsem.at[16])
    hidden = xg[ten].astype(F32)
    scaled_in = mg[...] * jnp.sum(r11[...].astype(F32), axis=0)
    inner = to_column(jnp.sum(rit[...], axis=0), tt, ten * tt)
    squares = to_column(jnp.sum(sqr[...], axis=0), tt, ten * tt)
    inv_in = lax.rsqrt(squares / D + EPSILON)
    hg_out[...] = outer_grad + inv_in * scaled_in - hidden * (inv_in * inv_in * inner / D)
    with mark("end"):
        for cover, lane in sent:
            arrive(cover, ssem.at[lane])


def write_kernel(*refs):
    count = len(refs) // 2
    sem = refs[-1]
    copies = [
        pltpu.make_async_copy(refs[i], refs[count + i], sem.at[i]) for i in range(count)
    ]
    for copy in copies:
        copy.start()
    for copy in copies:
        copy.wait()


def fast(
    S, N, G, enc_hidden, mlp_gain, final_gain, w_gate, w_up, w_down, key_weight, value_weight,
    queries, context_grad,
):
    tt, F = enc_hidden.shape
    T = N * tt
    H = w_gate.shape[1]
    Hs = H // S
    vmem = pl.BlockSpec(memory_space=pltpu.VMEM)
    hbm = pl.BlockSpec(memory_space=pltpu.HBM)
    shape = jax.ShapeDtypeStruct
    dma = pltpu.SemaphoreType.DMA
    wk, wv, q, c = key_weight[0], value_weight[0], queries[0], context_grad[0]
    rows, width = q.shape
    heads = width // HEAD
    buf = lambda *dims: pltpu.VMEM(dims, BF16)
    wide = lambda *dims: pltpu.VMEM(dims, F32)
    scratch = [
        wide(2, 1, F), buf(2, F, H), buf(H, F), buf(2, *wk.shape), buf(2, rows, width),
        buf(N, tt, F),
        wide(S, 1, LANES),
        buf(S, 2, T, Hs),
        buf(S, 2, T, Hs),
        wide(2, T, Hs),
        buf(2, T, Hs),
        buf(2, T, Hs),
        buf(S, T, Hs),
        buf(4, T // 2, Hs),
        buf(S, 4, T // 2, Hs),
        wide(T, Hs),
        wide(T, Hs),
        wide(N, tt, F),
        buf(N, tt, F),
        buf(N, tt, F),
        buf(S * N, tt, F),
        wide(S * N, 1, LANES),
        buf(S * N, tt, F),
        buf(S * N, tt, F),
        wide(S * N, 1, LANES),
        buf(N, tt, F),
        buf(N, tt, F),
        buf(S, T, Hs),
        buf(S, T, Hs),
        buf(S, T, Hs),
        wide(S, 1, LANES),
        buf(S, T, Hs),
        buf(S, T, Hs),
        buf(S, T, Hs),
        buf(S, T, Hs),
        buf(N, tt, F),
        buf(N, tt, F),
        wide(1, LANES),
        wide(N, 1, LANES),
        buf(heads, T, rows),
        dma((6,)), dma((21,)), dma((21,)), dma((5, S)),
    ]
    results = [
        ((tt, F), F32), ((rows, width), BF16), ((F, H), BF16), ((F, H), BF16), ((H, F), BF16)
    ]
    made = pl.pallas_call(
        functools.partial(chain_kernel, S, N, G),
        out_shape=[pltpu.VMEM(*result) for result in results],
        in_specs=[hbm] * 10,
        out_specs=[vmem] * 5,
        scratch_shapes=scratch,
        compiler_params=pltpu.CompilerParams(
            collective_id=0, has_side_effects=True, vmem_limit_bytes=CHAIN_VMEM_LIMIT
        ),
    )(enc_hidden, mlp_gain[None, :], final_gain[None, :], w_gate, w_up, w_down, wk, wv, q, c)
    hidden_grad, query_grad, gate_grad, up_grad, down_grad = pl.pallas_call(
        write_kernel,
        out_shape=[shape(*result) for result in results],
        in_specs=[vmem] * 5,
        out_specs=[hbm] * 5,
        scratch_shapes=[dma((5,))],
        compiler_params=pltpu.CompilerParams(vmem_limit_bytes=WRITE_VMEM_LIMIT),
    )(*made)
    return query_grad[None, :, :], hidden_grad, gate_grad, up_grad, down_grad


def on_device(S, N, G, enc_hidden, mlp_gain, final_gain, w_gate, *rest):
    tt, F = enc_hidden.shape
    Hs = w_gate.shape[1] // S
    fits = Hs % LANES == 0 and F % LANES == 0 and tt % 16 == 0 and N * tt <= LANES
    run = functools.partial(fast, S, N, G) if fits and G == 2 else functools.partial(general, S, N)
    return run(enc_hidden, mlp_gain, final_gain, w_gate, *rest)


def solution(mesh):
    in_specs = (
        P(("dp", "tensor"), "section"),
        P("section"),
        P("section"),
        P("section", "tensor"),
        P("section", "tensor"),
        P("tensor", "section"),
        P("section", None, "tensor"),
        P("section", None, "tensor"),
        P("section", "dp", "tensor"),
        P("section", "dp", "tensor"),
    )
    out_specs = (
        P("section", "dp", "tensor"),
        P(("dp", "tensor"), "section"),
        P(("dp", "section"), "tensor"),
        P(("dp", "section"), "tensor"),
        P(("dp", "tensor"), "section"),
    )
    sizes = [mesh.shape[axis] for axis in ("section", "tensor", "dp")]
    body = functools.partial(on_device, *sizes)
    return jax.shard_map(
        body, mesh=mesh, in_specs=in_specs, out_specs=out_specs, check_vma=False
    )
```
